32 devices in a mesh: dp: 4 (over y, z), x: 8 (over x, core).
Axes of the slice: x: 4, y: 2, z: 2, core: 2. Of those that a mesh axis runs over, the one named last changes fastest.
The devices are a block of a 4x4x8 slice.
Arguments:
- start_pos: int32 [512], P('dp'), parts along dimension 0
- hidden_in: bfloat16 [4, 512, 2048], P(None, ('dp', 'x')), parts along dimension 1
- k_cache: bfloat16 [512, 256, 8, 128], P('dp', None, 'x'), parts along dimension 0
- v_cache: bfloat16 [512, 256, 8, 128], P('dp', None, 'x'), parts along dimension 0
- attn_norm: bfloat16 [2048], replicated
- w_q: bfloat16 [2048, 2048], replicated
- w_k: bfloat16 [2048, 1024], replicated
- w_v: bfloat16 [2048, 1024], replicated
- q_norm: bfloat16 [128], replicated
- k_norm: bfloat16 [128], replicated
- w_o: bfloat16 [2048, 2048], replicated
- mlp_norm: bfloat16 [2048], replicated
- w_gate: bfloat16 [2048, 6144], replicated
- w_up: bfloat16 [2048, 6144], replicated
- w_down: bfloat16 [6144, 2048], replicated
Outputs:
- output 1: bfloat16 [4, 512, 2048], P(None, ('dp', 'x')), parts along dimension 1
- output 2: bfloat16 [512, 256, 8, 128], P(('dp', 'x')), parts along dimension 0
- output 3: bfloat16 [512, 256, 8, 128], P(('dp', 'x')), parts along dimension 0
There are 4 independent parts. The reference program is written for one: setup_inputs(seed, part) draws one part's arguments, and reference() takes and returns one part's arrays. A program takes and returns all parts, laid end to end along the dimension named above; an argument that names none is the same for every part.
All inputs are finite; a program needn't handle non-finite values.
Results may differ from the reference program's by a relative error of at most 0.010446.
Values are sent between devices in bfloat16 or wider.
A program may use at most 768 MiB of HBM per device.

```python
import math
import jax
import jax.numpy as jnp
from jax import lax

BATCH = 128
T = 256
D = 2048
HEADS = 16
KV_HEADS = 8
HEAD = 128
FF = 6144
STEPS = 4

EPS = 1e-6
THETA = 1000000.0
Q_GAIN = math.sqrt(0.8 * math.log(T))
K_GAIN = math.sqrt(2.0 * math.log(T))


def rms_norm(values, gain_vec):
    values32 = values.astype(jnp.float32)
    inv_rms = lax.rsqrt(jnp.mean(values32 * values32, axis=-1, keepdims=True) + EPS)
    return values32 * inv_rms * gain_vec.astype(jnp.float32)


def rotary(values, positions):
    half_dim = HEAD // 2
    inv_freq = jnp.power(THETA, -jnp.arange(half_dim, dtype=jnp.float32) * 2.0 / HEAD)
    angles = positions.astype(jnp.float32)[..., None, None] * inv_freq
    cos_part = jnp.cos(angles)
    sin_part = jnp.sin(angles)
    first_half = values[..., :half_dim]
    second_half = values[..., half_dim:]
    return jnp.concatenate([first_half * cos_part - second_half * sin_part, second_half * cos_part + first_half * sin_part], axis=-1)


def setup_inputs(seed: int = 0, part: int = 0) -> dict:
    base_keys = jax.random.split(jax.random.key(seed), 16)

    def part_normal(index, shape):
        return jax.random.normal(jax.random.fold_in(base_keys[index], part), shape, jnp.float32)

    def shared_normal(index, shape):
        return jax.random.normal(base_keys[index], shape, jnp.float32)

    pos_key = jax.random.fold_in(base_keys[0], part)
    pos_draw = jax.random.randint(jax.random.fold_in(pos_key, 1), (BATCH,), T // 4, T - 3)
    top_row = jax.random.randint(jax.random.fold_in(pos_key, 2), (), 0, BATCH)
    start_pos = jnp.where(jnp.arange(BATCH) == top_row, T - 4, pos_draw).astype(jnp.int32)
    return dict(
        start_pos=start_pos,
        hidden_in=part_normal(1, (STEPS, BATCH, D)).astype(jnp.bfloat16),
        k_cache=part_normal(2, (BATCH, T, KV_HEADS, HEAD)).astype(jnp.bfloat16),
        v_cache=part_normal(3, (BATCH, T, KV_HEADS, HEAD)).astype(jnp.bfloat16),
        attn_norm=(1.0 + 0.2 * shared_normal(4, (D,))).astype(jnp.bfloat16),
        w_q=(shared_normal(5, (D, HEADS * HEAD)) * D ** -0.5).astype(jnp.bfloat16),
        w_k=(shared_normal(6, (D, KV_HEADS * HEAD)) * D ** -0.5).astype(jnp.bfloat16),
        w_v=(shared_normal(7, (D, KV_HEADS * HEAD)) * D ** -0.5).astype(jnp.bfloat16),
        q_norm=(Q_GAIN * (1.0 + 0.2 * shared_normal(8, (HEAD,)))).astype(jnp.bfloat16),
        k_norm=(K_GAIN * (1.0 + 0.2 * shared_normal(9, (HEAD,)))).astype(jnp.bfloat16),
        w_o=(shared_normal(10, (HEADS * HEAD, D)) * (HEADS * HEAD) ** -0.5).astype(jnp.bfloat16),
        mlp_norm=(1.0 + 0.2 * shared_normal(11, (D,))).astype(jnp.bfloat16),
        w_gate=(shared_normal(12, (D, FF)) * D ** -0.5).astype(jnp.bfloat16),
        w_up=(shared_normal(13, (D, FF)) * D ** -0.5).astype(jnp.bfloat16),
        w_down=(shared_normal(14, (FF, D)) * FF ** -0.5).astype(jnp.bfloat16),
    )


def reference(start_pos, hidden_in, k_cache, v_cache, attn_norm, w_q, w_k, w_v, q_norm, k_norm, w_o, mlp_norm, w_gate, w_up, w_down):
    group_size = HEADS // KV_HEADS
    score_scale = HEAD ** -0.5
    tokens = rms_norm(hidden_in, attn_norm).astype(jnp.bfloat16).reshape(STEPS * BATCH, D)
    queries = jnp.dot(tokens, w_q, preferred_element_type=jnp.float32).reshape(STEPS, BATCH, HEADS, HEAD)
    keys_new = jnp.dot(tokens, w_k, preferred_element_type=jnp.float32).reshape(STEPS, BATCH, KV_HEADS, HEAD)
    values_new = jnp.dot(tokens, w_v, preferred_element_type=jnp.float32).reshape(STEPS, BATCH, KV_HEADS, HEAD)
    positions = start_pos[None, :] + jnp.arange(STEPS)[:, None]
    queries = rotary(rms_norm(queries, q_norm), positions).astype(jnp.bfloat16)
    keys_new = rotary(rms_norm(keys_new, k_norm), positions).astype(jnp.bfloat16)
    values_new = values_new.astype(jnp.bfloat16)

    def one_row(row_inputs):
        row_q, row_k, row_v, row_kc, row_vc, row_pos = row_inputs

        def one_step(carry_in, step_inputs):
            cache_k, cache_v = carry_in
            step_q, step_k, step_v, slot_idx = step_inputs
            cache_k = lax.dynamic_update_slice(cache_k, step_k[None], (slot_idx, 0, 0))
            cache_v = lax.dynamic_update_slice(cache_v, step_v[None], (slot_idx, 0, 0))
            grouped = step_q.reshape(KV_HEADS, group_size, HEAD).astype(jnp.float32)
            scores = jnp.einsum('kgd,tkd->kgt', grouped, cache_k.astype(jnp.float32)) * score_scale
            slot_valid = jnp.arange(T) <= slot_idx
            scores = jnp.where(slot_valid, scores, -jnp.inf)
            weights = jnp.exp(scores - jnp.max(scores, axis=-1, keepdims=True))
            weight_sum = jnp.sum(weights, axis=-1)
            mixed_vals = jnp.einsum('kgt,tkd->kgd', weights.astype(jnp.bfloat16).astype(jnp.float32), cache_v.astype(jnp.float32))
            attended = (mixed_vals / weight_sum[..., None]).astype(jnp.bfloat16).reshape(HEADS * HEAD)
            return (cache_k, cache_v), attended

        (final_k, final_v), step_outs = lax.scan(one_step, (row_kc, row_vc), (row_q, row_k, row_v, row_pos + jnp.arange(STEPS)))
        return step_outs, final_k, final_v

    row_outs, k_out, v_out = lax.map(one_row, (jnp.swapaxes(queries, 0, 1), jnp.swapaxes(keys_new, 0, 1), jnp.swapaxes(values_new, 0, 1), k_cache, v_cache, start_pos))
    attended = jnp.swapaxes(row_outs, 0, 1).reshape(STEPS * BATCH, HEADS * HEAD)
    attn_out = jnp.dot(attended, w_o, preferred_element_type=jnp.float32).reshape(STEPS, BATCH, D)
    residual = (hidden_in.astype(jnp.float32) + attn_out).astype(jnp.bfloat16)
    normed = rms_norm(residual, mlp_norm).astype(jnp.bfloat16).reshape(STEPS * BATCH, D)
    gate_val = jnp.dot(normed, w_gate, preferred_element_type=jnp.float32)
    up_val = jnp.dot(normed, w_up, preferred_element_type=jnp.float32)
    activated = (jax.nn.silu(gate_val) * up_val).astype(jnp.bfloat16)
    down_val = jnp.dot(activated, w_down, preferred_element_type=jnp.float32).reshape(STEPS, BATCH, D)
    out_hidden = (residual.astype(jnp.float32) + down_val).astype(jnp.bfloat16)
    return (out_hidden, k_out, v_out)
```

```python
import functools

import jax
import jax.numpy as jnp
import numpy as np
from jax import lax
from jax.experimental import pallas as pl
from jax.experimental.pallas import tpu as pltpu
from jax.sharding import PartitionSpec as P

EPS = 1e-6
THETA = 1000000.0
F32 = jnp.float32
BF16 = jnp.bfloat16
MESH = pl.DeviceIdType.MESH
TILE = 512
SETS = (1, 1)


def rms(values, gain):
    inv_rms = lax.rsqrt(jnp.mean(values * values, axis=-1, keepdims=True) + EPS)
    return values * inv_rms * gain


def layer_kernel(
    n, steps, rows, heads, hd,
    pos_ref, freq_ref, hid_ref, k_hbm, v_hbm, an_ref, wq_hbm, wk_hbm, wv_hbm, qn_ref, kn_ref, wo_hbm, mn_ref,
    wg_hbm, wu_hbm, wd_hbm,
    out_ref, knew_ref, vnew_ref, rk_hbm, rv_hbm,
    hid_s, act_s, x1_s, acc_s, tmp_s, cs_s, sn_s, msg_s, msg_r, o_s, o_r, kbuf, vbuf, wbuf, ubuf, dbuf,
    wsem, usem, dsem, ksem, vsem, own_sem, msg_ss, msg_rs, o_ss, o_rs, bulk_s, bulk_r,
):
    me = lax.axis_index("x")
    num = steps * rows
    q_per = heads // n
    q_rows = q_per * num
    barrier = pltpu.get_barrier_semaphore()

    def peer(o):
        return lax.rem(me + o, n)

    for o in range(1, n):
        pl.semaphore_signal(barrier, inc=1, device_id={"x": peer(o)}, device_id_type=MESH)
    pl.semaphore_wait(barrier, n - 1)

    part = rows // 4
    rounds = 2 * (rows // part)
    order = (2, 6, 4, 3, 7, 5, 1) if n == 8 else tuple(range(1, n))

    def send_round(src, dst, which, first):
        for o in order:
            to = peer(o)
            pltpu.make_async_remote_copy(
                src_ref=src.at[pl.ds(to * rows + first, part)],
                dst_ref=dst.at[me, pl.ds(first, part)],
                send_sem=bulk_s.at[which], recv_sem=bulk_r.at[which], device_id={"x": to}, device_id_type=MESH,
            ).start()

    def bulk(lo, hi):
        def go(src, dst, which, a, b):
            if b > a:
                @pl.loop(a, b)
                def _(r):
                    send_round(src, dst, which, r * part)
        half = rounds // 2
        go(k_hbm, rk_hbm, 0, min(lo, half), min(hi, half))
        go(v_hbm, rv_hbm, 1, max(lo, half) - half, max(hi, half) - half)

    bulk(0, SETS[0])

    def cols(hbm, i):
        return hbm.at[:, pl.ds(pl.multiple_of(i * TILE, TILE), TILE)]

    def load(src, dst, sem, slot):
        return pltpu.make_async_copy(src, dst.at[slot], sem.at[slot])

    def stream(hbm, body):
        tiles = hbm.shape[1] // TILE
        load(cols(hbm, 0), wbuf, wsem, 0).start()

        @pl.loop(0, tiles)
        def _(i):
            slot = lax.rem(i, 2)

            @pl.when(i + 1 < tiles)
            def _():
                load(cols(hbm, i + 1), wbuf, wsem, 1 - slot).start()

            load(cols(hbm, i), wbuf, wsem, slot).wait()
            body(i, wbuf[slot])

    dim = hid_ref.shape[2]
    for c in range(0, dim, hd):
        for s in range(steps):
            tmp_s[pl.ds(s, rows, stride=steps), :] = hid_ref[s, :, c : c + hd].astype(F32)
        hid_s[:, c : c + hd] = tmp_s[...]
    act_s[...] = rms(hid_s[...], an_ref[...].astype(F32)).astype(BF16)

    row = lax.broadcasted_iota(jnp.int32, (num, hd), 0)
    pos = jnp.zeros((num, hd), jnp.int32)
    for b in range(rows):
        pos = jnp.where(row // steps == b, pos_ref[me * rows + b], pos)
    angles = (pos + row % steps).astype(F32) * freq_ref[...]
    lane = lax.broadcasted_iota(jnp.int32, (num, hd), 1)
    cs_s[...] = jnp.cos(angles)
    sn_s[...] = jnp.where(lane < hd // 2, -jnp.sin(angles), jnp.sin(angles))

    def rotate(v):
        return v * cs_s[...] + pltpu.roll(v, hd // 2, 1) * sn_s[...]

    per_tile = TILE // hd

    def q_tile(i, w):
        y = jnp.dot(act_s[...], w, preferred_element_type=F32)
        gain = qn_ref[...].astype(F32)
        for g in range(per_tile // q_per):
            pair = []
            for j in range(q_per):
                c = (g * q_per + j) * hd
                head = rotate(rms(y[:, c : c + hd], gain))
                pair.append(head.reshape(num // 8, 8, hd))
            both = jnp.concatenate(pair, axis=1).reshape(q_rows, hd)
            msg_s[i * (per_tile // q_per) + g, 0:q_rows, :] = both.astype(BF16)

    def k_tile(i, w):
        y = jnp.dot(act_s[...], w, preferred_element_type=F32)
        gain = kn_ref[...].astype(F32)
        for g in range(per_tile):
            head = rotate(rms(y[:, g * hd : (g + 1) * hd], gain)).astype(BF16)
            msg_s[i * per_tile + g, q_rows : q_rows + num, :] = head

    def v_tile(i, w):
        y = jnp.dot(act_s[...], w, preferred_element_type=F32).astype(BF16)
        for g in range(per_tile):
            msg_s[i * per_tile + g, q_rows + num : q_rows + 2 * num, :] = y[:, g * hd : (g + 1) * hd]

    stream(wq_hbm, q_tile)
    stream(wk_hbm, k_tile)
    stream(wv_hbm, v_tile)

    def msg_copy(to):
        return pltpu.make_async_remote_copy(
            src_ref=msg_s.at[to], dst_ref=msg_r.at[me], send_sem=msg_ss.at[to], recv_sem=msg_rs.at[me],
            device_id={"x": to}, device_id_type=MESH,
        )

    def msg_arrival(source):
        return pltpu.make_async_remote_copy(
            src_ref=msg_s.at[source], dst_ref=msg_r.at[source], send_sem=msg_ss.at[source], recv_sem=msg_rs.at[source],
            device_id={"x": source}, device_id_type=MESH,
        )

    def o_copy(to):
        return pltpu.make_async_remote_copy(
            src_ref=o_s.at[to], dst_ref=o_r.at[me], send_sem=o_ss.at[to], recv_sem=o_rs.at[me],
            device_id={"x": to}, device_id_type=MESH,
        )

    def o_arrival(source):
        return pltpu.make_async_remote_copy(
            src_ref=o_s.at[source], dst_ref=o_r.at[source], send_sem=o_ss.at[source], recv_sem=o_rs.at[source],
            device_id={"x": source}, device_id_type=MESH,
        )

    def kv_load(o, slot):
        first = peer(o) * rows
        return (
            pltpu.make_async_copy(k_hbm.at[pl.ds(first, rows)], kbuf.at[slot], ksem.at[slot]),
            pltpu.make_async_copy(v_hbm.at[pl.ds(first, rows)], vbuf.at[slot], vsem.at[slot]),
        )

    for c in kv_load(0, 0):
        c.start()
    for o in range(1, n):
        msg_copy(peer(o)).start()
    bulk(SETS[0], SETS[0] + SETS[1])
    msg_r[me] = msg_s[me]
    for h in range(n):
        knew_ref[:, h * hd : (h + 1) * hd] = msg_s[h, q_rows : q_rows + num, :]
        vnew_ref[:, h * hd : (h + 1) * hd] = msg_s[h, q_rows + num : q_rows + 2 * num, :]

    slots = k_hbm.shape[1]
    scale = hd ** -0.5
    tall = 8 * q_per
    nt = (((1,), (1,)), ((), ()))
    own = [
        pltpu.make_async_copy(kbuf.at[0], rk_hbm.at[me], own_sem.at[0]),
        pltpu.make_async_copy(vbuf.at[0], rv_hbm.at[me], own_sem.at[1]),
    ]

    @pl.loop(0, n)
    def _(o):
        slot = lax.rem(o, 2)
        source = peer(o)

        @pl.when(o == 1)
        def _():
            for c in own:
                c.wait()

        @pl.when(o + 1 < n)
        def _():
            for c in kv_load(o + 1, 1 - slot):
                c.start()

        for c in kv_load(o, slot):
            c.wait()

        @pl.when(o == 0)
        def _():
            for c in own:
                c.start()

        @pl.when(o > 0)
        def _():
            msg_arrival(source).wait_recv()

        k_new = msg_r[source, q_rows : q_rows + num, :]
        v_new = msg_r[source, q_rows + num : q_rows + 2 * num, :]
        fresh = lax.dot_general(msg_r[source, 0:q_rows, :], k_new, nt, preferred_element_type=F32) * scale
        r = lax.broadcasted_iota(jnp.int32, (q_rows, num), 0)
        c = lax.broadcasted_iota(jnp.int32, (q_rows, num), 1)
        seq = (r // tall) * (8 // steps) + (r % 8) // steps
        fresh = jnp.where((c // steps == seq) & (c % steps <= r % steps), fresh, -jnp.inf)
        in_pair = (lax.broadcasted_iota(jnp.int32, (tall, slots), 0) % 8) // steps
        in_pair_o = (lax.broadcasted_iota(jnp.int32, (tall, hd), 0) % 8) // steps
        t = lax.broadcasted_iota(jnp.int32, (tall, slots), 1)
        for i in range(q_rows // tall):
            q = msg_r[source, i * tall : (i + 1) * tall, :]
            b = i * (8 // steps)
            old = lax.dot_general(q, kbuf[slot, b], nt, preferred_element_type=F32)
            start = jnp.full((tall, slots), pos_ref[source * rows + b], jnp.int32)
            for e in range(1, 8 // steps):
                other = lax.dot_general(q, kbuf[slot, b + e], nt, preferred_element_type=F32)
                old = jnp.where(in_pair == e, other, old)
                start = jnp.where(in_pair == e, pos_ref[source * rows + b + e], start)
            old = jnp.where(t < start, old * scale, -jnp.inf)
            new = fresh[i * tall : (i + 1) * tall, :]
            peak = jnp.maximum(jnp.max(old, axis=-1, keepdims=True), jnp.max(new, axis=-1, keepdims=True))
            old = jnp.exp(old - peak)
            new = jnp.exp(new - peak)
            total = jnp.sum(old, axis=-1, keepdims=True) + jnp.sum(new, axis=-1, keepdims=True)
            weights = old.astype(BF16)
            mixed = jnp.dot(weights, vbuf[slot, b], preferred_element_type=F32)
            for e in range(1, 8 // steps):
                other = jnp.dot(weights, vbuf[slot, b + e], preferred_element_type=F32)
                mixed = jnp.where(in_pair_o == e, other, mixed)
            mixed = mixed + jnp.dot(new.astype(BF16), v_new, preferred_element_type=F32)
            o_s[source, i * tall : (i + 1) * tall, :] = (mixed / total).astype(BF16)

        @pl.when(o == 0)
        def _():
            o_r[me] = o_s[me]

        @pl.when(o > 0)
        def _():
            o_copy(source).start()

    bulk(SETS[0] + SETS[1], rounds)

    for o in range(1, n):
        o_arrival(peer(o)).wait_recv()
    for h in range(n):
        both = o_r[h].astype(F32).reshape(num // 8, tall, hd)
        for j in range(q_per):
            head = both[:, j * 8 : (j + 1) * 8, :].reshape(num, hd)
            act_s[:, (h * q_per + j) * hd : (h * q_per + j + 1) * hd] = head.astype(BF16)

    def wo_tile(i, w):
        at = pl.ds(pl.multiple_of(i * TILE, TILE), TILE)
        y = jnp.dot(act_s[...], w, preferred_element_type=F32)
        x1_s[:, at] = (hid_s[:, at] + y).astype(BF16).astype(F32)

    stream(wo_hbm, wo_tile)
    act_s[...] = rms(x1_s[...], mn_ref[...].astype(F32)).astype(BF16)
    acc_s[...] = jnp.zeros_like(acc_s)
    tiles = wg_hbm.shape[1] // TILE

    def mlp_loads(i, slot):
        at = pl.ds(pl.multiple_of(i * TILE, TILE), TILE)
        return (
            load(cols(wg_hbm, i), wbuf, wsem, slot),
            load(cols(wu_hbm, i), ubuf, usem, slot),
            load(wd_hbm.at[at, :], dbuf, dsem, slot),
        )

    for c in mlp_loads(0, 0):
        c.start()

    @pl.loop(0, tiles)
    def _(i):
        slot = lax.rem(i, 2)

        @pl.when(i + 1 < tiles)
        def _():
            for c in mlp_loads(i + 1, 1 - slot):
                c.start()

        for c in mlp_loads(i, slot):
            c.wait()
        z = act_s[...]
        gate = jnp.dot(z, wbuf[slot], preferred_element_type=F32)
        up = jnp.dot(z, ubuf[slot], preferred_element_type=F32)
        g = (jax.nn.silu(gate) * up).astype(BF16)
        acc_s[...] += jnp.dot(g, dbuf[slot], preferred_element_type=F32)

    for c in range(0, dim, hd):
        tmp_s[...] = x1_s[:, c : c + hd] + acc_s[:, c : c + hd]
        for s in range(steps):
            out_ref[s, :, c : c + hd] = tmp_s[pl.ds(s, rows, stride=steps), :].astype(BF16)

    for o in range(1, n):
        msg_copy(peer(o)).wait_send()
        o_copy(peer(o)).wait_send()
    for which, dst in enumerate((rk_hbm, rv_hbm)):
        whole = dst.at[pl.ds(0, n - 1)]
        pltpu.make_async_copy(whole, whole, bulk_s.at[which]).wait()
        pltpu.make_async_copy(whole, whole, bulk_r.at[which]).wait()


def place_kernel(steps, pos_ref, rk_ref, rv_ref, kn_ref, vn_ref, ko_ref, vo_ref, scr):
    b = pl.program_id(0)
    n, hd = rk_ref.shape[0], rk_ref.shape[-1]
    slots = rk_ref.shape[2]
    for src, new, dst in ((rk_ref, kn_ref, ko_ref), (rv_ref, vn_ref, vo_ref)):
        for h in range(n):
            scr[pl.ds(h, slots, stride=n), :] = src[h, 0].astype(F32)
        dst[0] = scr[...].reshape(slots, n, hd).astype(BF16)
        for s in range(steps):
            dst[0, pos_ref[b] + s] = new[b * steps + s]


def solution(mesh):
    row_spec = P(None, ("dp", "x"), None)
    cache_in = P("dp", None, "x", None)
    cache_out = P(("dp", "x"), None, None, None)
    n = mesh.shape["x"]

    def local_run(start_pos, hidden_in, k_heads, v_heads, attn_norm, w_q, w_k, w_v, q_norm, k_norm, w_o, mlp_norm, w_gate, w_up, w_down):
        steps, rows, dim = hidden_in.shape
        slots, hd = k_heads.shape[1], k_heads.shape[3]
        heads = w_q.shape[1] // hd
        num = steps * rows
        half = hd // 2
        inv_freq = np.power(np.float32(THETA), -np.arange(half, dtype=np.float32) * np.float32(2.0) / np.float32(hd))
        freq = jnp.asarray(np.concatenate([inv_freq, inv_freq])[None, :], F32)
        vmem = pl.BlockSpec(memory_space=pltpu.VMEM)
        hbm = pl.BlockSpec(memory_space=pltpu.HBM)
        smem = pl.BlockSpec(memory_space=pltpu.SMEM)
        q_rows = (heads // n) * num
        dma = pltpu.SemaphoreType.DMA
        blocks = jax.ShapeDtypeStruct((n, rows, slots, hd), BF16)
        fresh = jax.ShapeDtypeStruct((num, n * hd), BF16)
        out, k_new, v_new, rk, rv = pl.pallas_call(
            functools.partial(layer_kernel, n, steps, rows, heads, hd),
            name="layer",
            out_shape=(jax.ShapeDtypeStruct(hidden_in.shape, BF16), fresh, fresh, blocks, blocks),
            in_specs=[smem, vmem, vmem, hbm, hbm, vmem, hbm, hbm, hbm, vmem, vmem, hbm, vmem, hbm, hbm, hbm],
            out_specs=(vmem, vmem, vmem, hbm, hbm),
            scratch_shapes=[
                pltpu.VMEM((num, dim), F32), pltpu.VMEM((num, dim), BF16), pltpu.VMEM((num, dim), F32), pltpu.VMEM((num, dim), F32),
                pltpu.VMEM((num, hd), F32), pltpu.VMEM((num, hd), F32), pltpu.VMEM((num, hd), F32),
                pltpu.VMEM((n, q_rows + 2 * num, hd), BF16), pltpu.VMEM((n, q_rows + 2 * num, hd), BF16),
                pltpu.VMEM((n, q_rows, hd), BF16), pltpu.VMEM((n, q_rows, hd), BF16),
                pltpu.VMEM((2, rows, slots, hd), BF16), pltpu.VMEM((2, rows, slots, hd), BF16),
                pltpu.VMEM((2, dim, TILE), BF16), pltpu.VMEM((2, dim, TILE), BF16), pltpu.VMEM((2, TILE, dim), BF16),
                dma((2,)), dma((2,)), dma((2,)), dma((2,)), dma((2,)), dma((2,)),
                dma((n,)), dma((n,)), dma((n,)), dma((n,)), dma((2,)), dma((2,)),
            ],
            compiler_params=pltpu.CompilerParams(collective_id=0, has_side_effects=True, vmem_limit_bytes=60 * 2**20),
        )(
            start_pos, freq, hidden_in, k_heads.reshape(-1, slots, hd), v_heads.reshape(-1, slots, hd), attn_norm.reshape(1, -1),
            w_q, w_k, w_v, q_norm.reshape(1, -1), k_norm.reshape(1, -1), w_o, mlp_norm.reshape(1, -1), w_gate, w_up, w_down,
        )
        my_pos = lax.dynamic_slice_in_dim(start_pos, lax.axis_index("x") * rows, rows)
        in_block = pl.BlockSpec((n, 1, slots, hd), lambda b: (0, b, 0, 0))
        out_block = pl.BlockSpec((1, slots, n, hd), lambda b: (b, 0, 0, 0))
        new_block = pl.BlockSpec((num, n, hd), lambda b: (0, 0, 0))
        cache = jax.ShapeDtypeStruct((rows, slots, n, hd), BF16)
        k_out, v_out = pl.pallas_call(
            functools.partial(place_kernel, steps),
            name="place",
            grid=(rows,),
            out_shape=(cache, cache),
            in_specs=[smem, in_block, in_block, new_block, new_block],
            out_specs=(out_block, out_block),
            scratch_shapes=[pltpu.VMEM((slots * n, hd), F32)],
            compiler_params=pltpu.CompilerParams(dimension_semantics=("arbitrary",), vmem_limit_bytes=60 * 2**20),
        )(my_pos, rk, rv, k_new.reshape(num, n, hd), v_new.reshape(num, n, hd))
        return out, k_out, v_out

    return jax.shard_map(local_run, mesh=mesh, in_specs=(P("dp"), row_spec, cache_in, cache_in) + (P(),) * 11, out_specs=(row_spec, cache_out, cache_out), check_vma=False)
```

```python
import functools

import jax
import jax.numpy as jnp
import numpy as np
from jax import lax
from jax.experimental import pallas as pl
from jax.experimental.pallas import tpu as pltpu
from jax.sharding import PartitionSpec as P

EPS = 1e-6
THETA = 1000000.0
F32 = jnp.float32
BF16 = jnp.bfloat16
MESH = pl.DeviceIdType.MESH
TILE = 512
PAIR = 2
AWAY = 3
VMEM_LIMIT = 44 * 2**20
AHEAD = 4


def rms(values, gain):
    inv_rms = lax.rsqrt(jnp.mean(values * values, axis=-1, keepdims=True) + EPS)
    return values * inv_rms * gain


def layer_kernel(
    n, steps, rows, heads, hd,
    pos_ref, freq_ref, hid_ref, k_hbm, v_hbm, an_ref, wq_hbm, wk_hbm, wv_hbm, qn_ref, kn_ref, wo_hbm, mn_ref,
    wg_hbm, wu_hbm, wd_hbm,
    out_ref, knew_ref, vnew_ref, ka_ref, va_ref,
    hid_s, act_s, x1_s, acc_s, tmp_s, cs_s, sn_s, msg_s, msg_r, o_s, o_r, rk, rv, kbuf, vbuf, wbuf, ubuf, dbuf, mix_s, kmix_s, vmix_s,
    wsem, usem, dsem, ksem, vsem, own_sem, msg_ss, msg_rs, o_ss, o_rs, bulk_s, krs, vrs,
):
    me = lax.axis_index("x")
    num = steps * rows
    q_per = heads // n
    pairs = rows // PAIR
    home = pairs - AWAY
    slots = k_hbm.shape[1]
    dim = hid_ref.shape[2]
    tall = PAIR * steps * q_per
    new = PAIR * steps
    barrier = pltpu.get_barrier_semaphore()

    def peer(o):
        return lax.rem(me + o, n)

    for o in range(1, n):
        pl.semaphore_signal(barrier, inc=1, device_id={"x": peer(o)}, device_id_type=MESH)
    pl.semaphore_wait(barrier, n - 1)

    order = (2, 6, 4, 3, 7, 5, 1) if n == 8 else tuple(range(1, n))

    def bulk(r):
        for which, (src, dst, arrived) in enumerate(((k_hbm, rk, krs), (v_hbm, rv, vrs))):
            for o in order:
                to = peer(o)
                pltpu.make_async_remote_copy(
                    src_ref=src.at[pl.ds(to * rows + r * PAIR, PAIR)],
                    dst_ref=dst.at[me, pl.ds(r * PAIR, PAIR)],
                    send_sem=bulk_s.at[which], recv_sem=arrived.at[r], device_id={"x": to}, device_id_type=MESH,
                ).start()

    def bulk_wait(r):
        for dst, arrived in ((rk, krs), (rv, vrs)):
            whole = dst.at[pl.ds(0, n - 1), pl.ds(0, PAIR)]
            pltpu.make_async_copy(whole, whole, arrived.at[r]).wait()

    for r in range(2):
        bulk(r)

    own = [
        pltpu.make_async_copy(k_hbm.at[pl.ds(me * rows, rows)], rk.at[me], own_sem.at[0]),
        pltpu.make_async_copy(v_hbm.at[pl.ds(me * rows, rows)], rv.at[me], own_sem.at[1]),
    ]

    def cols(hbm, i):
        return hbm.at[:, pl.ds(pl.multiple_of(i * TILE, TILE), TILE)]

    def load(src, dst, sem, slot):
        return pltpu.make_async_copy(src, dst.at[slot], sem.at[slot])

    def stream(hbm, body):
        tiles = hbm.shape[1] // TILE
        load(cols(hbm, 0), wbuf, wsem, 0).start()

        @pl.loop(0, tiles)
        def _(i):
            slot = lax.rem(i, 2)

            @pl.when(i + 1 < tiles)
            def _():
                load(cols(hbm, i + 1), wbuf, wsem, 1 - slot).start()

            load(cols(hbm, i), wbuf, wsem, slot).wait()
            body(i, wbuf[slot])

    for c in range(0, dim, hd):
        for s in range(steps):
            tmp_s[pl.ds(s, rows, stride=steps), :] = hid_ref[s, :, c : c + hd].astype(F32)
        hid_s[:, c : c + hd] = tmp_s[...]
    act_s[...] = rms(hid_s[...], an_ref[...].astype(F32).reshape(1, dim)).astype(BF16)

    row = lax.broadcasted_iota(jnp.int32, (num, hd), 0)
    pos = jnp.zeros((num, hd), jnp.int32)
    for b in range(rows):
        pos = jnp.where(row // steps == b, pos_ref[me * rows + b], pos)
    angles = (pos + row % steps).astype(F32) * freq_ref[...]
    lane = lax.broadcasted_iota(jnp.int32, (num, hd), 1)
    cs_s[...] = jnp.cos(angles)
    sn_s[...] = jnp.where(lane < hd // 2, -jnp.sin(angles), jnp.sin(angles))

    def rotate(v):
        return v * cs_s[...] + pltpu.roll(v, hd // 2, 1) * sn_s[...]

    per_tile = TILE // hd

    def q_tile(i, w):
        y = jnp.dot(act_s[...], w, preferred_element_type=F32)
        gain = qn_ref[...].astype(F32)
        for g in range(per_tile // q_per):
            parts = []
            for j in range(q_per):
                c = (g * q_per + j) * hd
                head = rotate(rms(y[:, c : c + hd], gain))
                parts.append(head.reshape(pairs, new, hd))
            msg_s[i * (per_tile // q_per) + g, :, 0:tall, :] = jnp.concatenate(parts, axis=1).astype(BF16)

    def k_tile(i, w):
        y = jnp.dot(act_s[...], w, preferred_element_type=F32)
        gain = kn_ref[...].astype(F32)
        for g in range(per_tile):
            head = rotate(rms(y[:, g * hd : (g + 1) * hd], gain))
            msg_s[i * per_tile + g, :, tall : tall + new, :] = head.reshape(pairs, new, hd).astype(BF16)
            kmix_s[pl.ds(i * per_tile + g, num, stride=n), :] = head

    def v_tile(i, w):
        y = jnp.dot(act_s[...], w, preferred_element_type=F32)
        for g in range(per_tile):
            head = y[:, g * hd : (g + 1) * hd]
            msg_s[i * per_tile + g, :, tall + new : tall + 2 * new, :] = head.reshape(pairs, new, hd).astype(BF16)
            vmix_s[pl.ds(i * per_tile + g, num, stride=n), :] = head

    stream(wq_hbm, q_tile)
    stream(wk_hbm, k_tile)
    stream(wv_hbm, v_tile)

    def msg_copy(to):
        return pltpu.make_async_remote_copy(
            src_ref=msg_s.at[to, pl.ds(home, AWAY)], dst_ref=msg_r.at[me], send_sem=msg_ss.at[to], recv_sem=msg_rs.at[me],
            device_id={"x": to}, device_id_type=MESH,
        )

    def msg_arrival(source):
        return pltpu.make_async_remote_copy(
            src_ref=msg_s.at[source, pl.ds(home, AWAY)], dst_ref=msg_r.at[source], send_sem=msg_ss.at[source],
            recv_sem=msg_rs.at[source], device_id={"x": source}, device_id_type=MESH,
        )

    def o_copy(to):
        return pltpu.make_async_remote_copy(
            src_ref=o_s.at[to], dst_ref=o_r.at[me, pl.ds(home, AWAY)], send_sem=o_ss.at[to], recv_sem=o_rs.at[me],
            device_id={"x": to}, device_id_type=MESH,
        )

    def o_arrival(source):
        return pltpu.make_async_remote_copy(
            src_ref=o_s.at[source], dst_ref=o_r.at[source, pl.ds(home, AWAY)], send_sem=o_ss.at[source], recv_sem=o_rs.at[source],
            device_id={"x": source}, device_id_type=MESH,
        )

    def kv_load(o, slot):
        first = peer(o) * rows + home * PAIR
        return (
            pltpu.make_async_copy(k_hbm.at[pl.ds(first, AWAY * PAIR)], kbuf.at[slot], ksem.at[slot]),
            pltpu.make_async_copy(v_hbm.at[pl.ds(first, AWAY * PAIR)], vbuf.at[slot], vsem.at[slot]),
        )

    for c in kv_load(0, 0):
        c.start()
    for c in own:
        c.start()
    for o in range(1, n):
        msg_copy(peer(o)).start()
    for r in range(2, AHEAD):
        bulk(r)
    msg_r[me] = msg_s[me, home:pairs]
    knew_ref[...] = kmix_s[...].reshape(rows, steps, n, hd).astype(BF16)
    vnew_ref[...] = vmix_s[...].reshape(rows, steps, n, hd).astype(BF16)

    scale = hd ** -0.5
    nt = (((1,), (1,)), ((), ()))
    r_new = lax.broadcasted_iota(jnp.int32, (tall, new), 0) % new
    c_new = lax.broadcasted_iota(jnp.int32, (tall, new), 1)
    new_ok = (c_new // steps == r_new // steps) & (c_new % steps <= r_new % steps)
    in_pair = (lax.broadcasted_iota(jnp.int32, (tall, slots), 0) % new) // steps
    in_pair_o = (lax.broadcasted_iota(jnp.int32, (tall, hd), 0) % new) // steps
    t = lax.broadcasted_iota(jnp.int32, (tall, slots), 1)

    def attend(msg, keys, values, first):
        q = msg[0:tall]
        v_new = msg[tall + new : tall + 2 * new]
        fresh = lax.dot_general(q, msg[tall : tall + new], nt, preferred_element_type=F32)
        fresh = jnp.where(new_ok, fresh * scale, -jnp.inf)
        old = lax.dot_general(q, keys(0), nt, preferred_element_type=F32)
        start = jnp.full((tall, slots), pos_ref[first], jnp.int32)
        for e in range(1, PAIR):
            other = lax.dot_general(q, keys(e), nt, preferred_element_type=F32)
            old = jnp.where(in_pair == e, other, old)
            start = jnp.where(in_pair == e, pos_ref[first + e], start)
        old = jnp.where(t < start, old * scale, -jnp.inf)
        peak = jnp.maximum(jnp.max(old, axis=-1, keepdims=True), jnp.max(fresh, axis=-1, keepdims=True))
        old = jnp.exp(old - peak)
        fresh = jnp.exp(fresh - peak)
        total = jnp.sum(old, axis=-1, keepdims=True) + jnp.sum(fresh, axis=-1, keepdims=True)
        weights = old.astype(BF16)
        mixed = jnp.dot(weights, values(0), preferred_element_type=F32)
        for e in range(1, PAIR):
            other = jnp.dot(weights, values(e), preferred_element_type=F32)
            mixed = jnp.where(in_pair_o == e, other, mixed)
        mixed = mixed + jnp.dot(fresh.astype(BF16), v_new, preferred_element_type=F32)
        return (mixed / total).astype(BF16)

    @pl.loop(0, n)
    def _(o):
        slot = lax.rem(o, 2)
        source = peer(o)

        @pl.when(o + 1 < n)
        def _():
            for c in kv_load(o + 1, 1 - slot):
                c.start()

        for c in kv_load(o, slot):
            c.wait()

        @pl.when(o > 0)
        def _():
            msg_arrival(source).wait_recv()

        for i in range(AWAY):
            o_s[source, i] = attend(
                msg_r[source, i], lambda e: kbuf[slot, i * PAIR + e], lambda e: vbuf[slot, i * PAIR + e],
                source * rows + (home + i) * PAIR,
            )

        @pl.when(o == 0)
        def _():
            o_r[me, home:pairs] = o_s[me]

        @pl.when(o > 0)
        def _():
            o_copy(source).start()

    for c in own:
        c.wait()

    def place(r):
        for src, dst in ((rk, ka_ref), (rv, va_ref)):
            @pl.loop(0, PAIR)
            def _(e):
                for h in range(n):
                    mix_s[pl.ds(h, slots, stride=n), :] = src[h, r * PAIR + e].astype(F32)
                dst[r * PAIR + e] = mix_s[...].reshape(slots, n, hd).astype(BF16)

    @pl.loop(0, home)
    def _(r):
        bulk_wait(r)

        @pl.when(r + AHEAD < pairs)
        def _():
            bulk(r + AHEAD)

        place(r)

        @pl.loop(0, n)
        def _(h):
            o_r[h, r] = attend(
                msg_s[h, r], lambda e: rk[h, r * PAIR + e], lambda e: rv[h, r * PAIR + e], me * rows + r * PAIR
            )

    for r in range(home + AHEAD, pairs):
        bulk(r)
    for o in range(1, n):
        o_arrival(peer(o)).wait_recv()
    for h in range(n):
        both = o_r[h].astype(F32)
        for j in range(q_per):
            head = both[:, j * new : (j + 1) * new, :].reshape(num, hd)
            act_s[:, (h * q_per + j) * hd : (h * q_per + j + 1) * hd] = head.astype(BF16)

    def wo_tile(i, w):
        at = pl.ds(pl.multiple_of(i * TILE, TILE), TILE)
        y = jnp.dot(act_s[...], w, preferred_element_type=F32)
        x1_s[:, at] = (hid_s[:, at] + y).astype(BF16).astype(F32)

    stream(wo_hbm, wo_tile)
    act_s[...] = rms(x1_s[...], mn_ref[...].astype(F32).reshape(1, dim)).astype(BF16)
    acc_s[...] = jnp.zeros_like(acc_s)
    tiles = wg_hbm.shape[1] // TILE

    def mlp_loads(i, slot):
        at = pl.ds(pl.multiple_of(i * TILE, TILE), TILE)
        return (
            load(cols(wg_hbm, i), wbuf, wsem, slot),
            load(cols(wu_hbm, i), ubuf, usem, slot),
            load(wd_hbm.at[at, :], dbuf, dsem, slot),
        )

    for c in mlp_loads(0, 0):
        c.start()

    @pl.loop(0, tiles)
    def _(i):
        slot = lax.rem(i, 2)

        @pl.when(i + 1 < tiles)
        def _():
            for c in mlp_loads(i + 1, 1 - slot):
                c.start()

        for c in mlp_loads(i, slot):
            c.wait()
        z = act_s[...]
        gate = jnp.dot(z, wbuf[slot], preferred_element_type=F32)
        up = jnp.dot(z, ubuf[slot], preferred_element_type=F32)
        g = (jax.nn.silu(gate) * up).astype(BF16)
        acc_s[...] += jnp.dot(g, dbuf[slot], preferred_element_type=F32)

    for c in range(0, dim, hd):
        tmp_s[...] = x1_s[:, c : c + hd] + acc_s[:, c : c + hd]
        for s in range(steps):
            out_ref[s, :, c : c + hd] = tmp_s[pl.ds(s, rows, stride=steps), :].astype(BF16)

    for o in range(1, n):
        msg_copy(peer(o)).wait_send()
        o_copy(peer(o)).wait_send()

    @pl.loop(home, pairs)
    def _(r):
        bulk_wait(r)
        place(r)

    for which, dst in enumerate((rk, rv)):
        whole = dst.at[pl.ds(0, n - 1)]
        pltpu.make_async_copy(whole, whole, bulk_s.at[which]).wait()


def store_kernel(pos_ref, hid_ref, ka_ref, va_ref, kn_ref, vn_ref, out_hbm, ko_hbm, vo_hbm, hid_sem, big, small):
    rows, steps = kn_ref.shape[0], kn_ref.shape[1]
    first = lax.axis_index("x") * rows
    sides = ((ka_ref, kn_ref, ko_hbm), (va_ref, vn_ref, vo_hbm))

    def whole(i, b):
        return pltpu.make_async_copy(sides[i][0].at[b], sides[i][2].at[b], big.at[i, b])

    def fresh(i, b):
        return pltpu.make_async_copy(sides[i][1].at[b], sides[i][2].at[b, pl.ds(pos_ref[first + b], steps)], small.at[i, b])

    hidden = pltpu.make_async_copy(hid_ref, out_hbm, hid_sem)
    for b in range(rows):
        for i in range(2):
            whole(i, b).start()
    hidden.start()
    for b in range(rows):
        for i in range(2):
            whole(i, b).wait()
            fresh(i, b).start()
    for b in range(rows):
        for i in range(2):
            fresh(i, b).wait()
    hidden.wait()


def solution(mesh):
    row_spec = P(None, ("dp", "x"), None)
    cache_in = P("dp", None, "x", None)
    cache_out = P(("dp", "x"), None, None, None)
    n = mesh.shape["x"]

    def local_run(start_pos, hidden_in, k_heads, v_heads, attn_norm, w_q, w_k, w_v, q_norm, k_norm, w_o, mlp_norm, w_gate, w_up, w_down):
        steps, rows, dim = hidden_in.shape
        slots, hd = k_heads.shape[1], k_heads.shape[3]
        heads = w_q.shape[1] // hd
        num = steps * rows
        pairs = rows // PAIR
        half = hd // 2
        inv_freq = np.power(np.float32(THETA), -np.arange(half, dtype=np.float32) * np.float32(2.0) / np.float32(hd))
        freq = jnp.asarray(np.concatenate([inv_freq, inv_freq])[None, :], F32)
        vmem = pl.BlockSpec(memory_space=pltpu.VMEM)
        hbm = pl.BlockSpec(memory_space=pltpu.HBM)
        smem = pl.BlockSpec(memory_space=pltpu.SMEM)
        tall, new = PAIR * steps * (heads // n), PAIR * steps
        dma = pltpu.SemaphoreType.DMA
        cache = (rows, slots, n, hd)
        fresh = (rows, steps, n, hd)
        blocks = pltpu.VMEM((n, rows, slots, hd), BF16)
        chunk = pltpu.VMEM((2, AWAY * PAIR, slots, hd), BF16)
        wide = pltpu.VMEM((num, dim), F32)
        head = pltpu.VMEM((num, hd), F32)
        arrived = [pltpu.VMEM(hidden_in.shape, BF16), pltpu.VMEM(fresh, BF16), pltpu.VMEM(fresh, BF16), pltpu.VMEM(cache, BF16), pltpu.VMEM(cache, BF16)]
        out, k_new, v_new, k_all, v_all = pl.pallas_call(
            functools.partial(layer_kernel, n, steps, rows, heads, hd),
            name="layer",
            out_shape=tuple(arrived),
            in_specs=[smem, vmem, vmem, hbm, hbm, vmem, hbm, hbm, hbm, vmem, vmem, hbm, vmem, hbm, hbm, hbm],
            out_specs=(vmem,) * 5,
            scratch_shapes=[
                wide, pltpu.VMEM((num, dim), BF16), wide, wide, head, head, head,
                pltpu.VMEM((n, pairs, tall + 2 * new, hd), BF16), pltpu.VMEM((n, AWAY, tall + 2 * new, hd), BF16),
                pltpu.VMEM((n, AWAY, tall, hd), BF16), pltpu.VMEM((n, pairs, tall, hd), BF16),
                blocks, blocks, chunk, chunk,
                pltpu.VMEM((2, dim, TILE), BF16), pltpu.VMEM((2, dim, TILE), BF16), pltpu.VMEM((2, TILE, dim), BF16),
                pltpu.VMEM((slots * n, hd), F32), pltpu.VMEM((num * n, hd), F32), pltpu.VMEM((num * n, hd), F32),
                dma((2,)), dma((2,)), dma((2,)), dma((2,)), dma((2,)), dma((2,)),
                dma((n,)), dma((n,)), dma((n,)), dma((n,)), dma((2,)), dma((pairs,)), dma((pairs,)),
            ],
            compiler_params=pltpu.CompilerParams(collective_id=0, has_side_effects=True, vmem_limit_bytes=VMEM_LIMIT),
        )(
            start_pos, freq, hidden_in, k_heads.reshape(-1, slots, hd), v_heads.reshape(-1, slots, hd), attn_norm,
            w_q, w_k, w_v, q_norm.reshape(1, -1), k_norm.reshape(1, -1), w_o, mlp_norm, w_gate, w_up, w_down,
        )
        return pl.pallas_call(
            store_kernel,
            name="store",
            out_shape=(jax.ShapeDtypeStruct(hidden_in.shape, BF16), jax.ShapeDtypeStruct(cache, BF16), jax.ShapeDtypeStruct(cache, BF16)),
            in_specs=[smem] + [vmem] * 5,
            out_specs=(hbm,) * 3,
            scratch_shapes=[dma, dma((2, rows)), dma((2, rows))],
            compiler_params=pltpu.CompilerParams(vmem_limit_bytes=2**20),
        )(start_pos, out, k_all, v_all, k_new, v_new)

    return jax.shard_map(local_run, mesh=mesh, in_specs=(P("dp"), row_spec, cache_in, cache_in) + (P(),) * 11, out_specs=(row_spec, cache_out, cache_out), check_vma=False)
```

```python
import functools

import jax
import jax.numpy as jnp
import numpy as np
from jax import lax
from jax.experimental import pallas as pl
from jax.experimental.pallas import tpu as pltpu
from jax.sharding import PartitionSpec as P

EPS = 1e-6
THETA = 1000000.0
F32 = jnp.float32
BF16 = jnp.bfloat16
MESH = pl.DeviceIdType.MESH
TILE = 512
PAIR = 2
AWAY = 3
VMEM_LIMIT = 44 * 2**20
AHEAD = 4


def rms(values, gain):
    inv_rms = lax.rsqrt(jnp.mean(values * values, axis=-1, keepdims=True) + EPS)
    return values * inv_rms * gain


def layer_kernel(
    n, steps, rows, heads, hd,
    pos_ref, freq_hbm, hid_hbm, k_hbm, v_hbm, an_hbm, wq_hbm, wk_hbm, wv_hbm, qn_hbm, kn_hbm, wo_hbm, mn_hbm,
    wg_hbm, wu_hbm, wd_hbm,
    out_ref, knew_ref, vnew_ref, ka_ref, va_ref,
    freq_ref, hid_ref, an_ref, qn_ref, kn_ref, mn_ref, hid_s, act_s, x1_s, acc_s, tmp_s, cs_s, sn_s, msg_s, msg_r, o_s, o_r, rk, rv, kbuf, vbuf, wbuf, ubuf, dbuf, mix_s, kmix_s, vmix_s,
    wsem, usem, dsem, ksem, vsem, own_sem, msg_ss, msg_rs, o_ss, o_rs, bulk_s, krs, vrs, in_sem,
):
    me = lax.axis_index("x")
    num = steps * rows
    q_per = heads // n
    pairs = rows // PAIR
    home = pairs - AWAY
    slots = k_hbm.shape[1]
    dim = hid_ref.shape[2]
    tall = PAIR * steps * q_per
    new = PAIR * steps
    barrier = pltpu.get_barrier_semaphore()

    def peer(o):
        return lax.rem(me + o, n)

    for o in range(1, n):
        pl.semaphore_signal(barrier, inc=1, device_id={"x": peer(o)}, device_id_type=MESH)

    small = [
        pltpu.make_async_copy(src, dst, in_sem.at[i])
        for i, (src, dst) in enumerate((
            (hid_hbm, hid_ref), (an_hbm, an_ref), (freq_hbm, freq_ref), (qn_hbm, qn_ref), (kn_hbm, kn_ref), (mn_hbm, mn_ref),
        ))
    ]
    for c in small:
        c.start()

    def cols(hbm, i):
        return hbm.at[:, pl.ds(pl.multiple_of(i * TILE, TILE), TILE)]

    def load(src, dst, sem, slot):
        return pltpu.make_async_copy(src, dst.at[slot], sem.at[slot])

    load(cols(wq_hbm, 0), wbuf, wsem, 0).start()
    pl.semaphore_wait(barrier, n - 1)

    order = (2, 6, 4, 3, 7, 5, 1) if n == 8 else tuple(range(1, n))

    def send(which, sem, first, count):
        for o in order:
            to = peer(o)
            pltpu.make_async_remote_copy(
                src_ref=(k_hbm, v_hbm)[which].at[pl.ds(to * rows + first, count)],
                dst_ref=(rk, rv)[which].at[me, pl.ds(first, count)],
                send_sem=bulk_s.at[which], recv_sem=(krs, vrs)[which].at[sem], device_id={"x": to}, device_id_type=MESH,
            ).start()

    def bulk(r):
        send(0, r, r * PAIR, PAIR)
        send(1, r, r * PAIR, PAIR)

    def bulk_last():
        send(0, pairs - 1, rows - PAIR, PAIR)
        for e in range(PAIR):
            send(1, pairs - 1 + e, rows - PAIR + e, 1)

    def bulk_next(r):
        @pl.when(r < pairs - 1)
        def _():
            bulk(r)

        @pl.when(r == pairs - 1)
        def _():
            bulk_last()

    def bulk_wait(which, r, count=PAIR):
        whole = (rk, rv)[which].at[pl.ds(0, n - 1), pl.ds(0, count)]
        pltpu.make_async_copy(whole, whole, (krs, vrs)[which].at[r]).wait()

    for r in range(2):
        bulk(r)

    own = [
        pltpu.make_async_copy(k_hbm.at[pl.ds(me * rows, rows)], rk.at[me], own_sem.at[0]),
        pltpu.make_async_copy(v_hbm.at[pl.ds(me * rows, rows)], rv.at[me], own_sem.at[1]),
    ]

    def stream(hbm, body, started=False):
        tiles = hbm.shape[1] // TILE
        if not started:
            load(cols(hbm, 0), wbuf, wsem, 0).start()

        @pl.loop(0, tiles)
        def _(i):
            slot = lax.rem(i, 2)

            @pl.when(i + 1 < tiles)
            def _():
                load(cols(hbm, i + 1), wbuf, wsem, 1 - slot).start()

            load(cols(hbm, i), wbuf, wsem, slot).wait()
            body(i, wbuf[slot])

    for c in small:
        c.wait()
    for c in range(0, dim, hd):
        for s in range(steps):
            tmp_s[pl.ds(s, rows, stride=steps), :] = hid_ref[s, :, c : c + hd].astype(F32)
        hid_s[:, c : c + hd] = tmp_s[...]
    act_s[...] = rms(hid_s[...], an_ref[...].astype(F32).reshape(1, dim)).astype(BF16)

    row = lax.broadcasted_iota(jnp.int32, (num, hd), 0)
    pos = jnp.zeros((num, hd), jnp.int32)
    for b in range(rows):
        pos = jnp.where(row // steps == b, pos_ref[me * rows + b], pos)
    angles = (pos + row % steps).astype(F32) * freq_ref[...]
    lane = lax.broadcasted_iota(jnp.int32, (num, hd), 1)
    cs_s[...] = jnp.cos(angles)
    sn_s[...] = jnp.where(lane < hd // 2, -jnp.sin(angles), jnp.sin(angles))

    def rotate(v):
        return v * cs_s[...] + pltpu.roll(v, hd // 2, 1) * sn_s[...]

    per_tile = TILE // hd

    def q_tile(i, w):
        y = jnp.dot(act_s[...], w, preferred_element_type=F32)
        gain = qn_ref[...].astype(F32)
        for g in range(per_tile // q_per):
            parts = []
            for j in range(q_per):
                c = (g * q_per + j) * hd
                head = rotate(rms(y[:, c : c + hd], gain))
                parts.append(head.reshape(pairs, new, hd))
            msg_s[i * (per_tile // q_per) + g, :, 0:tall, :] = jnp.concatenate(parts, axis=1).astype(BF16)

    def k_tile(i, w):
        y = jnp.dot(act_s[...], w, preferred_element_type=F32)
        gain = kn_ref[...].astype(F32)
        for g in range(per_tile):
            head = rotate(rms(y[:, g * hd : (g + 1) * hd], gain))
            msg_s[i * per_tile + g, :, tall : tall + new, :] = head.reshape(pairs, new, hd).astype(BF16)
            kmix_s[pl.ds(i * per_tile + g, num, stride=n), :] = head

    def v_tile(i, w):
        y = jnp.dot(act_s[...], w, preferred_element_type=F32)
        for g in range(per_tile):
            head = y[:, g * hd : (g + 1) * hd]
            msg_s[i * per_tile + g, :, tall + new : tall + 2 * new, :] = head.reshape(pairs, new, hd).astype(BF16)
            vmix_s[pl.ds(i * per_tile + g, num, stride=n), :] = head

    stream(wq_hbm, q_tile, started=True)
    stream(wk_hbm, k_tile)
    stream(wv_hbm, v_tile)

    def msg_copy(to):
        return pltpu.make_async_remote_copy(
            src_ref=msg_s.at[to, pl.ds(home, AWAY)], dst_ref=msg_r.at[me], send_sem=msg_ss.at[to], recv_sem=msg_rs.at[me],
            device_id={"x": to}, device_id_type=MESH,
        )

    def msg_arrival(source):
        return pltpu.make_async_remote_copy(
            src_ref=msg_s.at[source, pl.ds(home, AWAY)], dst_ref=msg_r.at[source], send_sem=msg_ss.at[source],
            recv_sem=msg_rs.at[source], device_id={"x": source}, device_id_type=MESH,
        )

    def o_copy(to):
        return pltpu.make_async_remote_copy(
            src_ref=o_s.at[to], dst_ref=o_r.at[me, pl.ds(home, AWAY)], send_sem=o_ss.at[to], recv_sem=o_rs.at[me],
            device_id={"x": to}, device_id_type=MESH,
        )

    def o_arrival(source):
        return pltpu.make_async_remote_copy(
            src_ref=o_s.at[source], dst_ref=o_r.at[source, pl.ds(home, AWAY)], send_sem=o_ss.at[source], recv_sem=o_rs.at[source],
            device_id={"x": source}, device_id_type=MESH,
        )

    def kv_load(o, slot):
        first = peer(o) * rows + home * PAIR
        return (
            pltpu.make_async_copy(k_hbm.at[pl.ds(first, AWAY * PAIR)], kbuf.at[slot], ksem.at[slot]),
            pltpu.make_async_copy(v_hbm.at[pl.ds(first, AWAY * PAIR)], vbuf.at[slot], vsem.at[slot]),
        )

    for c in kv_load(0, 0):
        c.start()
    for c in own:
        c.start()
    knew_ref[...] = kmix_s[...].reshape(rows, steps, n, hd).astype(BF16)
    vnew_ref[...] = vmix_s[...].reshape(rows, steps, n, hd).astype(BF16)
    msg_r[me] = msg_s[me, home:pairs]
    for o in range(1, n):
        msg_copy(peer(o)).start()
    for r in range(2, AHEAD):
        bulk(r)

    scale = hd ** -0.5
    nt = (((1,), (1,)), ((), ()))
    r_new = lax.broadcasted_iota(jnp.int32, (tall, new), 0) % new
    c_new = lax.broadcasted_iota(jnp.int32, (tall, new), 1)
    new_ok = (c_new // steps == r_new // steps) & (c_new % steps <= r_new % steps)
    in_pair = (lax.broadcasted_iota(jnp.int32, (tall, slots), 0) % new) // steps
    in_pair_o = (lax.broadcasted_iota(jnp.int32, (tall, hd), 0) % new) // steps
    t = lax.broadcasted_iota(jnp.int32, (tall, slots), 1)

    def attend(msg, keys, values, first):
        q = msg[0:tall]
        v_new = msg[tall + new : tall + 2 * new]
        fresh = lax.dot_general(q, msg[tall : tall + new], nt, preferred_element_type=F32)
        fresh = jnp.where(new_ok, fresh * scale, -jnp.inf)
        old = lax.dot_general(q, keys(0), nt, preferred_element_type=F32)
        start = jnp.full((tall, slots), pos_ref[first], jnp.int32)
        for e in range(1, PAIR):
            other = lax.dot_general(q, keys(e), nt, preferred_element_type=F32)
            old = jnp.where(in_pair == e, other, old)
            start = jnp.where(in_pair == e, pos_ref[first + e], start)
        old = jnp.where(t < start, old * scale, -jnp.inf)
        peak = jnp.maximum(jnp.max(old, axis=-1, keepdims=True), jnp.max(fresh, axis=-1, keepdims=True))
        old = jnp.exp(old - peak)
        fresh = jnp.exp(fresh - peak)
        total = jnp.sum(old, axis=-1, keepdims=True) + jnp.sum(fresh, axis=-1, keepdims=True)
        weights = old.astype(BF16)
        mixed = jnp.dot(weights, values(0), preferred_element_type=F32)
        for e in range(1, PAIR):
            other = jnp.dot(weights, values(e), preferred_element_type=F32)
            mixed = jnp.where(in_pair_o == e, other, mixed)
        mixed = mixed + jnp.dot(fresh.astype(BF16), v_new, preferred_element_type=F32)
        return (mixed / total).astype(BF16)

    @pl.loop(0, n)
    def _(o):
        slot = lax.rem(o, 2)
        source = peer(o)

        @pl.when(o + 1 < n)
        def _():
            for c in kv_load(o + 1, 1 - slot):
                c.start()

        for c in kv_load(o, slot):
            c.wait()

        @pl.when(o > 0)
        def _():
            msg_arrival(source).wait_recv()

        for i in range(AWAY):
            o_s[source, i] = attend(
                msg_r[source, i], lambda e: kbuf[slot, i * PAIR + e], lambda e: vbuf[slot, i * PAIR + e],
                source * rows + (home + i) * PAIR,
            )

        @pl.when(o == 0)
        def _():
            o_r[me, home:pairs] = o_s[me]

        @pl.when(o > 1)
        def _():
            o_copy(peer(o - 1)).start()

    for c in own:
        c.wait()
    o_copy(peer(n - 1)).start()

    def place(which, first, count):
        src, dst = ((rk, ka_ref), (rv, va_ref))[which]

        @pl.loop(0, count)
        def _(e):
            for h in range(n):
                mix_s[pl.ds(h, slots, stride=n), :] = src[h, first + e].astype(F32)
            dst[first + e] = mix_s[...].reshape(slots, n, hd).astype(BF16)

    @pl.loop(0, home)
    def _(r):
        bulk_wait(0, r)
        bulk_wait(1, r)
        bulk_next(r + AHEAD)
        place(0, r * PAIR, PAIR)
        place(1, r * PAIR, PAIR)

        @pl.loop(0, n)
        def _(h):
            o_r[h, r] = attend(
                msg_s[h, r], lambda e: rk[h, r * PAIR + e], lambda e: rv[h, r * PAIR + e], me * rows + r * PAIR
            )

    for o in range(1, n):
        o_arrival(peer(o)).wait_recv()
    for h in range(n):
        both = o_r[h].astype(F32)
        for j in range(q_per):
            head = both[:, j * new : (j + 1) * new, :].reshape(num, hd)
            act_s[:, (h * q_per + j) * hd : (h * q_per + j + 1) * hd] = head.astype(BF16)

    def wo_tile(i, w):
        at = pl.ds(pl.multiple_of(i * TILE, TILE), TILE)
        y = jnp.dot(act_s[...], w, preferred_element_type=F32)
        x1_s[:, at] = (hid_s[:, at] + y).astype(BF16).astype(F32)

    stream(wo_hbm, wo_tile)
    act_s[...] = rms(x1_s[...], mn_ref[...].astype(F32).reshape(1, dim)).astype(BF16)
    acc_s[...] = jnp.zeros_like(acc_s)
    tiles = wg_hbm.shape[1] // TILE

    def mlp_loads(i, slot):
        at = pl.ds(pl.multiple_of(i * TILE, TILE), TILE)
        return (
            load(cols(wg_hbm, i), wbuf, wsem, slot),
            load(cols(wu_hbm, i), ubuf, usem, slot),
            load(wd_hbm.at[at, :], dbuf, dsem, slot),
        )

    for c in mlp_loads(0, 0):
        c.start()

    @pl.loop(0, tiles)
    def _(i):
        slot = lax.rem(i, 2)

        @pl.when(i + 1 < tiles)
        def _():
            for c in mlp_loads(i + 1, 1 - slot):
                c.start()

        for c in mlp_loads(i, slot):
            c.wait()
        z = act_s[...]
        gate = jnp.dot(z, wbuf[slot], preferred_element_type=F32)
        up = jnp.dot(z, ubuf[slot], preferred_element_type=F32)
        g = (jax.nn.silu(gate) * up).astype(BF16)
        acc_s[...] += jnp.dot(g, dbuf[slot], preferred_element_type=F32)

    for c in range(0, dim, hd):
        tmp_s[...] = x1_s[:, c : c + hd] + acc_s[:, c : c + hd]
        for s in range(steps):
            out_ref[s, :, c : c + hd] = tmp_s[pl.ds(s, rows, stride=steps), :].astype(BF16)

    for o in range(1, n):
        msg_copy(peer(o)).wait_send()
        o_copy(peer(o)).wait_send()

    @pl.loop(home, pairs - 1)
    def _(r):
        for which in range(2):
            bulk_wait(which, r)
            place(which, r * PAIR, PAIR)

    bulk_wait(0, pairs - 1)
    place(0, rows - PAIR, PAIR)
    for e in range(PAIR):
        bulk_wait(1, pairs - 1 + e, 1)
        place(1, rows - PAIR + e, 1)

    for which, dst in enumerate((rk, rv)):
        whole = dst.at[pl.ds(0, n - 1)]
        pltpu.make_async_copy(whole, whole, bulk_s.at[which]).wait()


def store_kernel(pos_ref, hid_ref, ka_in, va_in, kn_ref, vn_ref, out_hbm, ko_hbm, vo_hbm, ka_ref, va_ref, hid_sem, sems):
    rows, steps = kn_ref.shape[0], kn_ref.shape[1]
    first = lax.axis_index("x") * rows
    for b in range(rows):
        at = pos_ref[first + b]
        for s in range(steps):
            ka_ref[b, at + s] = kn_ref[b, s]
            va_ref[b, at + s] = vn_ref[b, s]
    copies = [pltpu.make_async_copy(hid_ref, out_hbm, hid_sem)]
    for b in range(rows):
        copies.append(pltpu.make_async_copy(ka_ref.at[b], ko_hbm.at[b], sems.at[0, b]))
        copies.append(pltpu.make_async_copy(va_ref.at[b], vo_hbm.at[b], sems.at[1, b]))
    for c in copies:
        c.start()
    for c in copies:
        c.wait()


def solution(mesh):
    row_spec = P(None, ("dp", "x"), None)
    cache_in = P("dp", None, "x", None)
    cache_out = P(("dp", "x"), None, None, None)
    n = mesh.shape["x"]

    def local_run(start_pos, hidden_in, k_heads, v_heads, attn_norm, w_q, w_k, w_v, q_norm, k_norm, w_o, mlp_norm, w_gate, w_up, w_down):
        steps, rows, dim = hidden_in.shape
        slots, hd = k_heads.shape[1], k_heads.shape[3]
        heads = w_q.shape[1] // hd
        num = steps * rows
        pairs = rows // PAIR
        half = hd // 2
        inv_freq = np.power(np.float32(THETA), -np.arange(half, dtype=np.float32) * np.float32(2.0) / np.float32(hd))
        freq = jnp.asarray(np.concatenate([inv_freq, inv_freq])[None, :], F32)
        vmem = pl.BlockSpec(memory_space=pltpu.VMEM)
        hbm = pl.BlockSpec(memory_space=pltpu.HBM)
        smem = pl.BlockSpec(memory_space=pltpu.SMEM)
        tall, new = PAIR * steps * (heads // n), PAIR * steps
        dma = pltpu.SemaphoreType.DMA
        cache = (rows, slots, n, hd)
        fresh = (rows, steps, n, hd)
        blocks = pltpu.VMEM((n, rows, slots, hd), BF16)
        chunk = pltpu.VMEM((2, AWAY * PAIR, slots, hd), BF16)
        wide = pltpu.VMEM((num, dim), F32)
        head = pltpu.VMEM((num, hd), F32)
        arrived = [pltpu.VMEM(hidden_in.shape, BF16), pltpu.VMEM(fresh, BF16), pltpu.VMEM(fresh, BF16), pltpu.VMEM(cache, BF16), pltpu.VMEM(cache, BF16)]
        out, k_new, v_new, k_all, v_all = pl.pallas_call(
            functools.partial(layer_kernel, n, steps, rows, heads, hd),
            name="layer",
            out_shape=tuple(arrived),
            in_specs=[smem] + [hbm] * 15,
            out_specs=(vmem,) * 5,
            scratch_shapes=[
                pltpu.VMEM(freq.shape, F32), pltpu.VMEM(hidden_in.shape, BF16), pltpu.VMEM((dim,), BF16),
                pltpu.VMEM((1, hd), BF16), pltpu.VMEM((1, hd), BF16), pltpu.VMEM((dim,), BF16),
                wide, pltpu.VMEM((num, dim), BF16), wide, wide, head, head, head,
                pltpu.VMEM((n, pairs, tall + 2 * new, hd), BF16), pltpu.VMEM((n, AWAY, tall + 2 * new, hd), BF16),
                pltpu.VMEM((n, AWAY, tall, hd), BF16), pltpu.VMEM((n, pairs, tall, hd), BF16),
                blocks, blocks, chunk, chunk,
                pltpu.VMEM((2, dim, TILE), BF16), pltpu.VMEM((2, dim, TILE), BF16), pltpu.VMEM((2, TILE, dim), BF16),
                pltpu.VMEM((slots * n, hd), F32), pltpu.VMEM((num * n, hd), F32), pltpu.VMEM((num * n, hd), F32),
                dma((2,)), dma((2,)), dma((2,)), dma((2,)), dma((2,)), dma((2,)),
                dma((n,)), dma((n,)), dma((n,)), dma((n,)), dma((2,)), dma((pairs,)), dma((pairs - 1 + PAIR,)), dma((6,)),
            ],
            compiler_params=pltpu.CompilerParams(collective_id=0, has_side_effects=True, vmem_limit_bytes=VMEM_LIMIT),
        )(
            start_pos, freq, hidden_in, k_heads.reshape(-1, slots, hd), v_heads.reshape(-1, slots, hd), attn_norm,
            w_q, w_k, w_v, q_norm.reshape(1, -1), k_norm.reshape(1, -1), w_o, mlp_norm, w_gate, w_up, w_down,
        )
        return pl.pallas_call(
            store_kernel,
            name="store",
            out_shape=(
                jax.ShapeDtypeStruct(hidden_in.shape, BF16), jax.ShapeDtypeStruct(cache, BF16), jax.ShapeDtypeStruct(cache, BF16),
                pltpu.VMEM(cache, BF16), pltpu.VMEM(cache, BF16),
            ),
            in_specs=[smem] + [vmem] * 5,
            out_specs=(hbm,) * 3 + (vmem,) * 2,
            input_output_aliases={2: 3, 3: 4},
            scratch_shapes=[dma, dma((2, rows))],
            compiler_params=pltpu.CompilerParams(vmem_limit_bytes=2**20),
        )(start_pos, out, k_all, v_all, k_new, v_new)[:3]

    return jax.shard_map(local_run, mesh=mesh, in_specs=(P("dp"), row_spec, cache_in, cache_in) + (P(),) * 11, out_specs=(row_spec, cache_out, cache_out), check_vma=False)
```

```python
import functools

import jax
import jax.numpy as jnp
import numpy as np
from jax import lax
from jax.experimental import pallas as pl
from jax.experimental.pallas import tpu as pltpu
from jax.sharding import PartitionSpec as P

EPS = 1e-6
THETA = 1000000.0
F32 = jnp.float32
BF16 = jnp.bfloat16
MESH = pl.DeviceIdType.MESH
TILE = 512
PAIR = 2
AWAY = 2
VMEM_LIMIT = 44 * 2**20
AHEAD = 4


def rms(values, gain):
    inv_rms = lax.rsqrt(jnp.mean(values * values, axis=-1, keepdims=True) + EPS)
    return values * inv_rms * gain


def layer_kernel(
    n, steps, rows, heads, hd,
    pos_ref, freq_hbm, hid_hbm, k_hbm, v_hbm, an_hbm, wq_hbm, wk_hbm, wv_hbm, qn_hbm, kn_hbm, wo_hbm, mn_hbm,
    wg_hbm, wu_hbm, wd_hbm,
    out_ref, knew_ref, vnew_ref, ka_ref, va_ref,
    freq_ref, hid_ref, an_ref, qn_ref, kn_ref, mn_ref, hid_s, act_s, x1_s, acc_s, tmp_s, cs_s, sn_s, msg_s, msg_r, o_s, o_r, rk, rv, kbuf, vbuf, wbuf, ubuf, dbuf, mix_s, kmix_s, vmix_s,
    wsem, usem, dsem, ksem, vsem, own_sem, msg_ss, msg_rs, o_ss, o_rs, bulk_s, krs, vrs, in_sem,
):
    me = lax.axis_index("x")
    num = steps * rows
    q_per = heads // n
    pairs = rows // PAIR
    home = pairs - AWAY
    slots = k_hbm.shape[1]
    dim = hid_ref.shape[2]
    tall = PAIR * steps * q_per
    new = PAIR * steps
    barrier = pltpu.get_barrier_semaphore()

    def peer(o):
        return lax.rem(me + o, n)

    for o in range(1, n):
        pl.semaphore_signal(barrier, inc=1, device_id={"x": peer(o)}, device_id_type=MESH)

    small = [
        pltpu.make_async_copy(src, dst, in_sem.at[i])
        for i, (src, dst) in enumerate((
            (hid_hbm, hid_ref), (an_hbm, an_ref), (freq_hbm, freq_ref), (qn_hbm, qn_ref), (kn_hbm, kn_ref), (mn_hbm, mn_ref),
        ))
    ]
    for c in small:
        c.start()

    def cols(hbm, i):
        return hbm.at[:, pl.ds(pl.multiple_of(i * TILE, TILE), TILE)]

    def load(src, dst, sem, slot):
        return pltpu.make_async_copy(src, dst.at[slot], sem.at[slot])

    load(cols(wq_hbm, 0), wbuf, wsem, 0).start()
    pl.semaphore_wait(barrier, n - 1)

    order = (2, 6, 4, 3, 7, 5, 1) if n == 8 else tuple(range(1, n))

    def send(which, sem, first, count):
        for o in order:
            to = peer(o)
            pltpu.make_async_remote_copy(
                src_ref=(k_hbm, v_hbm)[which].at[pl.ds(to * rows + first, count)],
                dst_ref=(rk, rv)[which].at[me, pl.ds(first, count)],
                send_sem=bulk_s.at[which], recv_sem=(krs, vrs)[which].at[sem], device_id={"x": to}, device_id_type=MESH,
            ).start()

    def bulk(r):
        send(0, r, r * PAIR, PAIR)
        send(1, r, r * PAIR, PAIR)

    def bulk_last():
        send(0, pairs - 1, rows - PAIR, PAIR)
        for e in range(PAIR):
            send(1, pairs - 1 + e, rows - PAIR + e, 1)

    def bulk_next(r):
        @pl.when(r < pairs - 1)
        def _():
            bulk(r)

        @pl.when(r == pairs - 1)
        def _():
            bulk_last()

    def bulk_wait(which, r, count=PAIR):
        whole = (rk, rv)[which].at[pl.ds(0, n - 1), pl.ds(0, count)]
        pltpu.make_async_copy(whole, whole, (krs, vrs)[which].at[r]).wait()

    for r in range(2):
        bulk(r)

    own = [
        pltpu.make_async_copy(k_hbm.at[pl.ds(me * rows, rows)], rk.at[me], own_sem.at[0]),
        pltpu.make_async_copy(v_hbm.at[pl.ds(me * rows, rows)], rv.at[me], own_sem.at[1]),
    ]

    def stream(hbm, body, started=False):
        tiles = hbm.shape[1] // TILE
        if not started:
            load(cols(hbm, 0), wbuf, wsem, 0).start()

        @pl.loop(0, tiles)
        def _(i):
            slot = lax.rem(i, 2)

            @pl.when(i + 1 < tiles)
            def _():
                load(cols(hbm, i + 1), wbuf, wsem, 1 - slot).start()

            load(cols(hbm, i), wbuf, wsem, slot).wait()
            body(i, wbuf[slot])

    for c in small:
        c.wait()
    for c in range(0, dim, hd):
        for s in range(steps):
            tmp_s[pl.ds(s, rows, stride=steps), :] = hid_ref[s, :, c : c + hd].astype(F32)
        hid_s[:, c : c + hd] = tmp_s[...]
    act_s[...] = rms(hid_s[...], an_ref[...].astype(F32).reshape(1, dim)).astype(BF16)

    row = lax.broadcasted_iota(jnp.int32, (num, hd), 0)
    pos = jnp.zeros((num, hd), jnp.int32)
    for b in range(rows):
        pos = jnp.where(row // steps == b, pos_ref[me * rows + b], pos)
    angles = (pos + row % steps).astype(F32) * freq_ref[...]
    lane = lax.broadcasted_iota(jnp.int32, (num, hd), 1)
    cs_s[...] = jnp.cos(angles)
    sn_s[...] = jnp.where(lane < hd // 2, -jnp.sin(angles), jnp.sin(angles))

    def rotate(v):
        return v * cs_s[...] + pltpu.roll(v, hd // 2, 1) * sn_s[...]

    per_tile = TILE // hd

    def q_tile(i, w):
        y = jnp.dot(act_s[...], w, preferred_element_type=F32)
        gain = qn_ref[...].astype(F32)
        for g in range(per_tile // q_per):
            parts = []
            for j in range(q_per):
                c = (g * q_per + j) * hd
                head = rotate(rms(y[:, c : c + hd], gain))
                parts.append(head.reshape(pairs, new, hd))
            msg_s[i * (per_tile // q_per) + g, :, 0:tall, :] = jnp.concatenate(parts, axis=1).astype(BF16)

    def k_tile(i, w):
        y = jnp.dot(act_s[...], w, preferred_element_type=F32)
        gain = kn_ref[...].astype(F32)
        for g in range(per_tile):
            head = rotate(rms(y[:, g * hd : (g + 1) * hd], gain))
            msg_s[i * per_tile + g, :, tall : tall + new, :] = head.reshape(pairs, new, hd).astype(BF16)
            kmix_s[pl.ds(i * per_tile + g, num, stride=n), :] = head

    def v_tile(i, w):
        y = jnp.dot(act_s[...], w, preferred_element_type=F32)
        for g in range(per_tile):
            head = y[:, g * hd : (g + 1) * hd]
            msg_s[i * per_tile + g, :, tall + new : tall + 2 * new, :] = head.reshape(pairs, new, hd).astype(BF16)
            vmix_s[pl.ds(i * per_tile + g, num, stride=n), :] = head

    stream(wq_hbm, q_tile, started=True)
    stream(wk_hbm, k_tile)
    stream(wv_hbm, v_tile)

    def msg_copy(to):
        return pltpu.make_async_remote_copy(
            src_ref=msg_s.at[to, pl.ds(home, AWAY)], dst_ref=msg_r.at[me], send_sem=msg_ss.at[to], recv_sem=msg_rs.at[me],
            device_id={"x": to}, device_id_type=MESH,
        )

    def msg_arrival(source):
        return pltpu.make_async_remote_copy(
            src_ref=msg_s.at[source, pl.ds(home, AWAY)], dst_ref=msg_r.at[source], send_sem=msg_ss.at[source],
            recv_sem=msg_rs.at[source], device_id={"x": source}, device_id_type=MESH,
        )

    def o_copy(to):
        return pltpu.make_async_remote_copy(
            src_ref=o_s.at[to], dst_ref=o_r.at[me, pl.ds(home, AWAY)], send_sem=o_ss.at[to], recv_sem=o_rs.at[me],
            device_id={"x": to}, device_id_type=MESH,
        )

    def o_arrival(source):
        return pltpu.make_async_remote_copy(
            src_ref=o_s.at[source], dst_ref=o_r.at[source, pl.ds(home, AWAY)], send_sem=o_ss.at[source], recv_sem=o_rs.at[source],
            device_id={"x": source}, device_id_type=MESH,
        )

    def kv_load(o, slot):
        first = peer(o) * rows + home * PAIR
        return (
            pltpu.make_async_copy(k_hbm.at[pl.ds(first, AWAY * PAIR)], kbuf.at[slot], ksem.at[slot]),
            pltpu.make_async_copy(v_hbm.at[pl.ds(first, AWAY * PAIR)], vbuf.at[slot], vsem.at[slot]),
        )

    for c in kv_load(0, 0):
        c.start()
    for c in own:
        c.start()
    knew_ref[...] = kmix_s[...].reshape(rows, steps, n, hd).astype(BF16)
    vnew_ref[...] = vmix_s[...].reshape(rows, steps, n, hd).astype(BF16)
    msg_r[me] = msg_s[me, home:pairs]
    for o in range(1, n):
        msg_copy(peer(o)).start()
    for r in range(2, AHEAD):
        bulk(r)

    scale = hd ** -0.5
    nt = (((1,), (1,)), ((), ()))
    r_new = lax.broadcasted_iota(jnp.int32, (tall, new), 0) % new
    c_new = lax.broadcasted_iota(jnp.int32, (tall, new), 1)
    new_ok = (c_new // steps == r_new // steps) & (c_new % steps <= r_new % steps)
    in_pair = (lax.broadcasted_iota(jnp.int32, (tall, slots), 0) % new) // steps
    in_pair_o = (lax.broadcasted_iota(jnp.int32, (tall, hd), 0) % new) // steps
    t = lax.broadcasted_iota(jnp.int32, (tall, slots), 1)

    def attend(msg, keys, values, first):
        q = msg[0:tall]
        v_new = msg[tall + new : tall + 2 * new]
        fresh = lax.dot_general(q, msg[tall : tall + new], nt, preferred_element_type=F32)
        fresh = jnp.where(new_ok, fresh * scale, -jnp.inf)
        old = lax.dot_general(q, keys(0), nt, preferred_element_type=F32)
        start = jnp.full((tall, slots), pos_ref[first], jnp.int32)
        for e in range(1, PAIR):
            other = lax.dot_general(q, keys(e), nt, preferred_element_type=F32)
            old = jnp.where(in_pair == e, other, old)
            start = jnp.where(in_pair == e, pos_ref[first + e], start)
        old = jnp.where(t < start, old * scale, -jnp.inf)
        peak = jnp.maximum(jnp.max(old, axis=-1, keepdims=True), jnp.max(fresh, axis=-1, keepdims=True))
        old = jnp.exp(old - peak)
        fresh = jnp.exp(fresh - peak)
        total = jnp.sum(old, axis=-1, keepdims=True) + jnp.sum(fresh, axis=-1, keepdims=True)
        weights = old.astype(BF16)
        mixed = jnp.dot(weights, values(0), preferred_element_type=F32)
        for e in range(1, PAIR):
            other = jnp.dot(weights, values(e), preferred_element_type=F32)
            mixed = jnp.where(in_pair_o == e, other, mixed)
        mixed = mixed + jnp.dot(fresh.astype(BF16), v_new, preferred_element_type=F32)
        return (mixed / total).astype(BF16)

    @pl.loop(0, n)
    def _(o):
        slot = lax.rem(o, 2)
        source = peer(o)

        @pl.when(o + 1 < n)
        def _():
            for c in kv_load(o + 1, 1 - slot):
                c.start()

        for c in kv_load(o, slot):
            c.wait()

        @pl.when(o > 0)
        def _():
            msg_arrival(source).wait_recv()

        for i in range(AWAY):
            o_s[source, i] = attend(
                msg_r[source, i], lambda e: kbuf[slot, i * PAIR + e], lambda e: vbuf[slot, i * PAIR + e],
                source * rows + (home + i) * PAIR,
            )

        @pl.when(o == 0)
        def _():
            o_r[me, home:pairs] = o_s[me]

        @pl.when(o > 1)
        def _():
            o_copy(peer(o - 1)).start()

    for c in own:
        c.wait()
    o_copy(peer(n - 1)).start()

    def place(which, first, count):
        src, dst = ((rk, ka_ref), (rv, va_ref))[which]

        @pl.loop(0, count)
        def _(e):
            for h in range(n):
                mix_s[pl.ds(h, slots, stride=n), :] = src[h, first + e].astype(F32)
            dst[first + e] = mix_s[...].reshape(slots, n, hd).astype(BF16)

    @pl.loop(0, home)
    def _(r):
        bulk_wait(0, r)
        bulk_wait(1, r)
        bulk_next(r + AHEAD)
        place(0, r * PAIR, PAIR)
        place(1, r * PAIR, PAIR)

        @pl.loop(0, n)
        def _(h):
            o_r[h, r] = attend(
                msg_s[h, r], lambda e: rk[h, r * PAIR + e], lambda e: rv[h, r * PAIR + e], me * rows + r * PAIR
            )

    for o in range(1, n):
        o_arrival(peer(o)).wait_recv()
    for h in range(n):
        both = o_r[h].astype(F32)
        for j in range(q_per):
            head = both[:, j * new : (j + 1) * new, :].reshape(num, hd)
            act_s[:, (h * q_per + j) * hd : (h * q_per + j + 1) * hd] = head.astype(BF16)

    def wo_tile(i, w):
        at = pl.ds(pl.multiple_of(i * TILE, TILE), TILE)
        y = jnp.dot(act_s[...], w, preferred_element_type=F32)
        x1_s[:, at] = (hid_s[:, at] + y).astype(BF16).astype(F32)

    stream(wo_hbm, wo_tile)
    act_s[...] = rms(x1_s[...], mn_ref[...].astype(F32).reshape(1, dim)).astype(BF16)
    acc_s[...] = jnp.zeros_like(acc_s)
    tiles = wg_hbm.shape[1] // TILE

    def mlp_loads(i, slot):
        at = pl.ds(pl.multiple_of(i * TILE, TILE), TILE)
        return (
            load(cols(wg_hbm, i), wbuf, wsem, slot),
            load(cols(wu_hbm, i), ubuf, usem, slot),
            load(wd_hbm.at[at, :], dbuf, dsem, slot),
        )

    for c in mlp_loads(0, 0):
        c.start()

    @pl.loop(0, tiles)
    def _(i):
        slot = lax.rem(i, 2)

        @pl.when(i + 1 < tiles)
        def _():
            for c in mlp_loads(i + 1, 1 - slot):
                c.start()

        for c in mlp_loads(i, slot):
            c.wait()
        z = act_s[...]
        gate = jnp.dot(z, wbuf[slot], preferred_element_type=F32)
        up = jnp.dot(z, ubuf[slot], preferred_element_type=F32)
        g = (jax.nn.silu(gate) * up).astype(BF16)
        acc_s[...] += jnp.dot(g, dbuf[slot], preferred_element_type=F32)

    for c in range(0, dim, hd):
        tmp_s[...] = x1_s[:, c : c + hd] + acc_s[:, c : c + hd]
        for s in range(steps):
            out_ref[s, :, c : c + hd] = tmp_s[pl.ds(s, rows, stride=steps), :].astype(BF16)

    for o in range(1, n):
        msg_copy(peer(o)).wait_send()
        o_copy(peer(o)).wait_send()

    @pl.loop(home, pairs - 1)
    def _(r):
        for which in range(2):
            bulk_wait(which, r)
            place(which, r * PAIR, PAIR)

    bulk_wait(0, pairs - 1)
    place(0, rows - PAIR, PAIR)
    for e in range(PAIR):
        bulk_wait(1, pairs - 1 + e, 1)
        place(1, rows - PAIR + e, 1)

    for which, dst in enumerate((rk, rv)):
        whole = dst.at[pl.ds(0, n - 1)]
        pltpu.make_async_copy(whole, whole, bulk_s.at[which]).wait()


def store_kernel(pos_ref, hid_ref, ka_in, va_in, kn_ref, vn_ref, out_hbm, ko_hbm, vo_hbm, ka_ref, va_ref, hid_sem, sems):
    rows, steps = kn_ref.shape[0], kn_ref.shape[1]
    first = lax.axis_index("x") * rows
    for b in range(rows):
        at = pos_ref[first + b]
        for s in range(steps):
            ka_ref[b, at + s] = kn_ref[b, s]
            va_ref[b, at + s] = vn_ref[b, s]
    copies = [pltpu.make_async_copy(hid_ref, out_hbm, hid_sem)]
    for b in range(rows):
        copies.append(pltpu.make_async_copy(ka_ref.at[b], ko_hbm.at[b], sems.at[0, b]))
        copies.append(pltpu.make_async_copy(va_ref.at[b], vo_hbm.at[b], sems.at[1, b]))
    for c in copies:
        c.start()
    for c in copies:
        c.wait()


def solution(mesh):
    row_spec = P(None, ("dp", "x"), None)
    cache_in = P("dp", None, "x", None)
    cache_out = P(("dp", "x"), None, None, None)
    n = mesh.shape["x"]

    def local_run(start_pos, hidden_in, k_heads, v_heads, attn_norm, w_q, w_k, w_v, q_norm, k_norm, w_o, mlp_norm, w_gate, w_up, w_down):
        steps, rows, dim = hidden_in.shape
        slots, hd = k_heads.shape[1], k_heads.shape[3]
        heads = w_q.shape[1] // hd
        num = steps * rows
        pairs = rows // PAIR
        half = hd // 2
        inv_freq = np.power(np.float32(THETA), -np.arange(half, dtype=np.float32) * np.float32(2.0) / np.float32(hd))
        freq = jnp.asarray(np.concatenate([inv_freq, inv_freq])[None, :], F32)
        vmem = pl.BlockSpec(memory_space=pltpu.VMEM)
        hbm = pl.BlockSpec(memory_space=pltpu.HBM)
        smem = pl.BlockSpec(memory_space=pltpu.SMEM)
        tall, new = PAIR * steps * (heads // n), PAIR * steps
        dma = pltpu.SemaphoreType.DMA
        cache = (rows, slots, n, hd)
        fresh = (rows, steps, n, hd)
        blocks = pltpu.VMEM((n, rows, slots, hd), BF16)
        chunk = pltpu.VMEM((2, AWAY * PAIR, slots, hd), BF16)
        wide = pltpu.VMEM((num, dim), F32)
        head = pltpu.VMEM((num, hd), F32)
        arrived = [pltpu.VMEM(hidden_in.shape, BF16), pltpu.VMEM(fresh, BF16), pltpu.VMEM(fresh, BF16), pltpu.VMEM(cache, BF16), pltpu.VMEM(cache, BF16)]
        out, k_new, v_new, k_all, v_all = pl.pallas_call(
            functools.partial(layer_kernel, n, steps, rows, heads, hd),
            name="layer",
            out_shape=tuple(arrived),
            in_specs=[smem] + [hbm] * 15,
            out_specs=(vmem,) * 5,
            scratch_shapes=[
                pltpu.VMEM(freq.shape, F32), pltpu.VMEM(hidden_in.shape, BF16), pltpu.VMEM((dim,), BF16),
                pltpu.VMEM((1, hd), BF16), pltpu.VMEM((1, hd), BF16), pltpu.VMEM((dim,), BF16),
                wide, pltpu.VMEM((num, dim), BF16), wide, wide, head, head, head,
                pltpu.VMEM((n, pairs, tall + 2 * new, hd), BF16), pltpu.VMEM((n, AWAY, tall + 2 * new, hd), BF16),
                pltpu.VMEM((n, AWAY, tall, hd), BF16), pltpu.VMEM((n, pairs, tall, hd), BF16),
                blocks, blocks, chunk, chunk,
                pltpu.VMEM((2, dim, TILE), BF16), pltpu.VMEM((2, dim, TILE), BF16), pltpu.VMEM((2, TILE, dim), BF16),
                pltpu.VMEM((slots * n, hd), F32), pltpu.VMEM((num * n, hd), F32), pltpu.VMEM((num * n, hd), F32),
                dma((2,)), dma((2,)), dma((2,)), dma((2,)), dma((2,)), dma((2,)),
                dma((n,)), dma((n,)), dma((n,)), dma((n,)), dma((2,)), dma((pairs,)), dma((pairs - 1 + PAIR,)), dma((6,)),
            ],
            compiler_params=pltpu.CompilerParams(collective_id=0, has_side_effects=True, vmem_limit_bytes=VMEM_LIMIT),
        )(
            start_pos, freq, hidden_in, k_heads.reshape(-1, slots, hd), v_heads.reshape(-1, slots, hd), attn_norm,
            w_q, w_k, w_v, q_norm.reshape(1, -1), k_norm.reshape(1, -1), w_o, mlp_norm, w_gate, w_up, w_down,
        )
        return pl.pallas_call(
            store_kernel,
            name="store",
            out_shape=(
                jax.ShapeDtypeStruct(hidden_in.shape, BF16), jax.ShapeDtypeStruct(cache, BF16), jax.ShapeDtypeStruct(cache, BF16),
                pltpu.VMEM(cache, BF16), pltpu.VMEM(cache, BF16),
            ),
            in_specs=[smem] + [vmem] * 5,
            out_specs=(hbm,) * 3 + (vmem,) * 2,
            input_output_aliases={2: 3, 3: 4},
            scratch_shapes=[dma, dma((2, rows))],
            compiler_params=pltpu.CompilerParams(vmem_limit_bytes=2**20),
        )(start_pos, out, k_all, v_all, k_new, v_new)[:3]

    return jax.shard_map(local_run, mesh=mesh, in_specs=(P("dp"), row_spec, cache_in, cache_in) + (P(),) * 11, out_specs=(row_spec, cache_out, cache_out), check_vma=False)
```

```python
import functools

import jax
import jax.numpy as jnp
import numpy as np
from jax import lax
from jax.experimental import pallas as pl
from jax.experimental.pallas import tpu as pltpu
from jax.sharding import PartitionSpec as P

EPS = 1e-6
THETA = 1000000.0
F32 = jnp.float32
BF16 = jnp.bfloat16
MESH = pl.DeviceIdType.MESH
TILE = 512
PAIR = 2
AWAY = 2
VMEM_LIMIT = 44 * 2**20
AHEAD = 4


def rms(values, gain):
    inv_rms = lax.rsqrt(jnp.mean(values * values, axis=-1, keepdims=True) + EPS)
    return values * inv_rms * gain


def layer_kernel(
    n, steps, rows, heads, hd,
    pos_ref, freq_hbm, hid_hbm, k_hbm, v_hbm, an_hbm, wq_hbm, wk_hbm, wv_hbm, qn_hbm, kn_hbm, wo_hbm, mn_hbm,
    wg_hbm, wu_hbm, wd_hbm,
    out_ref, knew_ref, vnew_ref, ka_ref, va_ref,
    freq_ref, hid_ref, an_ref, qn_ref, kn_ref, mn_ref, hid_s, act_s, x1_s, acc_s, tmp_s, cs_s, sn_s, msg_s, msg_r, o_s, o_r, rk, rv, kbuf, vbuf, wbuf, ubuf, dbuf, mix_s, kmix_s, vmix_s,
    wsem, usem, dsem, ksem, vsem, own_sem, msg_ss, msg_rs, o_ss, o_rs, bulk_s, krs, vrs, in_sem, ready,
):
    me = lax.axis_index("x")
    num = steps * rows
    q_per = heads // n
    pairs = rows // PAIR
    home = pairs - AWAY
    slots = k_hbm.shape[1]
    dim = hid_ref.shape[2]
    tall = PAIR * steps * q_per
    new = PAIR * steps
    barrier = pltpu.get_barrier_semaphore()

    chips = n // 2
    chip, core = me // 2, lax.rem(me, 2)

    def peer(o):
        return lax.rem(me + o, n)

    def away(hops, cross):
        return lax.rem(chip + hops, chips) * 2 + (1 - core if cross else core)

    near = [(0, True)] + [(hops, cross) for hops in (1, chips - 1) for cross in (False, True)]
    far = [(hops, cross) for hops in range(2, chips - 1) for cross in (False, True)]
    for to in near:
        pl.semaphore_signal(barrier, inc=1, device_id={"x": away(*to)}, device_id_type=MESH)

    small = [
        pltpu.make_async_copy(src, dst, in_sem.at[i])
        for i, (src, dst) in enumerate((
            (hid_hbm, hid_ref), (an_hbm, an_ref), (freq_hbm, freq_ref), (qn_hbm, qn_ref), (kn_hbm, kn_ref), (mn_hbm, mn_ref),
        ))
    ]
    for c in small:
        c.start()

    def cols(hbm, i):
        return hbm.at[:, pl.ds(pl.multiple_of(i * TILE, TILE), TILE)]

    def load(src, dst, sem, slot):
        return pltpu.make_async_copy(src, dst.at[slot], sem.at[slot])

    load(cols(wq_hbm, 0), wbuf, wsem, 0).start()
    pl.semaphore_wait(barrier, len(near))
    pl.semaphore_signal(ready, inc=1, device_id={"x": away(chips - 1, False)}, device_id_type=MESH)

    def send(which, sem, first, count, lo, size, order):
        for hops, cross in order:
            to = away(hops, cross)
            pltpu.make_async_remote_copy(
                src_ref=(k_hbm, v_hbm)[which].at[pl.ds(to * rows + first, count), pl.ds(lo, size)],
                dst_ref=(rk, rv)[which].at[me, pl.ds(first, count), pl.ds(lo, size)],
                send_sem=bulk_s.at[which], recv_sem=(krs, vrs)[which].at[sem], device_id={"x": to}, device_id_type=MESH,
            ).start()

    mixed_order = [(1, False), (chips - 1, False)] + far[:1] + [(1, True), (chips - 1, True)] + far[1:] + [(0, True)]
    far_first = far + [(1, False), (chips - 1, False), (1, True), (chips - 1, True), (0, True)]
    last = [(0, pairs - 1, rows - PAIR, PAIR, 0, slots)]
    last += [(1, pairs - 1 + e, rows - PAIR + e, 1, 0, slots) for e in range(PAIR - 1)]
    for i, (lo, size) in enumerate(((0, slots // 2), (slots // 2, slots // 4), (slots * 3 // 4, slots // 4))):
        last.append((1, pairs - 2 + PAIR + i, rows - 1, 1, lo, size))

    def bulk(r):
        send(0, r, r * PAIR, PAIR, 0, slots, mixed_order)
        send(1, r, r * PAIR, PAIR, 0, slots, mixed_order)

    def bulk_last():
        for which, sem, first, count, lo, size in last:
            send(which, sem, first, count, lo, size, far_first)

    def bulk_next(r):
        @pl.when(r < pairs - 1)
        def _():
            bulk(r)

        @pl.when(r == pairs - 1)
        def _():
            bulk_last()

    def bulk_wait(which, sem, count, size):
        whole = (rk, rv)[which].at[pl.ds(0, n - 1), pl.ds(0, count), pl.ds(0, size)]
        pltpu.make_async_copy(whole, whole, (krs, vrs)[which].at[sem]).wait()

    send(0, 0, 0, PAIR, 0, slots, near)
    pl.semaphore_wait(ready, 1)
    send(0, 0, 0, PAIR, 0, slots, far)
    send(1, 0, 0, PAIR, 0, slots, mixed_order)
    bulk(1)

    own = [
        pltpu.make_async_copy(k_hbm.at[pl.ds(me * rows, rows)], rk.at[me], own_sem.at[0]),
        pltpu.make_async_copy(v_hbm.at[pl.ds(me * rows, rows)], rv.at[me], own_sem.at[1]),
    ]

    def stream(hbm, body, started=False):
        tiles = hbm.shape[1] // TILE
        if not started:
            load(cols(hbm, 0), wbuf, wsem, 0).start()

        @pl.loop(0, tiles)
        def _(i):
            slot = lax.rem(i, 2)

            @pl.when(i + 1 < tiles)
            def _():
                load(cols(hbm, i + 1), wbuf, wsem, 1 - slot).start()

            load(cols(hbm, i), wbuf, wsem, slot).wait()
            body(i, wbuf[slot])

    for c in small:
        c.wait()
    for c in range(0, dim, hd):
        for s in range(steps):
            tmp_s[pl.ds(s, rows, stride=steps), :] = hid_ref[s, :, c : c + hd].astype(F32)
        hid_s[:, c : c + hd] = tmp_s[...]
    act_s[...] = rms(hid_s[...], an_ref[...].astype(F32).reshape(1, dim)).astype(BF16)

    row = lax.broadcasted_iota(jnp.int32, (num, hd), 0)
    pos = jnp.zeros((num, hd), jnp.int32)
    for b in range(rows):
        pos = jnp.where(row // steps == b, pos_ref[me * rows + b], pos)
    angles = (pos + row % steps).astype(F32) * freq_ref[...]
    lane = lax.broadcasted_iota(jnp.int32, (num, hd), 1)
    cs_s[...] = jnp.cos(angles)
    sn_s[...] = jnp.where(lane < hd // 2, -jnp.sin(angles), jnp.sin(angles))

    def rotate(v):
        return v * cs_s[...] + pltpu.roll(v, hd // 2, 1) * sn_s[...]

    per_tile = TILE // hd

    def q_tile(i, w):
        y = jnp.dot(act_s[...], w, preferred_element_type=F32)
        gain = qn_ref[...].astype(F32)
        for g in range(per_tile // q_per):
            parts = []
            for j in range(q_per):
                c = (g * q_per + j) * hd
                head = rotate(rms(y[:, c : c + hd], gain))
                parts.append(head.reshape(pairs, new, hd))
            msg_s[i * (per_tile // q_per) + g, :, 0:tall, :] = jnp.concatenate(parts, axis=1).astype(BF16)

    def k_tile(i, w):
        y = jnp.dot(act_s[...], w, preferred_element_type=F32)
        gain = kn_ref[...].astype(F32)
        for g in range(per_tile):
            head = rotate(rms(y[:, g * hd : (g + 1) * hd], gain))
            msg_s[i * per_tile + g, :, tall : tall + new, :] = head.reshape(pairs, new, hd).astype(BF16)
            kmix_s[pl.ds(i * per_tile + g, num, stride=n), :] = head

    def v_tile(i, w):
        y = jnp.dot(act_s[...], w, preferred_element_type=F32)
        for g in range(per_tile):
            head = y[:, g * hd : (g + 1) * hd]
            msg_s[i * per_tile + g, :, tall + new : tall + 2 * new, :] = head.reshape(pairs, new, hd).astype(BF16)
            vmix_s[pl.ds(i * per_tile + g, num, stride=n), :] = head

    stream(wq_hbm, q_tile, started=True)
    stream(wk_hbm, k_tile)
    stream(wv_hbm, v_tile)

    def msg_copy(to):
        return pltpu.make_async_remote_copy(
            src_ref=msg_s.at[to, pl.ds(home, AWAY)], dst_ref=msg_r.at[me], send_sem=msg_ss.at[to], recv_sem=msg_rs.at[me],
            device_id={"x": to}, device_id_type=MESH,
        )

    def msg_arrival(source):
        return pltpu.make_async_remote_copy(
            src_ref=msg_s.at[source, pl.ds(home, AWAY)], dst_ref=msg_r.at[source], send_sem=msg_ss.at[source],
            recv_sem=msg_rs.at[source], device_id={"x": source}, device_id_type=MESH,
        )

    def o_copy(to):
        return pltpu.make_async_remote_copy(
            src_ref=o_s.at[to], dst_ref=o_r.at[me, pl.ds(home, AWAY)], send_sem=o_ss.at[to], recv_sem=o_rs.at[me],
            device_id={"x": to}, device_id_type=MESH,
        )

    def o_arrival(source):
        return pltpu.make_async_remote_copy(
            src_ref=o_s.at[source], dst_ref=o_r.at[source, pl.ds(home, AWAY)], send_sem=o_ss.at[source], recv_sem=o_rs.at[source],
            device_id={"x": source}, device_id_type=MESH,
        )

    def kv_load(o, slot):
        first = peer(o) * rows + home * PAIR
        return (
            pltpu.make_async_copy(k_hbm.at[pl.ds(first, AWAY * PAIR)], kbuf.at[slot], ksem.at[slot]),
            pltpu.make_async_copy(v_hbm.at[pl.ds(first, AWAY * PAIR)], vbuf.at[slot], vsem.at[slot]),
        )

    for c in kv_load(0, 0):
        c.start()
    for c in own:
        c.start()
    knew_ref[...] = kmix_s[...].reshape(rows, steps, n, hd).astype(BF16)
    vnew_ref[...] = vmix_s[...].reshape(rows, steps, n, hd).astype(BF16)
    msg_r[me] = msg_s[me, home:pairs]
    for o in range(1, n):
        msg_copy(peer(o)).start()
    for r in range(2, AHEAD):
        bulk(r)

    scale = hd ** -0.5
    nt = (((1,), (1,)), ((), ()))
    r_new = lax.broadcasted_iota(jnp.int32, (tall, new), 0) % new
    c_new = lax.broadcasted_iota(jnp.int32, (tall, new), 1)
    new_ok = (c_new // steps == r_new // steps) & (c_new % steps <= r_new % steps)
    in_pair = (lax.broadcasted_iota(jnp.int32, (tall, slots), 0) % new) // steps
    in_pair_o = (lax.broadcasted_iota(jnp.int32, (tall, hd), 0) % new) // steps
    t = lax.broadcasted_iota(jnp.int32, (tall, slots), 1)

    def attend(msg, keys, values, first):
        q = msg[0:tall]
        v_new = msg[tall + new : tall + 2 * new]
        fresh = lax.dot_general(q, msg[tall : tall + new], nt, preferred_element_type=F32)
        fresh = jnp.where(new_ok, fresh * scale, -jnp.inf)
        old = lax.dot_general(q, keys(0), nt, preferred_element_type=F32)
        start = jnp.full((tall, slots), pos_ref[first], jnp.int32)
        for e in range(1, PAIR):
            other = lax.dot_general(q, keys(e), nt, preferred_element_type=F32)
            old = jnp.where(in_pair == e, other, old)
            start = jnp.where(in_pair == e, pos_ref[first + e], start)
        old = jnp.where(t < start, old * scale, -jnp.inf)
        peak = jnp.maximum(jnp.max(old, axis=-1, keepdims=True), jnp.max(fresh, axis=-1, keepdims=True))
        old = jnp.exp(old - peak)
        fresh = jnp.exp(fresh - peak)
        total = jnp.sum(old, axis=-1, keepdims=True) + jnp.sum(fresh, axis=-1, keepdims=True)
        weights = old.astype(BF16)
        mixed = jnp.dot(weights, values(0), preferred_element_type=F32)
        for e in range(1, PAIR):
            other = jnp.dot(weights, values(e), preferred_element_type=F32)
            mixed = jnp.where(in_pair_o == e, other, mixed)
        mixed = mixed + jnp.dot(fresh.astype(BF16), v_new, preferred_element_type=F32)
        return (mixed / total).astype(BF16)

    @pl.loop(0, n)
    def _(o):
        slot = lax.rem(o, 2)
        source = peer(o)

        @pl.when(o + 1 < n)
        def _():
            for c in kv_load(o + 1, 1 - slot):
                c.start()

        for c in kv_load(o, slot):
            c.wait()

        @pl.when(o > 0)
        def _():
            msg_arrival(source).wait_recv()

        for i in range(AWAY):
            o_s[source, i] = attend(
                msg_r[source, i], lambda e: kbuf[slot, i * PAIR + e], lambda e: vbuf[slot, i * PAIR + e],
                source * rows + (home + i) * PAIR,
            )

        @pl.when(o == 0)
        def _():
            o_r[me, home:pairs] = o_s[me]

        @pl.when(o > 1)
        def _():
            o_copy(peer(o - 1)).start()

    for c in own:
        c.wait()
    o_copy(peer(n - 1)).start()

    def place(which, first, count, lo=0, size=slots):
        src, dst = ((rk, ka_ref), (rv, va_ref))[which]

        @pl.loop(0, count)
        def _(e):
            for h in range(n):
                mix_s[pl.ds(h, size, stride=n), :] = src[h, first + e, lo : lo + size].astype(F32)
            dst[first + e, lo : lo + size] = mix_s[0 : size * n].reshape(size, n, hd).astype(BF16)

    @pl.loop(0, home)
    def _(r):
        bulk_wait(0, r, PAIR, slots)
        bulk_wait(1, r, PAIR, slots)
        bulk_next(r + AHEAD)
        place(0, r * PAIR, PAIR)
        place(1, r * PAIR, PAIR)

        @pl.loop(0, n)
        def _(h):
            o_r[h, r] = attend(
                msg_s[h, r], lambda e: rk[h, r * PAIR + e], lambda e: rv[h, r * PAIR + e], me * rows + r * PAIR
            )

    for o in range(1, n):
        o_arrival(peer(o)).wait_recv()
    for h in range(n):
        both = o_r[h].astype(F32)
        for j in range(q_per):
            head = both[:, j * new : (j + 1) * new, :].reshape(num, hd)
            act_s[:, (h * q_per + j) * hd : (h * q_per + j + 1) * hd] = head.astype(BF16)

    def wo_tile(i, w):
        at = pl.ds(pl.multiple_of(i * TILE, TILE), TILE)
        y = jnp.dot(act_s[...], w, preferred_element_type=F32)
        x1_s[:, at] = (hid_s[:, at] + y).astype(BF16).astype(F32)

    stream(wo_hbm, wo_tile)
    act_s[...] = rms(x1_s[...], mn_ref[...].astype(F32).reshape(1, dim)).astype(BF16)
    acc_s[...] = jnp.zeros_like(acc_s)
    tiles = wg_hbm.shape[1] // TILE

    def mlp_loads(i, slot):
        at = pl.ds(pl.multiple_of(i * TILE, TILE), TILE)
        return (
            load(cols(wg_hbm, i), wbuf, wsem, slot),
            load(cols(wu_hbm, i), ubuf, usem, slot),
            load(wd_hbm.at[at, :], dbuf, dsem, slot),
        )

    for c in mlp_loads(0, 0):
        c.start()

    @pl.loop(0, tiles)
    def _(i):
        slot = lax.rem(i, 2)

        @pl.when(i + 1 < tiles)
        def _():
            for c in mlp_loads(i + 1, 1 - slot):
                c.start()

        for c in mlp_loads(i, slot):
            c.wait()
        z = act_s[...]
        gate = jnp.dot(z, wbuf[slot], preferred_element_type=F32)
        up = jnp.dot(z, ubuf[slot], preferred_element_type=F32)
        g = (jax.nn.silu(gate) * up).astype(BF16)
        acc_s[...] += jnp.dot(g, dbuf[slot], preferred_element_type=F32)

    for c in range(0, dim, hd):
        tmp_s[...] = x1_s[:, c : c + hd] + acc_s[:, c : c + hd]
        for s in range(steps):
            out_ref[s, :, c : c + hd] = tmp_s[pl.ds(s, rows, stride=steps), :].astype(BF16)

    for o in range(1, n):
        msg_copy(peer(o)).wait_send()
        o_copy(peer(o)).wait_send()

    @pl.loop(home, pairs - 1)
    def _(r):
        for which in range(2):
            bulk_wait(which, r, PAIR, slots)
            place(which, r * PAIR, PAIR)

    for which, sem, first, count, lo, size in last:
        bulk_wait(which, sem, count, size)
        place(which, first, count, lo, size)

    for which, dst in enumerate((rk, rv)):
        whole = dst.at[pl.ds(0, n - 1)]
        pltpu.make_async_copy(whole, whole, bulk_s.at[which]).wait()


def store_kernel(pos_ref, hid_ref, ka_in, va_in, kn_ref, vn_ref, out_hbm, ko_hbm, vo_hbm, ka_ref, va_ref, hid_sem, sems):
    rows, steps = kn_ref.shape[0], kn_ref.shape[1]
    first = lax.axis_index("x") * rows
    hidden = pltpu.make_async_copy(hid_ref, out_hbm, hid_sem)
    hidden.start()
    copies = []
    for b in range(rows):
        copies.append((
            pltpu.make_async_copy(ka_ref.at[b], ko_hbm.at[b], sems.at[0, b]),
            pltpu.make_async_copy(va_ref.at[b], vo_hbm.at[b], sems.at[1, b]),
        ))
    for b in range(rows + 1):
        if b < rows:
            at = pos_ref[first + b]
            for s in range(steps):
                ka_ref[b, at + s] = kn_ref[b, s]
                va_ref[b, at + s] = vn_ref[b, s]
        if b > 0:
            for c in copies[b - 1]:
                c.start()
    for pair in copies:
        for c in pair:
            c.wait()
    hidden.wait()


def solution(mesh):
    row_spec = P(None, ("dp", "x"), None)
    cache_in = P("dp", None, "x", None)
    cache_out = P(("dp", "x"), None, None, None)
    n = mesh.shape["x"]

    def local_run(start_pos, hidden_in, k_heads, v_heads, attn_norm, w_q, w_k, w_v, q_norm, k_norm, w_o, mlp_norm, w_gate, w_up, w_down):
        steps, rows, dim = hidden_in.shape
        slots, hd = k_heads.shape[1], k_heads.shape[3]
        heads = w_q.shape[1] // hd
        num = steps * rows
        pairs = rows // PAIR
        half = hd // 2
        inv_freq = np.power(np.float32(THETA), -np.arange(half, dtype=np.float32) * np.float32(2.0) / np.float32(hd))
        freq = jnp.asarray(np.concatenate([inv_freq, inv_freq])[None, :], F32)
        vmem = pl.BlockSpec(memory_space=pltpu.VMEM)
        hbm = pl.BlockSpec(memory_space=pltpu.HBM)
        smem = pl.BlockSpec(memory_space=pltpu.SMEM)
        tall, new = PAIR * steps * (heads // n), PAIR * steps
        dma = pltpu.SemaphoreType.DMA
        cache = (rows, slots, n, hd)
        fresh = (rows, steps, n, hd)
        blocks = pltpu.VMEM((n, rows, slots, hd), BF16)
        chunk = pltpu.VMEM((2, AWAY * PAIR, slots, hd), BF16)
        wide = pltpu.VMEM((num, dim), F32)
        head = pltpu.VMEM((num, hd), F32)
        arrived = [pltpu.VMEM(hidden_in.shape, BF16), pltpu.VMEM(fresh, BF16), pltpu.VMEM(fresh, BF16), pltpu.VMEM(cache, BF16), pltpu.VMEM(cache, BF16)]
        out, k_new, v_new, k_all, v_all = pl.pallas_call(
            functools.partial(layer_kernel, n, steps, rows, heads, hd),
            name="layer",
            out_shape=tuple(arrived),
            in_specs=[smem] + [hbm] * 15,
            out_specs=(vmem,) * 5,
            scratch_shapes=[
                pltpu.VMEM(freq.shape, F32), pltpu.VMEM(hidden_in.shape, BF16), pltpu.VMEM((dim,), BF16),
                pltpu.VMEM((1, hd), BF16), pltpu.VMEM((1, hd), BF16), pltpu.VMEM((dim,), BF16),
                wide, pltpu.VMEM((num, dim), BF16), wide, wide, head, head, head,
                pltpu.VMEM((n, pairs, tall + 2 * new, hd), BF16), pltpu.VMEM((n, AWAY, tall + 2 * new, hd), BF16),
                pltpu.VMEM((n, AWAY, tall, hd), BF16), pltpu.VMEM((n, pairs, tall, hd), BF16),
                blocks, blocks, chunk, chunk,
                pltpu.VMEM((2, dim, TILE), BF16), pltpu.VMEM((2, dim, TILE), BF16), pltpu.VMEM((2, TILE, dim), BF16),
                pltpu.VMEM((slots * n, hd), F32), pltpu.VMEM((num * n, hd), F32), pltpu.VMEM((num * n, hd), F32),
                dma((2,)), dma((2,)), dma((2,)), dma((2,)), dma((2,)), dma((2,)),
                dma((n,)), dma((n,)), dma((n,)), dma((n,)), dma((2,)), dma((pairs,)), dma((pairs + PAIR + 1,)), dma((6,)), pltpu.SemaphoreType.REGULAR,
            ],
            compiler_params=pltpu.CompilerParams(collective_id=0, has_side_effects=True, vmem_limit_bytes=VMEM_LIMIT),
        )(
            start_pos, freq, hidden_in, k_heads.reshape(-1, slots, hd), v_heads.reshape(-1, slots, hd), attn_norm,
            w_q, w_k, w_v, q_norm.reshape(1, -1), k_norm.reshape(1, -1), w_o, mlp_norm, w_gate, w_up, w_down,
        )
        return pl.pallas_call(
            store_kernel,
            name="store",
            out_shape=(
                jax.ShapeDtypeStruct(hidden_in.shape, BF16), jax.ShapeDtypeStruct(cache, BF16), jax.ShapeDtypeStruct(cache, BF16),
                pltpu.VMEM(cache, BF16), pltpu.VMEM(cache, BF16),
            ),
            in_specs=[smem] + [vmem] * 5,
            out_specs=(hbm,) * 3 + (vmem,) * 2,
            input_output_aliases={2: 3, 3: 4},
            scratch_shapes=[dma, dma((2, rows))],
            compiler_params=pltpu.CompilerParams(vmem_limit_bytes=2**20),
        )(start_pos, out, k_all, v_all, k_new, v_new)[:3]

    return jax.shard_map(local_run, mesh=mesh, in_specs=(P("dp"), row_spec, cache_in, cache_in) + (P(),) * 11, out_specs=(row_spec, cache_out, cache_out), check_vma=False)
```

```python
import functools

import jax
import jax.numpy as jnp
import numpy as np
from jax import lax
from jax.experimental import pallas as pl
from jax.experimental.pallas import tpu as pltpu
from jax.sharding import PartitionSpec as P

EPS = 1e-6
THETA = 1000000.0
F32 = jnp.float32
BF16 = jnp.bfloat16
MESH = pl.DeviceIdType.MESH
TILE = 512
PAIR = 2
AWAY = 2
VMEM_LIMIT = 44 * 2**20
AHEAD = 4


def rms(values, gain):
    inv_rms = lax.rsqrt(jnp.mean(values * values, axis=-1, keepdims=True) + EPS)
    return values * inv_rms * gain


def layer_kernel(
    n, steps, rows, heads, hd,
    pos_ref, freq_hbm, hid_hbm, k_hbm, v_hbm, an_hbm, wq_hbm, wk_hbm, wv_hbm, qn_hbm, kn_hbm, wo_hbm, mn_hbm,
    wg_hbm, wu_hbm, wd_hbm,
    out_ref, ka_ref, va_ref,
    freq_ref, hid_ref, an_ref, qn_ref, kn_ref, mn_ref, hid_s, act_s, x1_s, acc_s, tmp_s, cs_s, sn_s, msg_s, msg_r, o_s, o_r, rk, rv, kbuf, vbuf, wbuf, ubuf, dbuf, mix_s, kmix_s, vmix_s, stage_s,
    wsem, usem, dsem, ksem, vsem, own_sem, msg_ss, msg_rs, o_ss, o_rs, bulk_s, krs, vrs, in_sem, ready, stage_sem,
):
    me = lax.axis_index("x")
    num = steps * rows
    q_per = heads // n
    pairs = rows // PAIR
    home = pairs - AWAY
    slots = k_hbm.shape[1]
    dim = hid_ref.shape[2]
    tall = PAIR * steps * q_per
    new = PAIR * steps
    barrier = pltpu.get_barrier_semaphore()

    chips = n // 2
    chip, core = me // 2, lax.rem(me, 2)

    def peer(o):
        return lax.rem(me + o, n)

    def away(hops, cross):
        return lax.rem(chip + hops, chips) * 2 + (1 - core if cross else core)

    near = [(0, True)] + [(hops, cross) for hops in (1, chips - 1) for cross in (False, True)]
    far = [(hops, cross) for hops in range(2, chips - 1) for cross in (False, True)]
    for to in near:
        pl.semaphore_signal(barrier, inc=1, device_id={"x": away(*to)}, device_id_type=MESH)

    small = [
        pltpu.make_async_copy(src, dst, in_sem.at[i])
        for i, (src, dst) in enumerate((
            (hid_hbm, hid_ref), (an_hbm, an_ref), (freq_hbm, freq_ref), (qn_hbm, qn_ref), (kn_hbm, kn_ref), (mn_hbm, mn_ref),
        ))
    ]
    for c in small:
        c.start()

    def cols(hbm, i):
        return hbm.at[:, pl.ds(pl.multiple_of(i * TILE, TILE), TILE)]

    def load(src, dst, sem, slot):
        return pltpu.make_async_copy(src, dst.at[slot], sem.at[slot])

    staged = [
        pltpu.make_async_copy(k_hbm.at[away(*to) * rows], stage_s.at[i], stage_sem.at[i]) for i, to in enumerate(near[1:])
    ]
    for c in staged:
        c.start()
    load(cols(wq_hbm, 0), wbuf, wsem, 0).start()
    pl.semaphore_wait(barrier, len(near))
    pl.semaphore_signal(ready, inc=1, device_id={"x": away(chips - 1, False)}, device_id_type=MESH)

    def send(which, sem, first, count, lo, size, order):
        for hops, cross in order:
            to = away(hops, cross)
            pltpu.make_async_remote_copy(
                src_ref=(k_hbm, v_hbm)[which].at[pl.ds(to * rows + first, count), pl.ds(lo, size)],
                dst_ref=(rk, rv)[which].at[me, pl.ds(first, count), pl.ds(lo, size)],
                send_sem=bulk_s.at[which], recv_sem=(krs, vrs)[which].at[sem], device_id={"x": to}, device_id_type=MESH,
            ).start()

    mixed_order = [(1, False), (chips - 1, False)] + far[:1] + [(1, True), (chips - 1, True)] + far[1:] + [(0, True)]
    far_first = far + [(1, False), (chips - 1, False), (1, True), (chips - 1, True), (0, True)]
    last = [(0, pairs - 1, rows - PAIR, PAIR, 0, slots)]
    last += [(1, pairs - 1 + e, rows - PAIR + e, 1, 0, slots) for e in range(PAIR - 1)]
    for i, (lo, size) in enumerate(((0, slots // 2), (slots // 2, slots // 4), (slots * 3 // 4, slots // 4))):
        last.append((1, pairs - 2 + PAIR + i, rows - 1, 1, lo, size))

    def bulk(r):
        send(0, r, r * PAIR, PAIR, 0, slots, mixed_order)
        send(1, r, r * PAIR, PAIR, 0, slots, mixed_order)

    def bulk_last():
        for which, sem, first, count, lo, size in last:
            send(which, sem, first, count, lo, size, far_first)

    def bulk_next(r):
        @pl.when(r < pairs - 1)
        def _():
            bulk(r)

        @pl.when(r == pairs - 1)
        def _():
            bulk_last()

    def bulk_wait(which, sem, count, size):
        whole = (rk, rv)[which].at[pl.ds(0, n - 1), pl.ds(0, count), pl.ds(0, size)]
        pltpu.make_async_copy(whole, whole, (krs, vrs)[which].at[sem]).wait()

    for i, to in enumerate(near[1:]):
        staged[i].wait()
        pltpu.make_async_remote_copy(
            src_ref=stage_s.at[i], dst_ref=rk.at[me, 0], send_sem=bulk_s.at[0], recv_sem=krs.at[0],
            device_id={"x": away(*to)}, device_id_type=MESH,
        ).start()
    send(0, 0, 1, PAIR - 1, 0, slots, near[1:])
    send(0, 0, 0, PAIR, 0, slots, near[:1])
    pl.semaphore_wait(ready, 1)
    send(0, 0, 0, PAIR, 0, slots, far)
    send(1, 0, 0, PAIR, 0, slots, mixed_order)
    bulk(1)

    own = [
        pltpu.make_async_copy(k_hbm.at[pl.ds(me * rows, rows)], rk.at[me], own_sem.at[0]),
        pltpu.make_async_copy(v_hbm.at[pl.ds(me * rows, rows)], rv.at[me], own_sem.at[1]),
    ]

    def stream(hbm, body, started=False):
        tiles = hbm.shape[1] // TILE
        if not started:
            load(cols(hbm, 0), wbuf, wsem, 0).start()

        @pl.loop(0, tiles)
        def _(i):
            slot = lax.rem(i, 2)

            @pl.when(i + 1 < tiles)
            def _():
                load(cols(hbm, i + 1), wbuf, wsem, 1 - slot).start()

            load(cols(hbm, i), wbuf, wsem, slot).wait()
            body(i, wbuf[slot])

    for c in small:
        c.wait()
    for c in range(0, dim, hd):
        for s in range(steps):
            tmp_s[pl.ds(s, rows, stride=steps), :] = hid_ref[s, :, c : c + hd].astype(F32)
        hid_s[:, c : c + hd] = tmp_s[...]
    act_s[...] = rms(hid_s[...], an_ref[...].astype(F32).reshape(1, dim)).astype(BF16)

    row = lax.broadcasted_iota(jnp.int32, (num, hd), 0)
    pos = jnp.zeros((num, hd), jnp.int32)
    for b in range(rows):
        pos = jnp.where(row // steps == b, pos_ref[me * rows + b], pos)
    angles = (pos + row % steps).astype(F32) * freq_ref[...]
    lane = lax.broadcasted_iota(jnp.int32, (num, hd), 1)
    cs_s[...] = jnp.cos(angles)
    sn_s[...] = jnp.where(lane < hd // 2, -jnp.sin(angles), jnp.sin(angles))

    def rotate(v):
        return v * cs_s[...] + pltpu.roll(v, hd // 2, 1) * sn_s[...]

    per_tile = TILE // hd

    def q_tile(i, w):
        y = jnp.dot(act_s[...], w, preferred_element_type=F32)
        gain = qn_ref[...].astype(F32)
        for g in range(per_tile // q_per):
            parts = []
            for j in range(q_per):
                c = (g * q_per + j) * hd
                head = rotate(rms(y[:, c : c + hd], gain))
                parts.append(head.reshape(pairs, new, hd))
            msg_s[i * (per_tile // q_per) + g, :, 0:tall, :] = jnp.concatenate(parts, axis=1).astype(BF16)

    def k_tile(i, w):
        y = jnp.dot(act_s[...], w, preferred_element_type=F32)
        gain = kn_ref[...].astype(F32)
        for g in range(per_tile):
            head = rotate(rms(y[:, g * hd : (g + 1) * hd], gain))
            msg_s[i * per_tile + g, :, tall : tall + new, :] = head.reshape(pairs, new, hd).astype(BF16)
            kmix_s[pl.ds(i * per_tile + g, num, stride=n), :] = head

    def v_tile(i, w):
        y = jnp.dot(act_s[...], w, preferred_element_type=F32)
        for g in range(per_tile):
            head = y[:, g * hd : (g + 1) * hd]
            msg_s[i * per_tile + g, :, tall + new : tall + 2 * new, :] = head.reshape(pairs, new, hd).astype(BF16)
            vmix_s[pl.ds(i * per_tile + g, num, stride=n), :] = head

    stream(wq_hbm, q_tile, started=True)
    stream(wk_hbm, k_tile)
    stream(wv_hbm, v_tile)

    def msg_copy(to):
        return pltpu.make_async_remote_copy(
            src_ref=msg_s.at[to, pl.ds(home, AWAY)], dst_ref=msg_r.at[me], send_sem=msg_ss.at[to], recv_sem=msg_rs.at[me],
            device_id={"x": to}, device_id_type=MESH,
        )

    def msg_arrival(source):
        return pltpu.make_async_remote_copy(
            src_ref=msg_s.at[source, pl.ds(home, AWAY)], dst_ref=msg_r.at[source], send_sem=msg_ss.at[source],
            recv_sem=msg_rs.at[source], device_id={"x": source}, device_id_type=MESH,
        )

    def o_copy(to):
        return pltpu.make_async_remote_copy(
            src_ref=o_s.at[to], dst_ref=o_r.at[me, pl.ds(home, AWAY)], send_sem=o_ss.at[to], recv_sem=o_rs.at[me],
            device_id={"x": to}, device_id_type=MESH,
        )

    def o_arrival(source):
        return pltpu.make_async_remote_copy(
            src_ref=o_s.at[source], dst_ref=o_r.at[source, pl.ds(home, AWAY)], send_sem=o_ss.at[source], recv_sem=o_rs.at[source],
            device_id={"x": source}, device_id_type=MESH,
        )

    def kv_load(o, slot):
        first = peer(o) * rows + home * PAIR
        return (
            pltpu.make_async_copy(k_hbm.at[pl.ds(first, AWAY * PAIR)], kbuf.at[slot], ksem.at[slot]),
            pltpu.make_async_copy(v_hbm.at[pl.ds(first, AWAY * PAIR)], vbuf.at[slot], vsem.at[slot]),
        )

    for c in kv_load(0, 0):
        c.start()
    for c in own:
        c.start()
    msg_r[me] = msg_s[me, home:pairs]
    for o in range(1, n):
        msg_copy(peer(o)).start()
    for r in range(2, AHEAD):
        bulk(r)

    scale = hd ** -0.5
    nt = (((1,), (1,)), ((), ()))
    r_new = lax.broadcasted_iota(jnp.int32, (tall, new), 0) % new
    c_new = lax.broadcasted_iota(jnp.int32, (tall, new), 1)
    new_ok = (c_new // steps == r_new // steps) & (c_new % steps <= r_new % steps)
    in_pair = (lax.broadcasted_iota(jnp.int32, (tall, slots), 0) % new) // steps
    in_pair_o = (lax.broadcasted_iota(jnp.int32, (tall, hd), 0) % new) // steps
    t = lax.broadcasted_iota(jnp.int32, (tall, slots), 1)

    def attend(msg, keys, values, first):
        q = msg[0:tall]
        v_new = msg[tall + new : tall + 2 * new]
        fresh = lax.dot_general(q, msg[tall : tall + new], nt, preferred_element_type=F32)
        fresh = jnp.where(new_ok, fresh * scale, -jnp.inf)
        old = lax.dot_general(q, keys(0), nt, preferred_element_type=F32)
        start = jnp.full((tall, slots), pos_ref[first], jnp.int32)
        for e in range(1, PAIR):
            other = lax.dot_general(q, keys(e), nt, preferred_element_type=F32)
            old = jnp.where(in_pair == e, other, old)
            start = jnp.where(in_pair == e, pos_ref[first + e], start)
        old = jnp.where(t < start, old * scale, -jnp.inf)
        peak = jnp.maximum(jnp.max(old, axis=-1, keepdims=True), jnp.max(fresh, axis=-1, keepdims=True))
        old = jnp.exp(old - peak)
        fresh = jnp.exp(fresh - peak)
        total = jnp.sum(old, axis=-1, keepdims=True) + jnp.sum(fresh, axis=-1, keepdims=True)
        weights = old.astype(BF16)
        mixed = jnp.dot(weights, values(0), preferred_element_type=F32)
        for e in range(1, PAIR):
            other = jnp.dot(weights, values(e), preferred_element_type=F32)
            mixed = jnp.where(in_pair_o == e, other, mixed)
        mixed = mixed + jnp.dot(fresh.astype(BF16), v_new, preferred_element_type=F32)
        return (mixed / total).astype(BF16)

    @pl.loop(0, n)
    def _(o):
        slot = lax.rem(o, 2)
        source = peer(o)

        @pl.when(o + 1 < n)
        def _():
            for c in kv_load(o + 1, 1 - slot):
                c.start()

        for c in kv_load(o, slot):
            c.wait()

        @pl.when(o > 0)
        def _():
            msg_arrival(source).wait_recv()

        for i in range(AWAY):
            o_s[source, i] = attend(
                msg_r[source, i], lambda e: kbuf[slot, i * PAIR + e], lambda e: vbuf[slot, i * PAIR + e],
                source * rows + (home + i) * PAIR,
            )

        @pl.when(o == 0)
        def _():
            o_r[me, home:pairs] = o_s[me]

        @pl.when(o > 1)
        def _():
            o_copy(peer(o - 1)).start()

    for c in own:
        c.wait()
    o_copy(peer(n - 1)).start()

    def place(which, first, count, lo=0, size=slots):
        src, dst = ((rk, ka_ref), (rv, va_ref))[which]

        @pl.loop(0, count)
        def _(e):
            for h in range(n):
                mix_s[pl.ds(h, size, stride=n), :] = src[h, first + e, lo : lo + size].astype(F32)
            mixed = mix_s[0 : size * n].reshape(size, n, hd)
            slot = lo + lax.broadcasted_iota(jnp.int32, (size, n, hd), 0)
            for s in range(steps):
                at = pl.multiple_of(((first + e) * steps + s) * n, n)
                fresh = (kmix_s, vmix_s)[which][pl.ds(at, n), :]
                mixed = jnp.where(slot == pos_ref[me * rows + first + e] + s, fresh[None], mixed)
            dst[first + e, lo : lo + size] = mixed.astype(BF16)

    @pl.loop(0, home)
    def _(r):
        bulk_wait(0, r, PAIR, slots)
        bulk_wait(1, r, PAIR, slots)
        bulk_next(r + AHEAD)
        place(0, r * PAIR, PAIR)
        place(1, r * PAIR, PAIR)

        @pl.loop(0, n)
        def _(h):
            o_r[h, r] = attend(
                msg_s[h, r], lambda e: rk[h, r * PAIR + e], lambda e: rv[h, r * PAIR + e], me * rows + r * PAIR
            )

    for o in range(1, n):
        o_arrival(peer(o)).wait_recv()
    for h in range(n):
        both = o_r[h].astype(F32)
        for j in range(q_per):
            head = both[:, j * new : (j + 1) * new, :].reshape(num, hd)
            act_s[:, (h * q_per + j) * hd : (h * q_per + j + 1) * hd] = head.astype(BF16)

    def wo_tile(i, w):
        at = pl.ds(pl.multiple_of(i * TILE, TILE), TILE)
        y = jnp.dot(act_s[...], w, preferred_element_type=F32)
        x1_s[:, at] = (hid_s[:, at] + y).astype(BF16).astype(F32)

    stream(wo_hbm, wo_tile)
    act_s[...] = rms(x1_s[...], mn_ref[...].astype(F32).reshape(1, dim)).astype(BF16)
    acc_s[...] = jnp.zeros_like(acc_s)
    tiles = wg_hbm.shape[1] // TILE

    def mlp_loads(i, slot):
        at = pl.ds(pl.multiple_of(i * TILE, TILE), TILE)
        return (
            load(cols(wg_hbm, i), wbuf, wsem, slot),
            load(cols(wu_hbm, i), ubuf, usem, slot),
            load(wd_hbm.at[at, :], dbuf, dsem, slot),
        )

    for c in mlp_loads(0, 0):
        c.start()

    @pl.loop(0, tiles)
    def _(i):
        slot = lax.rem(i, 2)

        @pl.when(i + 1 < tiles)
        def _():
            for c in mlp_loads(i + 1, 1 - slot):
                c.start()

        for c in mlp_loads(i, slot):
            c.wait()
        z = act_s[...]
        gate = jnp.dot(z, wbuf[slot], preferred_element_type=F32)
        up = jnp.dot(z, ubuf[slot], preferred_element_type=F32)
        g = (jax.nn.silu(gate) * up).astype(BF16)
        acc_s[...] += jnp.dot(g, dbuf[slot], preferred_element_type=F32)

    for c in range(0, dim, hd):
        tmp_s[...] = x1_s[:, c : c + hd] + acc_s[:, c : c + hd]
        for s in range(steps):
            out_ref[s, :, c : c + hd] = tmp_s[pl.ds(s, rows, stride=steps), :].astype(BF16)

    for o in range(1, n):
        msg_copy(peer(o)).wait_send()
        o_copy(peer(o)).wait_send()

    @pl.loop(home, pairs - 1)
    def _(r):
        for which in range(2):
            bulk_wait(which, r, PAIR, slots)
            place(which, r * PAIR, PAIR)

    for which, sem, first, count, lo, size in last:
        bulk_wait(which, sem, count, size)
        place(which, first, count, lo, size)

    for which, dst in enumerate((rk, rv)):
        whole = dst.at[pl.ds(0, n - 1)]
        pltpu.make_async_copy(whole, whole, bulk_s.at[which]).wait()


def store_kernel(hid_ref, ka_ref, va_ref, out_hbm, ko_hbm, vo_hbm, hid_sem, sems):
    copies = []
    for b in range(ka_ref.shape[0]):
        copies.append(pltpu.make_async_copy(ka_ref.at[b], ko_hbm.at[b], sems.at[0, b]))
        copies.append(pltpu.make_async_copy(va_ref.at[b], vo_hbm.at[b], sems.at[1, b]))
    copies.append(pltpu.make_async_copy(hid_ref, out_hbm, hid_sem))
    for c in copies:
        c.start()
    for c in copies:
        c.wait()


def solution(mesh):
    row_spec = P(None, ("dp", "x"), None)
    cache_in = P("dp", None, "x", None)
    cache_out = P(("dp", "x"), None, None, None)
    n = mesh.shape["x"]

    def local_run(start_pos, hidden_in, k_heads, v_heads, attn_norm, w_q, w_k, w_v, q_norm, k_norm, w_o, mlp_norm, w_gate, w_up, w_down):
        steps, rows, dim = hidden_in.shape
        slots, hd = k_heads.shape[1], k_heads.shape[3]
        heads = w_q.shape[1] // hd
        num = steps * rows
        pairs = rows // PAIR
        half = hd // 2
        inv_freq = np.power(np.float32(THETA), -np.arange(half, dtype=np.float32) * np.float32(2.0) / np.float32(hd))
        freq = jnp.asarray(np.concatenate([inv_freq, inv_freq])[None, :], F32)
        vmem = pl.BlockSpec(memory_space=pltpu.VMEM)
        hbm = pl.BlockSpec(memory_space=pltpu.HBM)
        smem = pl.BlockSpec(memory_space=pltpu.SMEM)
        tall, new = PAIR * steps * (heads // n), PAIR * steps
        dma = pltpu.SemaphoreType.DMA
        cache = (rows, slots, n, hd)
        blocks = pltpu.VMEM((n, rows, slots, hd), BF16)
        chunk = pltpu.VMEM((2, AWAY * PAIR, slots, hd), BF16)
        wide = pltpu.VMEM((num, dim), F32)
        head = pltpu.VMEM((num, hd), F32)
        arrived = (pltpu.VMEM(hidden_in.shape, BF16), pltpu.VMEM(cache, BF16), pltpu.VMEM(cache, BF16))
        held = pl.pallas_call(
            functools.partial(layer_kernel, n, steps, rows, heads, hd),
            name="layer",
            out_shape=arrived,
            in_specs=[smem] + [hbm] * 15,
            out_specs=(vmem,) * 3,
            scratch_shapes=[
                pltpu.VMEM(freq.shape, F32), pltpu.VMEM(hidden_in.shape, BF16), pltpu.VMEM((dim,), BF16),
                pltpu.VMEM((1, hd), BF16), pltpu.VMEM((1, hd), BF16), pltpu.VMEM((dim,), BF16),
                wide, pltpu.VMEM((num, dim), BF16), wide, wide, head, head, head,
                pltpu.VMEM((n, pairs, tall + 2 * new, hd), BF16), pltpu.VMEM((n, AWAY, tall + 2 * new, hd), BF16),
                pltpu.VMEM((n, AWAY, tall, hd), BF16), pltpu.VMEM((n, pairs, tall, hd), BF16),
                blocks, blocks, chunk, chunk,
                pltpu.VMEM((2, dim, TILE), BF16), pltpu.VMEM((2, dim, TILE), BF16), pltpu.VMEM((2, TILE, dim), BF16),
                pltpu.VMEM((slots * n, hd), F32), pltpu.VMEM((num * n, hd), F32), pltpu.VMEM((num * n, hd), F32),
                pltpu.VMEM((4, slots, hd), BF16),
                dma((2,)), dma((2,)), dma((2,)), dma((2,)), dma((2,)), dma((2,)),
                dma((n,)), dma((n,)), dma((n,)), dma((n,)), dma((2,)), dma((pairs,)), dma((pairs + PAIR + 1,)), dma((6,)), pltpu.SemaphoreType.REGULAR, dma((4,)),
            ],
            compiler_params=pltpu.CompilerParams(collective_id=0, has_side_effects=True, vmem_limit_bytes=VMEM_LIMIT),
        )(
            start_pos, freq, hidden_in, k_heads.reshape(-1, slots, hd), v_heads.reshape(-1, slots, hd), attn_norm,
            w_q, w_k, w_v, q_norm.reshape(1, -1), k_norm.reshape(1, -1), w_o, mlp_norm, w_gate, w_up, w_down,
        )
        return pl.pallas_call(
            store_kernel,
            name="store",
            out_shape=tuple(jax.ShapeDtypeStruct(a.shape, BF16) for a in (hidden_in, held[1], held[2])),
            in_specs=[vmem] * 3,
            out_specs=(hbm,) * 3,
            scratch_shapes=[dma, dma((2, rows))],
            compiler_params=pltpu.CompilerParams(vmem_limit_bytes=2**20),
        )(*held)

    return jax.shard_map(local_run, mesh=mesh, in_specs=(P("dp"), row_spec, cache_in, cache_in) + (P(),) * 11, out_specs=(row_spec, cache_out, cache_out), check_vma=False)
```

```python
import functools

import jax
import jax.numpy as jnp
import numpy as np
from jax import lax
from jax.experimental import pallas as pl
from jax.experimental.pallas import tpu as pltpu
from jax.sharding import PartitionSpec as P

EPS = 1e-6
THETA = 1000000.0
F32 = jnp.float32
BF16 = jnp.bfloat16
MESH = pl.DeviceIdType.MESH
TILE = 512
PAIR = 2
AWAY = 2
VMEM_LIMIT = 44 * 2**20
UNIT = 4
AHEAD = 2


def rms(values, gain):
    inv_rms = lax.rsqrt(jnp.mean(values * values, axis=-1, keepdims=True) + EPS)
    return values * inv_rms * gain


def layer_kernel(
    n, steps, rows, heads, hd,
    pos_ref, freq_hbm, hid_hbm, k_hbm, v_hbm, an_hbm, wq_hbm, wk_hbm, wv_hbm, qn_hbm, kn_hbm, wo_hbm, mn_hbm,
    wg_hbm, wu_hbm, wd_hbm,
    out_ref, ka_ref, va_ref,
    freq_ref, hid_ref, an_ref, qn_ref, kn_ref, mn_ref, hid_s, act_s, x1_s, acc_s, tmp_s, cs_s, sn_s, msg_s, msg_r, o_s, o_r, rk, rv, kbuf, vbuf, wbuf, ubuf, dbuf, mix_s, kmix_s, vmix_s, stage_s,
    wsem, usem, dsem, ksem, vsem, own_sem, msg_ss, msg_rs, o_ss, o_rs, bulk_s, krs, vrs, in_sem, ready, stage_sem,
):
    me = lax.axis_index("x")
    num = steps * rows
    q_per = heads // n
    pairs = rows // PAIR
    home = pairs - AWAY
    rounds = rows // UNIT
    per_unit = UNIT // PAIR
    slots = k_hbm.shape[1]
    dim = hid_ref.shape[2]
    tall = PAIR * steps * q_per
    new = PAIR * steps
    barrier = pltpu.get_barrier_semaphore()

    chips = n // 2
    chip, core = me // 2, lax.rem(me, 2)

    def peer(o):
        return lax.rem(me + o, n)

    def away(hops, cross):
        return lax.rem(chip + hops, chips) * 2 + (1 - core if cross else core)

    near = [(0, True)] + [(hops, cross) for hops in (1, chips - 1) for cross in (False, True)]
    far = [(hops, cross) for hops in range(2, chips - 1) for cross in (False, True)]
    for to in near:
        pl.semaphore_signal(barrier, inc=1, device_id={"x": away(*to)}, device_id_type=MESH)

    small = [
        pltpu.make_async_copy(src, dst, in_sem.at[i])
        for i, (src, dst) in enumerate((
            (hid_hbm, hid_ref), (an_hbm, an_ref), (freq_hbm, freq_ref), (qn_hbm, qn_ref), (kn_hbm, kn_ref), (mn_hbm, mn_ref),
        ))
    ]
    for c in small:
        c.start()

    def cols(hbm, i):
        return hbm.at[:, pl.ds(pl.multiple_of(i * TILE, TILE), TILE)]

    def load(src, dst, sem, slot):
        return pltpu.make_async_copy(src, dst.at[slot], sem.at[slot])

    staged = [
        pltpu.make_async_copy(k_hbm.at[away(*to) * rows], stage_s.at[i], stage_sem.at[i]) for i, to in enumerate(near[1:])
    ]
    for c in staged:
        c.start()
    load(cols(wq_hbm, 0), wbuf, wsem, 0).start()
    pl.semaphore_wait(barrier, len(near))
    pl.semaphore_signal(ready, inc=1, device_id={"x": away(chips - 1, False)}, device_id_type=MESH)

    def send(which, sem, first, count, lo, size, order):
        for hops, cross in order:
            to = away(hops, cross)
            pltpu.make_async_remote_copy(
                src_ref=(k_hbm, v_hbm)[which].at[pl.ds(to * rows + first, count), pl.ds(lo, size)],
                dst_ref=(rk, rv)[which].at[me, pl.ds(first, count), pl.ds(lo, size)],
                send_sem=bulk_s.at[which], recv_sem=(krs, vrs)[which].at[sem], device_id={"x": to}, device_id_type=MESH,
            ).start()

    mixed_order = [(1, False), (chips - 1, False)] + far[:1] + [(1, True), (chips - 1, True)] + far[1:] + [(0, True)]
    far_first = far + [(1, False), (chips - 1, False), (1, True), (chips - 1, True), (0, True)]
    last = [(0, rounds - 1, rows - UNIT, UNIT, 0, slots), (1, rounds - 1, rows - UNIT, UNIT - 2, 0, slots)]
    last.append((1, rounds, rows - 2, 1, 0, slots))
    for i, (lo, size) in enumerate(((0, slots // 2), (slots // 2, slots // 4), (slots * 3 // 4, slots // 4))):
        last.append((1, rounds + 1 + i, rows - 1, 1, lo, size))

    def bulk(r):
        send(0, r, r * UNIT, UNIT, 0, slots, mixed_order)
        send(1, r, r * UNIT, UNIT, 0, slots, mixed_order)

    def bulk_last():
        for which, sem, first, count, lo, size in last:
            send(which, sem, first, count, lo, size, far_first)

    def bulk_next(r):
        @pl.when(r < rounds - 1)
        def _():
            bulk(r)

        @pl.when(r == rounds - 1)
        def _():
            bulk_last()

    def bulk_wait(which, sem, count, size):
        whole = (rk, rv)[which].at[pl.ds(0, n - 1), pl.ds(0, count), pl.ds(0, size)]
        pltpu.make_async_copy(whole, whole, (krs, vrs)[which].at[sem]).wait()

    for i, to in enumerate(near[1:]):
        staged[i].wait()
        pltpu.make_async_remote_copy(
            src_ref=stage_s.at[i], dst_ref=rk.at[me, 0], send_sem=bulk_s.at[0], recv_sem=krs.at[0],
            device_id={"x": away(*to)}, device_id_type=MESH,
        ).start()
    send(0, 0, 1, UNIT - 1, 0, slots, near[1:])
    send(0, 0, 0, UNIT, 0, slots, near[:1])
    pl.semaphore_wait(ready, 1)
    send(0, 0, 0, UNIT, 0, slots, far)
    send(1, 0, 0, UNIT, 0, slots, mixed_order)

    own = [
        pltpu.make_async_copy(k_hbm.at[pl.ds(me * rows, rows)], rk.at[me], own_sem.at[0]),
        pltpu.make_async_copy(v_hbm.at[pl.ds(me * rows, rows)], rv.at[me], own_sem.at[1]),
    ]

    def stream(hbm, body, started=False):
        tiles = hbm.shape[1] // TILE
        if not started:
            load(cols(hbm, 0), wbuf, wsem, 0).start()

        @pl.loop(0, tiles)
        def _(i):
            slot = lax.rem(i, 2)

            @pl.when(i + 1 < tiles)
            def _():
                load(cols(hbm, i + 1), wbuf, wsem, 1 - slot).start()

            load(cols(hbm, i), wbuf, wsem, slot).wait()
            body(i, wbuf[slot])

    for c in small:
        c.wait()
    for c in range(0, dim, hd):
        for s in range(steps):
            tmp_s[pl.ds(s, rows, stride=steps), :] = hid_ref[s, :, c : c + hd].astype(F32)
        hid_s[:, c : c + hd] = tmp_s[...]
    act_s[...] = rms(hid_s[...], an_ref[...].astype(F32).reshape(1, dim)).astype(BF16)

    row = lax.broadcasted_iota(jnp.int32, (num, hd), 0)
    pos = jnp.zeros((num, hd), jnp.int32)
    for b in range(rows):
        pos = jnp.where(row // steps == b, pos_ref[me * rows + b], pos)
    angles = (pos + row % steps).astype(F32) * freq_ref[...]
    lane = lax.broadcasted_iota(jnp.int32, (num, hd), 1)
    cs_s[...] = jnp.cos(angles)
    sn_s[...] = jnp.where(lane < hd // 2, -jnp.sin(angles), jnp.sin(angles))

    def rotate(v):
        return v * cs_s[...] + pltpu.roll(v, hd // 2, 1) * sn_s[...]

    per_tile = TILE // hd

    def q_tile(i, w):
        y = jnp.dot(act_s[...], w, preferred_element_type=F32)
        gain = qn_ref[...].astype(F32)
        for g in range(per_tile // q_per):
            parts = []
            for j in range(q_per):
                c = (g * q_per + j) * hd
                head = rotate(rms(y[:, c : c + hd], gain))
                parts.append(head.reshape(pairs, new, hd))
            msg_s[i * (per_tile // q_per) + g, :, 0:tall, :] = jnp.concatenate(parts, axis=1).astype(BF16)

    def k_tile(i, w):
        y = jnp.dot(act_s[...], w, preferred_element_type=F32)
        gain = kn_ref[...].astype(F32)
        for g in range(per_tile):
            head = rotate(rms(y[:, g * hd : (g + 1) * hd], gain))
            msg_s[i * per_tile + g, :, tall : tall + new, :] = head.reshape(pairs, new, hd).astype(BF16)
            kmix_s[pl.ds(i * per_tile + g, num, stride=n), :] = head

    def v_tile(i, w):
        y = jnp.dot(act_s[...], w, preferred_element_type=F32)
        for g in range(per_tile):
            head = y[:, g * hd : (g + 1) * hd]
            msg_s[i * per_tile + g, :, tall + new : tall + 2 * new, :] = head.reshape(pairs, new, hd).astype(BF16)
            vmix_s[pl.ds(i * per_tile + g, num, stride=n), :] = head

    stream(wq_hbm, q_tile, started=True)
    stream(wk_hbm, k_tile)
    stream(wv_hbm, v_tile)

    def msg_copy(to):
        return pltpu.make_async_remote_copy(
            src_ref=msg_s.at[to, pl.ds(home, AWAY)], dst_ref=msg_r.at[me], send_sem=msg_ss.at[to], recv_sem=msg_rs.at[me],
            device_id={"x": to}, device_id_type=MESH,
        )

    def msg_arrival(source):
        return pltpu.make_async_remote_copy(
            src_ref=msg_s.at[source, pl.ds(home, AWAY)], dst_ref=msg_r.at[source], send_sem=msg_ss.at[source],
            recv_sem=msg_rs.at[source], device_id={"x": source}, device_id_type=MESH,
        )

    def o_copy(to):
        return pltpu.make_async_remote_copy(
            src_ref=o_s.at[to], dst_ref=o_r.at[me, pl.ds(home, AWAY)], send_sem=o_ss.at[to], recv_sem=o_rs.at[me],
            device_id={"x": to}, device_id_type=MESH,
        )

    def o_arrival(source):
        return pltpu.make_async_remote_copy(
            src_ref=o_s.at[source], dst_ref=o_r.at[source, pl.ds(home, AWAY)], send_sem=o_ss.at[source], recv_sem=o_rs.at[source],
            device_id={"x": source}, device_id_type=MESH,
        )

    def kv_load(o, slot):
        first = peer(o) * rows + home * PAIR
        return (
            pltpu.make_async_copy(k_hbm.at[pl.ds(first, AWAY * PAIR)], kbuf.at[slot], ksem.at[slot]),
            pltpu.make_async_copy(v_hbm.at[pl.ds(first, AWAY * PAIR)], vbuf.at[slot], vsem.at[slot]),
        )

    for c in kv_load(0, 0):
        c.start()
    for c in own:
        c.start()
    msg_r[me] = msg_s[me, home:pairs]
    for o in range(1, n):
        msg_copy(peer(o)).start()
    for r in range(1, AHEAD):
        bulk(r)

    scale = hd ** -0.5
    nt = (((1,), (1,)), ((), ()))
    r_new = lax.broadcasted_iota(jnp.int32, (tall, new), 0) % new
    c_new = lax.broadcasted_iota(jnp.int32, (tall, new), 1)
    new_ok = (c_new // steps == r_new // steps) & (c_new % steps <= r_new % steps)
    in_pair = (lax.broadcasted_iota(jnp.int32, (tall, slots), 0) % new) // steps
    in_pair_o = (lax.broadcasted_iota(jnp.int32, (tall, hd), 0) % new) // steps
    t = lax.broadcasted_iota(jnp.int32, (tall, slots), 1)

    def attend(msg, keys, values, first):
        q = msg[0:tall]
        v_new = msg[tall + new : tall + 2 * new]
        fresh = lax.dot_general(q, msg[tall : tall + new], nt, preferred_element_type=F32)
        fresh = jnp.where(new_ok, fresh * scale, -jnp.inf)
        old = lax.dot_general(q, keys(0), nt, preferred_element_type=F32)
        start = jnp.full((tall, slots), pos_ref[first], jnp.int32)
        for e in range(1, PAIR):
            other = lax.dot_general(q, keys(e), nt, preferred_element_type=F32)
            old = jnp.where(in_pair == e, other, old)
            start = jnp.where(in_pair == e, pos_ref[first + e], start)
        old = jnp.where(t < start, old * scale, -jnp.inf)
        peak = jnp.maximum(jnp.max(old, axis=-1, keepdims=True), jnp.max(fresh, axis=-1, keepdims=True))
        old = jnp.exp(old - peak)
        fresh = jnp.exp(fresh - peak)
        total = jnp.sum(old, axis=-1, keepdims=True) + jnp.sum(fresh, axis=-1, keepdims=True)
        weights = old.astype(BF16)
        mixed = jnp.dot(weights, values(0), preferred_element_type=F32)
        for e in range(1, PAIR):
            other = jnp.dot(weights, values(e), preferred_element_type=F32)
            mixed = jnp.where(in_pair_o == e, other, mixed)
        mixed = mixed + jnp.dot(fresh.astype(BF16), v_new, preferred_element_type=F32)
        return (mixed / total).astype(BF16)

    @pl.loop(0, n)
    def _(o):
        slot = lax.rem(o, 2)
        source = peer(o)

        @pl.when(o + 1 < n)
        def _():
            for c in kv_load(o + 1, 1 - slot):
                c.start()

        for c in kv_load(o, slot):
            c.wait()

        @pl.when(o > 0)
        def _():
            msg_arrival(source).wait_recv()

        for i in range(AWAY):
            o_s[source, i] = attend(
                msg_r[source, i], lambda e: kbuf[slot, i * PAIR + e], lambda e: vbuf[slot, i * PAIR + e],
                source * rows + (home + i) * PAIR,
            )

        @pl.when(o == 0)
        def _():
            o_r[me, home:pairs] = o_s[me]

        @pl.when(o > 1)
        def _():
            o_copy(peer(o - 1)).start()

    for c in own:
        c.wait()
    o_copy(peer(n - 1)).start()

    def place(which, first, count, lo=0, size=slots):
        src, dst = ((rk, ka_ref), (rv, va_ref))[which]

        @pl.loop(0, count)
        def _(e):
            for h in range(n):
                mix_s[pl.ds(h, size, stride=n), :] = src[h, first + e, lo : lo + size].astype(F32)
            mixed = mix_s[0 : size * n].reshape(size, n, hd)
            slot = lo + lax.broadcasted_iota(jnp.int32, (size, n, hd), 0)
            for s in range(steps):
                at = pl.multiple_of(((first + e) * steps + s) * n, n)
                fresh = (kmix_s, vmix_s)[which][pl.ds(at, n), :]
                mixed = jnp.where(slot == pos_ref[me * rows + first + e] + s, fresh[None], mixed)
            dst[first + e, lo : lo + size] = mixed.astype(BF16)

    @pl.loop(0, home // per_unit)
    def _(r):
        bulk_wait(0, r, UNIT, slots)
        bulk_wait(1, r, UNIT, slots)
        bulk_next(r + AHEAD)
        place(0, r * UNIT, UNIT)
        place(1, r * UNIT, UNIT)

        @pl.loop(0, n)
        def _(h):
            for i in range(per_unit):
                b = r * UNIT + i * PAIR
                o_r[h, r * per_unit + i] = attend(
                    msg_s[h, r * per_unit + i], lambda e: rk[h, b + e], lambda e: rv[h, b + e], me * rows + b
                )

    for o in range(1, n):
        o_arrival(peer(o)).wait_recv()
    for h in range(n):
        both = o_r[h].astype(F32)
        for j in range(q_per):
            head = both[:, j * new : (j + 1) * new, :].reshape(num, hd)
            act_s[:, (h * q_per + j) * hd : (h * q_per + j + 1) * hd] = head.astype(BF16)

    def wo_tile(i, w):
        at = pl.ds(pl.multiple_of(i * TILE, TILE), TILE)
        y = jnp.dot(act_s[...], w, preferred_element_type=F32)
        x1_s[:, at] = (hid_s[:, at] + y).astype(BF16).astype(F32)

    stream(wo_hbm, wo_tile)
    act_s[...] = rms(x1_s[...], mn_ref[...].astype(F32).reshape(1, dim)).astype(BF16)
    acc_s[...] = jnp.zeros_like(acc_s)
    tiles = wg_hbm.shape[1] // TILE

    def mlp_loads(i, slot):
        at = pl.ds(pl.multiple_of(i * TILE, TILE), TILE)
        return (
            load(cols(wg_hbm, i), wbuf, wsem, slot),
            load(cols(wu_hbm, i), ubuf, usem, slot),
            load(wd_hbm.at[at, :], dbuf, dsem, slot),
        )

    for c in mlp_loads(0, 0):
        c.start()

    @pl.loop(0, tiles)
    def _(i):
        slot = lax.rem(i, 2)

        @pl.when(i + 1 < tiles)
        def _():
            for c in mlp_loads(i + 1, 1 - slot):
                c.start()

        for c in mlp_loads(i, slot):
            c.wait()
        z = act_s[...]
        gate = jnp.dot(z, wbuf[slot], preferred_element_type=F32)
        up = jnp.dot(z, ubuf[slot], preferred_element_type=F32)
        g = (jax.nn.silu(gate) * up).astype(BF16)
        acc_s[...] += jnp.dot(g, dbuf[slot], preferred_element_type=F32)

    for c in range(0, dim, hd):
        tmp_s[...] = x1_s[:, c : c + hd] + acc_s[:, c : c + hd]
        for s in range(steps):
            out_ref[s, :, c : c + hd] = tmp_s[pl.ds(s, rows, stride=steps), :].astype(BF16)

    for o in range(1, n):
        msg_copy(peer(o)).wait_send()
        o_copy(peer(o)).wait_send()

    for which, sem, first, count, lo, size in last:
        bulk_wait(which, sem, count, size)
        place(which, first, count, lo, size)

    for which, dst in enumerate((rk, rv)):
        whole = dst.at[pl.ds(0, n - 1)]
        pltpu.make_async_copy(whole, whole, bulk_s.at[which]).wait()


def store_kernel(hid_ref, ka_ref, va_ref, out_hbm, ko_hbm, vo_hbm, hid_sem, sems):
    copies = []
    for b in range(ka_ref.shape[0]):
        copies.append(pltpu.make_async_copy(ka_ref.at[b], ko_hbm.at[b], sems.at[0, b]))
        copies.append(pltpu.make_async_copy(va_ref.at[b], vo_hbm.at[b], sems.at[1, b]))
    copies.append(pltpu.make_async_copy(hid_ref, out_hbm, hid_sem))
    for c in copies:
        c.start()
    for c in copies:
        c.wait()


def solution(mesh):
    row_spec = P(None, ("dp", "x"), None)
    cache_in = P("dp", None, "x", None)
    cache_out = P(("dp", "x"), None, None, None)
    n = mesh.shape["x"]

    def local_run(start_pos, hidden_in, k_heads, v_heads, attn_norm, w_q, w_k, w_v, q_norm, k_norm, w_o, mlp_norm, w_gate, w_up, w_down):
        steps, rows, dim = hidden_in.shape
        slots, hd = k_heads.shape[1], k_heads.shape[3]
        heads = w_q.shape[1] // hd
        num = steps * rows
        pairs = rows // PAIR
        half = hd // 2
        inv_freq = np.power(np.float32(THETA), -np.arange(half, dtype=np.float32) * np.float32(2.0) / np.float32(hd))
        freq = jnp.asarray(np.concatenate([inv_freq, inv_freq])[None, :], F32)
        vmem = pl.BlockSpec(memory_space=pltpu.VMEM)
        hbm = pl.BlockSpec(memory_space=pltpu.HBM)
        smem = pl.BlockSpec(memory_space=pltpu.SMEM)
        tall, new = PAIR * steps * (heads // n), PAIR * steps
        dma = pltpu.SemaphoreType.DMA
        cache = (rows, slots, n, hd)
        blocks = pltpu.VMEM((n, rows, slots, hd), BF16)
        chunk = pltpu.VMEM((2, AWAY * PAIR, slots, hd), BF16)
        wide = pltpu.VMEM((num, dim), F32)
        head = pltpu.VMEM((num, hd), F32)
        arrived = (pltpu.VMEM(hidden_in.shape, BF16), pltpu.VMEM(cache, BF16), pltpu.VMEM(cache, BF16))
        held = pl.pallas_call(
            functools.partial(layer_kernel, n, steps, rows, heads, hd),
            name="layer",
            out_shape=arrived,
            in_specs=[smem] + [hbm] * 15,
            out_specs=(vmem,) * 3,
            scratch_shapes=[
                pltpu.VMEM(freq.shape, F32), pltpu.VMEM(hidden_in.shape, BF16), pltpu.VMEM((dim,), BF16),
                pltpu.VMEM((1, hd), BF16), pltpu.VMEM((1, hd), BF16), pltpu.VMEM((dim,), BF16),
                wide, pltpu.VMEM((num, dim), BF16), wide, wide, head, head, head,
                pltpu.VMEM((n, pairs, tall + 2 * new, hd), BF16), pltpu.VMEM((n, AWAY, tall + 2 * new, hd), BF16),
                pltpu.VMEM((n, AWAY, tall, hd), BF16), pltpu.VMEM((n, pairs, tall, hd), BF16),
                blocks, blocks, chunk, chunk,
                pltpu.VMEM((2, dim, TILE), BF16), pltpu.VMEM((2, dim, TILE), BF16), pltpu.VMEM((2, TILE, dim), BF16),
                pltpu.VMEM((slots * n, hd), F32), pltpu.VMEM((num * n, hd), F32), pltpu.VMEM((num * n, hd), F32),
                pltpu.VMEM((4, slots, hd), BF16),
                dma((2,)), dma((2,)), dma((2,)), dma((2,)), dma((2,)), dma((2,)),
                dma((n,)), dma((n,)), dma((n,)), dma((n,)), dma((2,)), dma((rows // UNIT,)), dma((rows // UNIT + 4,)), dma((6,)), pltpu.SemaphoreType.REGULAR, dma((4,)),
            ],
            compiler_params=pltpu.CompilerParams(collective_id=0, has_side_effects=True, vmem_limit_bytes=VMEM_LIMIT),
        )(
            start_pos, freq, hidden_in, k_heads.reshape(-1, slots, hd), v_heads.reshape(-1, slots, hd), attn_norm,
            w_q, w_k, w_v, q_norm.reshape(1, -1), k_norm.reshape(1, -1), w_o, mlp_norm, w_gate, w_up, w_down,
        )
        return pl.pallas_call(
            store_kernel,
            name="store",
            out_shape=tuple(jax.ShapeDtypeStruct(a.shape, BF16) for a in (hidden_in, held[1], held[2])),
            in_specs=[vmem] * 3,
            out_specs=(hbm,) * 3,
            scratch_shapes=[dma, dma((2, rows))],
            compiler_params=pltpu.CompilerParams(vmem_limit_bytes=2**20),
        )(*held)

    return jax.shard_map(local_run, mesh=mesh, in_specs=(P("dp"), row_spec, cache_in, cache_in) + (P(),) * 11, out_specs=(row_spec, cache_out, cache_out), check_vma=False)
```

```python
import functools

import jax
import jax.numpy as jnp
import numpy as np
from jax import lax
from jax.experimental import pallas as pl
from jax.experimental.pallas import tpu as pltpu
from jax.sharding import PartitionSpec as P

EPS = 1e-6
THETA = 1000000.0
F32 = jnp.float32
BF16 = jnp.bfloat16
MESH = pl.DeviceIdType.MESH
TILE = 512
PAIR = 2
AWAY = 2
VMEM_LIMIT = 44 * 2**20
AHEAD = 4


def rms(values, gain):
    inv_rms = lax.rsqrt(jnp.mean(values * values, axis=-1, keepdims=True) + EPS)
    return values * inv_rms * gain


def layer_kernel(
    n, steps, rows, heads, hd,
    pos_ref, freq_hbm, hid_hbm, k_hbm, v_hbm, an_hbm, wq_hbm, wk_hbm, wv_hbm, qn_hbm, kn_hbm, wo_hbm, mn_hbm,
    wg_hbm, wu_hbm, wd_hbm,
    out_ref, ka_ref, va_ref,
    freq_ref, hid_ref, an_ref, qn_ref, kn_ref, mn_ref, hid_s, act_s, x1_s, acc_s, tmp_s, cs_s, sn_s, msg_s, msg_r, o_s, o_r, rk, rv, kbuf, vbuf, wbuf, ubuf, dbuf, mix_s, kmix_s, vmix_s,
    wsem, usem, dsem, ksem, vsem, own_sem, msg_ss, msg_rs, o_ss, o_rs, bulk_s, krs, vrs, in_sem, ready,
):
    me = lax.axis_index("x")
    num = steps * rows
    q_per = heads // n
    pairs = rows // PAIR
    home = pairs - AWAY
    slots = k_hbm.shape[1]
    dim = hid_ref.shape[2]
    tall = PAIR * steps * q_per
    new = PAIR * steps
    barrier = pltpu.get_barrier_semaphore()

    chips = n // 2
    chip, core = me // 2, lax.rem(me, 2)

    def peer(o):
        return lax.rem(me + o, n)

    def away(hops, cross):
        return lax.rem(chip + hops, chips) * 2 + (1 - core if cross else core)

    near = [(0, True)] + [(hops, cross) for hops in (1, chips - 1) for cross in (False, True)]
    for to in near:
        pl.semaphore_signal(barrier, inc=1, device_id={"x": away(*to)}, device_id_type=MESH)

    small = [
        pltpu.make_async_copy(src, dst, in_sem.at[i])
        for i, (src, dst) in enumerate((
            (hid_hbm, hid_ref), (an_hbm, an_ref), (freq_hbm, freq_ref), (qn_hbm, qn_ref), (kn_hbm, kn_ref), (mn_hbm, mn_ref),
        ))
    ]
    for c in small:
        c.start()

    def cols(hbm, i):
        return hbm.at[:, pl.ds(pl.multiple_of(i * TILE, TILE), TILE)]

    def load(src, dst, sem, slot):
        return pltpu.make_async_copy(src, dst.at[slot], sem.at[slot])

    load(cols(wq_hbm, 0), wbuf, wsem, 0).start()
    pl.semaphore_wait(barrier, len(near))
    pl.semaphore_signal(ready, inc=1, device_id={"x": away(chips - 1, False)}, device_id_type=MESH)

    def send(which, sem, first, count, lo, size, targets):
        for hops, cross in targets:
            to = away(hops, cross)
            pltpu.make_async_remote_copy(
                src_ref=(k_hbm, v_hbm)[which].at[pl.ds(to * rows + first, count), pl.ds(lo, size)],
                dst_ref=(rk, rv)[which].at[me, pl.ds(first, count), pl.ds(lo, size)],
                send_sem=bulk_s.at[which], recv_sem=(krs, vrs)[which].at[sem], device_id={"x": to}, device_id_type=MESH,
            ).start()

    turn = core * (chips - 2)
    one_way, other_way = 1 + turn, chips - 1 - turn
    order = [(hops, cross) for cross in (False, True) for hops in [one_way, *range(2, chips - 1), other_way]] + [(0, True)]

    last = [(0, pairs - 1, rows - PAIR, PAIR, 0, slots)]
    last += [(1, pairs - 1 + e, rows - PAIR + e, 1, 0, slots) for e in range(PAIR - 1)]
    for i, (lo, size) in enumerate(((0, slots // 2), (slots // 2, slots // 4), (slots * 3 // 4, slots // 4))):
        last.append((1, pairs - 2 + PAIR + i, rows - 1, 1, lo, size))

    def bulk(r):
        send(0, r, r * PAIR, PAIR, 0, slots, order)
        send(1, r, r * PAIR, PAIR, 0, slots, order)

    def bulk_last():
        for which, sem, first, count, lo, size in last:
            send(which, sem, first, count, lo, size, order)

    def bulk_next(r):
        @pl.when(r < pairs - 1)
        def _():
            bulk(r)

        @pl.when(r == pairs - 1)
        def _():
            bulk_last()

    def bulk_wait(which, sem, count, size):
        whole = (rk, rv)[which].at[pl.ds(0, n - 1), pl.ds(0, count), pl.ds(0, size)]
        pltpu.make_async_copy(whole, whole, (krs, vrs)[which].at[sem]).wait()

    send(0, 0, 0, PAIR, 0, slots, order[:1])
    pl.semaphore_wait(ready, 1)
    send(0, 0, 0, PAIR, 0, slots, order[1:])
    send(1, 0, 0, PAIR, 0, slots, order)
    bulk(1)

    own = [
        pltpu.make_async_copy(k_hbm.at[pl.ds(me * rows, rows)], rk.at[me], own_sem.at[0]),
        pltpu.make_async_copy(v_hbm.at[pl.ds(me * rows, rows)], rv.at[me], own_sem.at[1]),
    ]

    def stream(hbm, body, started=False):
        tiles = hbm.shape[1] // TILE
        if not started:
            load(cols(hbm, 0), wbuf, wsem, 0).start()

        @pl.loop(0, tiles)
        def _(i):
            slot = lax.rem(i, 2)

            @pl.when(i + 1 < tiles)
            def _():
                load(cols(hbm, i + 1), wbuf, wsem, 1 - slot).start()

            load(cols(hbm, i), wbuf, wsem, slot).wait()
            body(i, wbuf[slot])

    for c in small:
        c.wait()
    for c in range(0, dim, hd):
        for s in range(steps):
            tmp_s[pl.ds(s, rows, stride=steps), :] = hid_ref[s, :, c : c + hd].astype(F32)
        hid_s[:, c : c + hd] = tmp_s[...]
    act_s[...] = rms(hid_s[...], an_ref[...].astype(F32).reshape(1, dim)).astype(BF16)

    row = lax.broadcasted_iota(jnp.int32, (num, hd), 0)
    pos = jnp.zeros((num, hd), jnp.int32)
    for b in range(rows):
        pos = jnp.where(row // steps == b, pos_ref[me * rows + b], pos)
    angles = (pos + row % steps).astype(F32) * freq_ref[...]
    lane = lax.broadcasted_iota(jnp.int32, (num, hd), 1)
    cs_s[...] = jnp.cos(angles)
    sn_s[...] = jnp.where(lane < hd // 2, -jnp.sin(angles), jnp.sin(angles))

    def rotate(v):
        return v * cs_s[...] + pltpu.roll(v, hd // 2, 1) * sn_s[...]

    per_tile = TILE // hd

    def q_tile(i, w):
        y = jnp.dot(act_s[...], w, preferred_element_type=F32)
        gain = qn_ref[...].astype(F32)
        for g in range(per_tile // q_per):
            parts = []
            for j in range(q_per):
                c = (g * q_per + j) * hd
                head = rotate(rms(y[:, c : c + hd], gain))
                parts.append(head.reshape(pairs, new, hd))
            msg_s[i * (per_tile // q_per) + g, :, 0:tall, :] = jnp.concatenate(parts, axis=1).astype(BF16)

    def k_tile(i, w):
        y = jnp.dot(act_s[...], w, preferred_element_type=F32)
        gain = kn_ref[...].astype(F32)
        for g in range(per_tile):
            head = rotate(rms(y[:, g * hd : (g + 1) * hd], gain))
            msg_s[i * per_tile + g, :, tall : tall + new, :] = head.reshape(pairs, new, hd).astype(BF16)
            kmix_s[pl.ds(i * per_tile + g, num, stride=n), :] = head

    def v_tile(i, w):
        y = jnp.dot(act_s[...], w, preferred_element_type=F32)
        for g in range(per_tile):
            head = y[:, g * hd : (g + 1) * hd]
            msg_s[i * per_tile + g, :, tall + new : tall + 2 * new, :] = head.reshape(pairs, new, hd).astype(BF16)
            vmix_s[pl.ds(i * per_tile + g, num, stride=n), :] = head

    stream(wq_hbm, q_tile, started=True)
    stream(wk_hbm, k_tile)
    stream(wv_hbm, v_tile)

    def msg_copy(to):
        return pltpu.make_async_remote_copy(
            src_ref=msg_s.at[to, pl.ds(home, AWAY)], dst_ref=msg_r.at[me], send_sem=msg_ss.at[to], recv_sem=msg_rs.at[me],
            device_id={"x": to}, device_id_type=MESH,
        )

    def msg_arrival(source):
        return pltpu.make_async_remote_copy(
            src_ref=msg_s.at[source, pl.ds(home, AWAY)], dst_ref=msg_r.at[source], send_sem=msg_ss.at[source],
            recv_sem=msg_rs.at[source], device_id={"x": source}, device_id_type=MESH,
        )

    def o_copy(to):
        return pltpu.make_async_remote_copy(
            src_ref=o_s.at[to], dst_ref=o_r.at[me, pl.ds(home, AWAY)], send_sem=o_ss.at[to], recv_sem=o_rs.at[me],
            device_id={"x": to}, device_id_type=MESH,
        )

    def o_arrival(source):
        return pltpu.make_async_remote_copy(
            src_ref=o_s.at[source], dst_ref=o_r.at[source, pl.ds(home, AWAY)], send_sem=o_ss.at[source], recv_sem=o_rs.at[source],
            device_id={"x": source}, device_id_type=MESH,
        )

    def kv_load(o, slot):
        first = peer(o) * rows + home * PAIR
        return (
            pltpu.make_async_copy(k_hbm.at[pl.ds(first, AWAY * PAIR)], kbuf.at[slot], ksem.at[slot]),
            pltpu.make_async_copy(v_hbm.at[pl.ds(first, AWAY * PAIR)], vbuf.at[slot], vsem.at[slot]),
        )

    for c in kv_load(0, 0):
        c.start()
    for c in own:
        c.start()
    msg_r[me] = msg_s[me, home:pairs]
    for o in range(1, n):
        msg_copy(peer(o)).start()
    for r in range(2, AHEAD):
        bulk(r)

    scale = hd ** -0.5
    nt = (((1,), (1,)), ((), ()))
    r_new = lax.broadcasted_iota(jnp.int32, (tall, new), 0) % new
    c_new = lax.broadcasted_iota(jnp.int32, (tall, new), 1)
    new_ok = (c_new // steps == r_new // steps) & (c_new % steps <= r_new % steps)
    in_pair = (lax.broadcasted_iota(jnp.int32, (tall, slots), 0) % new) // steps
    in_pair_o = (lax.broadcasted_iota(jnp.int32, (tall, hd), 0) % new) // steps
    t = lax.broadcasted_iota(jnp.int32, (tall, slots), 1)

    def attend(msg, keys, values, first):
        q = msg[0:tall]
        v_new = msg[tall + new : tall + 2 * new]
        fresh = lax.dot_general(q, msg[tall : tall + new], nt, preferred_element_type=F32)
        fresh = jnp.where(new_ok, fresh * scale, -jnp.inf)
        old = lax.dot_general(q, keys(0), nt, preferred_element_type=F32)
        start = jnp.full((tall, slots), pos_ref[first], jnp.int32)
        for e in range(1, PAIR):
            other = lax.dot_general(q, keys(e), nt, preferred_element_type=F32)
            old = jnp.where(in_pair == e, other, old)
            start = jnp.where(in_pair == e, pos_ref[first + e], start)
        old = jnp.where(t < start, old * scale, -jnp.inf)
        peak = jnp.maximum(jnp.max(old, axis=-1, keepdims=True), jnp.max(fresh, axis=-1, keepdims=True))
        old = jnp.exp(old - peak)
        fresh = jnp.exp(fresh - peak)
        total = jnp.sum(old, axis=-1, keepdims=True) + jnp.sum(fresh, axis=-1, keepdims=True)
        weights = old.astype(BF16)
        mixed = jnp.dot(weights, values(0), preferred_element_type=F32)
        for e in range(1, PAIR):
            other = jnp.dot(weights, values(e), preferred_element_type=F32)
            mixed = jnp.where(in_pair_o == e, other, mixed)
        mixed = mixed + jnp.dot(fresh.astype(BF16), v_new, preferred_element_type=F32)
        return (mixed / total).astype(BF16)

    @pl.loop(0, n)
    def _(o):
        slot = lax.rem(o, 2)
        source = peer(o)

        @pl.when(o + 1 < n)
        def _():
            for c in kv_load(o + 1, 1 - slot):
                c.start()

        for c in kv_load(o, slot):
            c.wait()

        @pl.when(o > 0)
        def _():
            msg_arrival(source).wait_recv()

        for i in range(AWAY):
            o_s[source, i] = attend(
                msg_r[source, i], lambda e: kbuf[slot, i * PAIR + e], lambda e: vbuf[slot, i * PAIR + e],
                source * rows + (home + i) * PAIR,
            )

        @pl.when(o == 0)
        def _():
            o_r[me, home:pairs] = o_s[me]

        @pl.when(o > 1)
        def _():
            o_copy(peer(o - 1)).start()

    for c in own:
        c.wait()
    o_copy(peer(n - 1)).start()

    def place(which, first, count, lo=0, size=slots):
        src, dst = ((rk, ka_ref), (rv, va_ref))[which]

        @pl.loop(0, count)
        def _(e):
            for h in range(n):
                mix_s[pl.ds(h, size, stride=n), :] = src[h, first + e, lo : lo + size].astype(F32)
            mixed = mix_s[0 : size * n].reshape(size, n, hd)
            slot = lo + lax.broadcasted_iota(jnp.int32, (size, n, hd), 0)
            for s in range(steps):
                at = pl.multiple_of(((first + e) * steps + s) * n, n)
                fresh = (kmix_s, vmix_s)[which][pl.ds(at, n), :]
                mixed = jnp.where(slot == pos_ref[me * rows + first + e] + s, fresh[None], mixed)
            dst[first + e, lo : lo + size] = mixed.astype(BF16)

    @pl.loop(0, home)
    def _(r):
        bulk_wait(0, r, PAIR, slots)
        bulk_wait(1, r, PAIR, slots)
        bulk_next(r + AHEAD)
        place(0, r * PAIR, PAIR)
        place(1, r * PAIR, PAIR)

        @pl.loop(0, n)
        def _(h):
            o_r[h, r] = attend(
                msg_s[h, r], lambda e: rk[h, r * PAIR + e], lambda e: rv[h, r * PAIR + e], me * rows + r * PAIR
            )

    for o in range(1, n):
        o_arrival(peer(o)).wait_recv()
    for h in range(n):
        both = o_r[h].astype(F32)
        for j in range(q_per):
            head = both[:, j * new : (j + 1) * new, :].reshape(num, hd)
            act_s[:, (h * q_per + j) * hd : (h * q_per + j + 1) * hd] = head.astype(BF16)

    def wo_tile(i, w):
        at = pl.ds(pl.multiple_of(i * TILE, TILE), TILE)
        y = jnp.dot(act_s[...], w, preferred_element_type=F32)
        x1_s[:, at] = (hid_s[:, at] + y).astype(BF16).astype(F32)

    stream(wo_hbm, wo_tile)
    act_s[...] = rms(x1_s[...], mn_ref[...].astype(F32).reshape(1, dim)).astype(BF16)
    acc_s[...] = jnp.zeros_like(acc_s)
    tiles = wg_hbm.shape[1] // TILE

    def mlp_loads(i, slot):
        at = pl.ds(pl.multiple_of(i * TILE, TILE), TILE)
        return (
            load(cols(wg_hbm, i), wbuf, wsem, slot),
            load(cols(wu_hbm, i), ubuf, usem, slot),
            load(wd_hbm.at[at, :], dbuf, dsem, slot),
        )

    for c in mlp_loads(0, 0):
        c.start()

    @pl.loop(0, tiles)
    def _(i):
        slot = lax.rem(i, 2)

        @pl.when(i + 1 < tiles)
        def _():
            for c in mlp_loads(i + 1, 1 - slot):
                c.start()

        for c in mlp_loads(i, slot):
            c.wait()
        z = act_s[...]
        gate = jnp.dot(z, wbuf[slot], preferred_element_type=F32)
        up = jnp.dot(z, ubuf[slot], preferred_element_type=F32)
        g = (jax.nn.silu(gate) * up).astype(BF16)
        acc_s[...] += jnp.dot(g, dbuf[slot], preferred_element_type=F32)

    for c in range(0, dim, hd):
        tmp_s[...] = x1_s[:, c : c + hd] + acc_s[:, c : c + hd]
        for s in range(steps):
            out_ref[s, :, c : c + hd] = tmp_s[pl.ds(s, rows, stride=steps), :].astype(BF16)

    for o in range(1, n):
        msg_copy(peer(o)).wait_send()
        o_copy(peer(o)).wait_send()

    @pl.loop(home, pairs - 1)
    def _(r):
        for which in range(2):
            bulk_wait(which, r, PAIR, slots)
            place(which, r * PAIR, PAIR)

    for which, sem, first, count, lo, size in last:
        bulk_wait(which, sem, count, size)
        place(which, first, count, lo, size)

    for which, dst in enumerate((rk, rv)):
        whole = dst.at[pl.ds(0, n - 1)]
        pltpu.make_async_copy(whole, whole, bulk_s.at[which]).wait()


def store_kernel(hid_ref, ka_ref, va_ref, out_hbm, ko_hbm, vo_hbm, hid_sem, sems):
    copies = []
    for b in range(ka_ref.shape[0]):
        copies.append(pltpu.make_async_copy(ka_ref.at[b], ko_hbm.at[b], sems.at[0, b]))
        copies.append(pltpu.make_async_copy(va_ref.at[b], vo_hbm.at[b], sems.at[1, b]))
    copies.append(pltpu.make_async_copy(hid_ref, out_hbm, hid_sem))
    for c in copies:
        c.start()
    for c in copies:
        c.wait()


def solution(mesh):
    row_spec = P(None, ("dp", "x"), None)
    cache_in = P("dp", None, "x", None)
    cache_out = P(("dp", "x"), None, None, None)
    n = mesh.shape["x"]

    def local_run(start_pos, hidden_in, k_heads, v_heads, attn_norm, w_q, w_k, w_v, q_norm, k_norm, w_o, mlp_norm, w_gate, w_up, w_down):
        steps, rows, dim = hidden_in.shape
        slots, hd = k_heads.shape[1], k_heads.shape[3]
        heads = w_q.shape[1] // hd
        num = steps * rows
        pairs = rows // PAIR
        half = hd // 2
        inv_freq = np.power(np.float32(THETA), -np.arange(half, dtype=np.float32) * np.float32(2.0) / np.float32(hd))
        freq = jnp.asarray(np.concatenate([inv_freq, inv_freq])[None, :], F32)
        vmem = pl.BlockSpec(memory_space=pltpu.VMEM)
        hbm = pl.BlockSpec(memory_space=pltpu.HBM)
        smem = pl.BlockSpec(memory_space=pltpu.SMEM)
        tall, new = PAIR * steps * (heads // n), PAIR * steps
        dma = pltpu.SemaphoreType.DMA
        cache = (rows, slots, n, hd)
        blocks = pltpu.VMEM((n, rows, slots, hd), BF16)
        chunk = pltpu.VMEM((2, AWAY * PAIR, slots, hd), BF16)
        wide = pltpu.VMEM((num, dim), F32)
        head = pltpu.VMEM((num, hd), F32)
        arrived = (pltpu.VMEM(hidden_in.shape, BF16), pltpu.VMEM(cache, BF16), pltpu.VMEM(cache, BF16))
        held = pl.pallas_call(
            functools.partial(layer_kernel, n, steps, rows, heads, hd),
            name="layer",
            out_shape=arrived,
            in_specs=[smem] + [hbm] * 15,
            out_specs=(vmem,) * 3,
            scratch_shapes=[
                pltpu.VMEM(freq.shape, F32), pltpu.VMEM(hidden_in.shape, BF16), pltpu.VMEM((dim,), BF16),
                pltpu.VMEM((1, hd), BF16), pltpu.VMEM((1, hd), BF16), pltpu.VMEM((dim,), BF16),
                wide, pltpu.VMEM((num, dim), BF16), wide, wide, head, head, head,
                pltpu.VMEM((n, pairs, tall + 2 * new, hd), BF16), pltpu.VMEM((n, AWAY, tall + 2 * new, hd), BF16),
                pltpu.VMEM((n, AWAY, tall, hd), BF16), pltpu.VMEM((n, pairs, tall, hd), BF16),
                blocks, blocks, chunk, chunk,
                pltpu.VMEM((2, dim, TILE), BF16), pltpu.VMEM((2, dim, TILE), BF16), pltpu.VMEM((2, TILE, dim), BF16),
                pltpu.VMEM((slots * n, hd), F32), pltpu.VMEM((num * n, hd), F32), pltpu.VMEM((num * n, hd), F32),
                dma((2,)), dma((2,)), dma((2,)), dma((2,)), dma((2,)), dma((2,)),
                dma((n,)), dma((n,)), dma((n,)), dma((n,)), dma((2,)), dma((pairs,)), dma((pairs + PAIR + 1,)), dma((6,)), pltpu.SemaphoreType.REGULAR,
            ],
            compiler_params=pltpu.CompilerParams(collective_id=0, has_side_effects=True, vmem_limit_bytes=VMEM_LIMIT),
        )(
            start_pos, freq, hidden_in, k_heads.reshape(-1, slots, hd), v_heads.reshape(-1, slots, hd), attn_norm,
            w_q, w_k, w_v, q_norm.reshape(1, -1), k_norm.reshape(1, -1), w_o, mlp_norm, w_gate, w_up, w_down,
        )
        return pl.pallas_call(
            store_kernel,
            name="store",
            out_shape=tuple(jax.ShapeDtypeStruct(a.shape, BF16) for a in (hidden_in, held[1], held[2])),
            in_specs=[vmem] * 3,
            out_specs=(hbm,) * 3,
            scratch_shapes=[dma, dma((2, rows))],
            compiler_params=pltpu.CompilerParams(vmem_limit_bytes=2**20),
        )(*held)

    return jax.shard_map(local_run, mesh=mesh, in_specs=(P("dp"), row_spec, cache_in, cache_in) + (P(),) * 11, out_specs=(row_spec, cache_out, cache_out), check_vma=False)
```

```python
import functools

import jax
import jax.numpy as jnp
import numpy as np
from jax import lax
from jax.experimental import pallas as pl
from jax.experimental.pallas import tpu as pltpu
from jax.sharding import PartitionSpec as P

EPS = 1e-6
THETA = 1000000.0
F32 = jnp.float32
BF16 = jnp.bfloat16
MESH = pl.DeviceIdType.MESH
TILE = 512
PAIR = 2
AWAY = 2
VMEM_LIMIT = 44 * 2**20
AHEAD = 4


def rms(values, gain):
    inv_rms = lax.rsqrt(jnp.mean(values * values, axis=-1, keepdims=True) + EPS)
    return values * inv_rms * gain


def layer_kernel(
    n, steps, rows, heads, hd,
    pos_hbm, freq_hbm, hid_hbm, k_hbm, v_hbm, an_hbm, wq_hbm, wk_hbm, wv_hbm, qn_hbm, kn_hbm, wo_hbm, mn_hbm,
    wg_hbm, wu_hbm, wd_hbm,
    out_ref, ka_ref, va_ref,
    pos_ref, freq_ref, hid_ref, an_ref, qn_ref, kn_ref, mn_ref, hid_s, act_s, x1_s, acc_s, tmp_s, cs_s, sn_s, msg_s, msg_r, o_s, o_r, rk, rv, kbuf, vbuf, wbuf, ubuf, dbuf, mix_s, kmix_s, vmix_s,
    wsem, usem, dsem, ksem, vsem, own_sem, msg_ss, msg_rs, o_ss, o_rs, bulk_s, krs, vrs, in_sem, ready,
):
    me = lax.axis_index("x")
    num = steps * rows
    q_per = heads // n
    pairs = rows // PAIR
    home = pairs - AWAY
    slots = k_hbm.shape[1]
    dim = hid_ref.shape[2]
    tall = PAIR * steps * q_per
    new = PAIR * steps
    barrier = pltpu.get_barrier_semaphore()

    chips = n // 2
    chip, core = me // 2, lax.rem(me, 2)

    def peer(o):
        return lax.rem(me + o, n)

    def away(hops, cross):
        return lax.rem(chip + hops, chips) * 2 + (1 - core if cross else core)

    near = [(0, True)] + [(hops, cross) for hops in (1, chips - 1) for cross in (False, True)]
    for to in near:
        pl.semaphore_signal(barrier, inc=1, device_id={"x": away(*to)}, device_id_type=MESH)

    small = [
        pltpu.make_async_copy(src, dst, in_sem.at[i])
        for i, (src, dst) in enumerate((
            (hid_hbm, hid_ref), (an_hbm, an_ref), (freq_hbm, freq_ref), (qn_hbm, qn_ref), (kn_hbm, kn_ref), (mn_hbm, mn_ref), (pos_hbm, pos_ref),
        ))
    ]
    for c in small:
        c.start()

    def cols(hbm, i):
        return hbm.at[:, pl.ds(pl.multiple_of(i * TILE, TILE), TILE)]

    def load(src, dst, sem, slot):
        return pltpu.make_async_copy(src, dst.at[slot], sem.at[slot])

    load(cols(wq_hbm, 0), wbuf, wsem, 0).start()
    pl.semaphore_wait(barrier, len(near))
    pl.semaphore_signal(ready, inc=1, device_id={"x": away(chips - 1, False)}, device_id_type=MESH)

    def send(which, sem, first, count, lo, size, targets):
        for hops, cross in targets:
            to = away(hops, cross)
            pltpu.make_async_remote_copy(
                src_ref=(k_hbm, v_hbm)[which].at[pl.ds(to * rows + first, count), pl.ds(lo, size)],
                dst_ref=(rk, rv)[which].at[me, pl.ds(first, count), pl.ds(lo, size)],
                send_sem=bulk_s.at[which], recv_sem=(krs, vrs)[which].at[sem], device_id={"x": to}, device_id_type=MESH,
            ).start()

    turn = core * (chips - 2)
    one_way, other_way = 1 + turn, chips - 1 - turn
    order = [(hops, cross) for cross in (False, True) for hops in [one_way, *range(2, chips - 1), other_way]] + [(0, True)]

    last = [(0, pairs - 1, rows - PAIR, PAIR, 0, slots)]
    last += [(1, pairs - 1 + e, rows - PAIR + e, 1, 0, slots) for e in range(PAIR - 1)]
    for i, (lo, size) in enumerate(((0, slots // 2), (slots // 2, slots // 4), (slots * 3 // 4, slots // 4))):
        last.append((1, pairs - 2 + PAIR + i, rows - 1, 1, lo, size))

    def bulk(r):
        send(0, r, r * PAIR, PAIR, 0, slots, order)
        send(1, r, r * PAIR, PAIR, 0, slots, order)

    def bulk_last():
        for which, sem, first, count, lo, size in last:
            send(which, sem, first, count, lo, size, order)

    def bulk_next(r):
        @pl.when(r < pairs - 1)
        def _():
            bulk(r)

        @pl.when(r == pairs - 1)
        def _():
            bulk_last()

    def bulk_wait(which, sem, count, size):
        whole = (rk, rv)[which].at[pl.ds(0, n - 1), pl.ds(0, count), pl.ds(0, size)]
        pltpu.make_async_copy(whole, whole, (krs, vrs)[which].at[sem]).wait()

    send(0, 0, 0, PAIR, 0, slots, order[:1])
    pl.semaphore_wait(ready, 1)
    send(0, 0, 0, PAIR, 0, slots, order[1:])
    send(1, 0, 0, PAIR, 0, slots, order)
    bulk(1)

    own = [
        pltpu.make_async_copy(k_hbm.at[pl.ds(me * rows, rows)], rk.at[me], own_sem.at[0]),
        pltpu.make_async_copy(v_hbm.at[pl.ds(me * rows, rows)], rv.at[me], own_sem.at[1]),
    ]

    def stream(hbm, body, started=False):
        tiles = hbm.shape[1] // TILE
        if not started:
            load(cols(hbm, 0), wbuf, wsem, 0).start()

        @pl.loop(0, tiles)
        def _(i):
            slot = lax.rem(i, 2)

            @pl.when(i + 1 < tiles)
            def _():
                load(cols(hbm, i + 1), wbuf, wsem, 1 - slot).start()

            load(cols(hbm, i), wbuf, wsem, slot).wait()
            body(i, wbuf[slot])

    for c in small:
        c.wait()
    for c in range(0, dim, hd):
        for s in range(steps):
            tmp_s[pl.ds(s, rows, stride=steps), :] = hid_ref[s, :, c : c + hd].astype(F32)
        hid_s[:, c : c + hd] = tmp_s[...]
    act_s[...] = rms(hid_s[...], an_ref[...].astype(F32).reshape(1, dim)).astype(BF16)

    row = lax.broadcasted_iota(jnp.int32, (num, hd), 0)
    pos = jnp.zeros((num, hd), jnp.int32)
    for b in range(rows):
        pos = jnp.where(row // steps == b, pos_ref[me * rows + b], pos)
    angles = (pos + row % steps).astype(F32) * freq_ref[...]
    lane = lax.broadcasted_iota(jnp.int32, (num, hd), 1)
    cs_s[...] = jnp.cos(angles)
    sn_s[...] = jnp.where(lane < hd // 2, -jnp.sin(angles), jnp.sin(angles))

    def rotate(v):
        return v * cs_s[...] + pltpu.roll(v, hd // 2, 1) * sn_s[...]

    per_tile = TILE // hd

    def q_tile(i, w):
        y = jnp.dot(act_s[...], w, preferred_element_type=F32)
        gain = qn_ref[...].astype(F32)
        for g in range(per_tile // q_per):
            parts = []
            for j in range(q_per):
                c = (g * q_per + j) * hd
                head = rotate(rms(y[:, c : c + hd], gain))
                parts.append(head.reshape(pairs, new, hd))
            msg_s[i * (per_tile // q_per) + g, :, 0:tall, :] = jnp.concatenate(parts, axis=1).astype(BF16)

    def k_tile(i, w):
        y = jnp.dot(act_s[...], w, preferred_element_type=F32)
        gain = kn_ref[...].astype(F32)
        for g in range(per_tile):
            head = rotate(rms(y[:, g * hd : (g + 1) * hd], gain))
            msg_s[i * per_tile + g, :, tall : tall + new, :] = head.reshape(pairs, new, hd).astype(BF16)
            kmix_s[pl.ds(i * per_tile + g, num, stride=n), :] = head

    def v_tile(i, w):
        y = jnp.dot(act_s[...], w, preferred_element_type=F32)
        for g in range(per_tile):
            head = y[:, g * hd : (g + 1) * hd]
            msg_s[i * per_tile + g, :, tall + new : tall + 2 * new, :] = head.reshape(pairs, new, hd).astype(BF16)
            vmix_s[pl.ds(i * per_tile + g, num, stride=n), :] = head

    stream(wq_hbm, q_tile, started=True)
    stream(wk_hbm, k_tile)
    stream(wv_hbm, v_tile)

    def msg_copy(to):
        return pltpu.make_async_remote_copy(
            src_ref=msg_s.at[to, pl.ds(home, AWAY)], dst_ref=msg_r.at[me], send_sem=msg_ss.at[to], recv_sem=msg_rs.at[me],
            device_id={"x": to}, device_id_type=MESH,
        )

    def msg_arrival(source):
        return pltpu.make_async_remote_copy(
            src_ref=msg_s.at[source, pl.ds(home, AWAY)], dst_ref=msg_r.at[source], send_sem=msg_ss.at[source],
            recv_sem=msg_rs.at[source], device_id={"x": source}, device_id_type=MESH,
        )

    def o_copy(to):
        return pltpu.make_async_remote_copy(
            src_ref=o_s.at[to], dst_ref=o_r.at[me, pl.ds(home, AWAY)], send_sem=o_ss.at[to], recv_sem=o_rs.at[me],
            device_id={"x": to}, device_id_type=MESH,
        )

    def o_arrival(source):
        return pltpu.make_async_remote_copy(
            src_ref=o_s.at[source], dst_ref=o_r.at[source, pl.ds(home, AWAY)], send_sem=o_ss.at[source], recv_sem=o_rs.at[source],
            device_id={"x": source}, device_id_type=MESH,
        )

    def kv_load(o, slot):
        first = peer(o) * rows + home * PAIR
        return (
            pltpu.make_async_copy(k_hbm.at[pl.ds(first, AWAY * PAIR)], kbuf.at[slot], ksem.at[slot]),
            pltpu.make_async_copy(v_hbm.at[pl.ds(first, AWAY * PAIR)], vbuf.at[slot], vsem.at[slot]),
        )

    for c in kv_load(0, 0):
        c.start()
    for c in own:
        c.start()
    msg_r[me] = msg_s[me, home:pairs]
    for o in range(1, n):
        msg_copy(peer(o)).start()
    for r in range(2, AHEAD):
        bulk(r)

    scale = hd ** -0.5
    nt = (((1,), (1,)), ((), ()))
    r_new = lax.broadcasted_iota(jnp.int32, (tall, new), 0) % new
    c_new = lax.broadcasted_iota(jnp.int32, (tall, new), 1)
    new_ok = (c_new // steps == r_new // steps) & (c_new % steps <= r_new % steps)
    in_pair = (lax.broadcasted_iota(jnp.int32, (tall, slots), 0) % new) // steps
    in_pair_o = (lax.broadcasted_iota(jnp.int32, (tall, hd), 0) % new) // steps
    t = lax.broadcasted_iota(jnp.int32, (tall, slots), 1)

    def attend(msg, keys, values, first):
        q = msg[0:tall]
        v_new = msg[tall + new : tall + 2 * new]
        fresh = lax.dot_general(q, msg[tall : tall + new], nt, preferred_element_type=F32)
        fresh = jnp.where(new_ok, fresh * scale, -jnp.inf)
        old = lax.dot_general(q, keys(0), nt, preferred_element_type=F32)
        start = jnp.full((tall, slots), pos_ref[first], jnp.int32)
        for e in range(1, PAIR):
            other = lax.dot_general(q, keys(e), nt, preferred_element_type=F32)
            old = jnp.where(in_pair == e, other, old)
            start = jnp.where(in_pair == e, pos_ref[first + e], start)
        old = jnp.where(t < start, old * scale, -jnp.inf)
        peak = jnp.maximum(jnp.max(old, axis=-1, keepdims=True), jnp.max(fresh, axis=-1, keepdims=True))
        old = jnp.exp(old - peak)
        fresh = jnp.exp(fresh - peak)
        total = jnp.sum(old, axis=-1, keepdims=True) + jnp.sum(fresh, axis=-1, keepdims=True)
        weights = old.astype(BF16)
        mixed = jnp.dot(weights, values(0), preferred_element_type=F32)
        for e in range(1, PAIR):
            other = jnp.dot(weights, values(e), preferred_element_type=F32)
            mixed = jnp.where(in_pair_o == e, other, mixed)
        mixed = mixed + jnp.dot(fresh.astype(BF16), v_new, preferred_element_type=F32)
        return (mixed / total).astype(BF16)

    @pl.loop(0, n)
    def _(o):
        slot = lax.rem(o, 2)
        source = peer(o)

        @pl.when(o + 1 < n)
        def _():
            for c in kv_load(o + 1, 1 - slot):
                c.start()

        for c in kv_load(o, slot):
            c.wait()

        @pl.when(o > 0)
        def _():
            msg_arrival(source).wait_recv()

        for i in range(AWAY):
            o_s[source, i] = attend(
                msg_r[source, i], lambda e: kbuf[slot, i * PAIR + e], lambda e: vbuf[slot, i * PAIR + e],
                source * rows + (home + i) * PAIR,
            )

        @pl.when(o == 0)
        def _():
            o_r[me, home:pairs] = o_s[me]

        @pl.when(o > 1)
        def _():
            o_copy(peer(o - 1)).start()

    for c in own:
        c.wait()
    o_copy(peer(n - 1)).start()

    def place(which, first, count, lo=0, size=slots):
        src, dst = ((rk, ka_ref), (rv, va_ref))[which]

        @pl.loop(0, count)
        def _(e):
            for h in range(n):
                mix_s[pl.ds(h, size, stride=n), :] = src[h, first + e, lo : lo + size].astype(F32)
            mixed = mix_s[0 : size * n].reshape(size, n, hd)
            slot = lo + lax.broadcasted_iota(jnp.int32, (size, n, hd), 0)
            for s in range(steps):
                at = pl.multiple_of(((first + e) * steps + s) * n, n)
                fresh = (kmix_s, vmix_s)[which][pl.ds(at, n), :]
                mixed = jnp.where(slot == pos_ref[me * rows + first + e] + s, fresh[None], mixed)
            dst[first + e, lo : lo + size] = mixed.astype(BF16)

    @pl.loop(0, home)
    def _(r):
        bulk_wait(0, r, PAIR, slots)
        bulk_wait(1, r, PAIR, slots)
        bulk_next(r + AHEAD)
        place(0, r * PAIR, PAIR)
        place(1, r * PAIR, PAIR)

        @pl.loop(0, n)
        def _(h):
            o_r[h, r] = attend(
                msg_s[h, r], lambda e: rk[h, r * PAIR + e], lambda e: rv[h, r * PAIR + e], me * rows + r * PAIR
            )

    for o in range(1, n):
        o_arrival(peer(o)).wait_recv()
    for h in range(n):
        both = o_r[h].astype(F32)
        for j in range(q_per):
            head = both[:, j * new : (j + 1) * new, :].reshape(num, hd)
            act_s[:, (h * q_per + j) * hd : (h * q_per + j + 1) * hd] = head.astype(BF16)

    def wo_tile(i, w):
        at = pl.ds(pl.multiple_of(i * TILE, TILE), TILE)
        y = jnp.dot(act_s[...], w, preferred_element_type=F32)
        x1_s[:, at] = (hid_s[:, at] + y).astype(BF16).astype(F32)

    stream(wo_hbm, wo_tile)
    act_s[...] = rms(x1_s[...], mn_ref[...].astype(F32).reshape(1, dim)).astype(BF16)
    acc_s[...] = jnp.zeros_like(acc_s)
    tiles = wg_hbm.shape[1] // TILE

    def mlp_loads(i, slot):
        at = pl.ds(pl.multiple_of(i * TILE, TILE), TILE)
        return (
            load(cols(wg_hbm, i), wbuf, wsem, slot),
            load(cols(wu_hbm, i), ubuf, usem, slot),
            load(wd_hbm.at[at, :], dbuf, dsem, slot),
        )

    for c in mlp_loads(0, 0):
        c.start()

    @pl.loop(0, tiles)
    def _(i):
        slot = lax.rem(i, 2)

        @pl.when(i + 1 < tiles)
        def _():
            for c in mlp_loads(i + 1, 1 - slot):
                c.start()

        for c in mlp_loads(i, slot):
            c.wait()
        z = act_s[...]
        gate = jnp.dot(z, wbuf[slot], preferred_element_type=F32)
        up = jnp.dot(z, ubuf[slot], preferred_element_type=F32)
        g = (jax.nn.silu(gate) * up).astype(BF16)
        acc_s[...] += jnp.dot(g, dbuf[slot], preferred_element_type=F32)

    for c in range(0, dim, hd):
        tmp_s[...] = x1_s[:, c : c + hd] + acc_s[:, c : c + hd]
        for s in range(steps):
            out_ref[s, :, c : c + hd] = tmp_s[pl.ds(s, rows, stride=steps), :].astype(BF16)

    for o in range(1, n):
        msg_copy(peer(o)).wait_send()
        o_copy(peer(o)).wait_send()

    @pl.loop(home, pairs - 1)
    def _(r):
        for which in range(2):
            bulk_wait(which, r, PAIR, slots)
            place(which, r * PAIR, PAIR)

    for which, sem, first, count, lo, size in last:
        bulk_wait(which, sem, count, size)
        place(which, first, count, lo, size)

    for which, dst in enumerate((rk, rv)):
        whole = dst.at[pl.ds(0, n - 1)]
        pltpu.make_async_copy(whole, whole, bulk_s.at[which]).wait()


def store_kernel(hid_ref, ka_ref, va_ref, out_hbm, ko_hbm, vo_hbm, hid_sem, sems):
    copies = []
    for b in range(ka_ref.shape[0]):
        copies.append(pltpu.make_async_copy(ka_ref.at[b], ko_hbm.at[b], sems.at[0, b]))
        copies.append(pltpu.make_async_copy(va_ref.at[b], vo_hbm.at[b], sems.at[1, b]))
    copies.append(pltpu.make_async_copy(hid_ref, out_hbm, hid_sem))
    for c in copies:
        c.start()
    for c in copies:
        c.wait()


def solution(mesh):
    row_spec = P(None, ("dp", "x"), None)
    cache_in = P("dp", None, "x", None)
    cache_out = P(("dp", "x"), None, None, None)
    n = mesh.shape["x"]

    def local_run(start_pos, hidden_in, k_heads, v_heads, attn_norm, w_q, w_k, w_v, q_norm, k_norm, w_o, mlp_norm, w_gate, w_up, w_down):
        steps, rows, dim = hidden_in.shape
        slots, hd = k_heads.shape[1], k_heads.shape[3]
        heads = w_q.shape[1] // hd
        num = steps * rows
        pairs = rows // PAIR
        half = hd // 2
        inv_freq = np.power(np.float32(THETA), -np.arange(half, dtype=np.float32) * np.float32(2.0) / np.float32(hd))
        freq = jnp.asarray(np.concatenate([inv_freq, inv_freq])[None, :], F32)
        vmem = pl.BlockSpec(memory_space=pltpu.VMEM)
        hbm = pl.BlockSpec(memory_space=pltpu.HBM)
        tall, new = PAIR * steps * (heads // n), PAIR * steps
        dma = pltpu.SemaphoreType.DMA
        cache = (rows, slots, n, hd)
        blocks = pltpu.VMEM((n, rows, slots, hd), BF16)
        chunk = pltpu.VMEM((2, AWAY * PAIR, slots, hd), BF16)
        wide = pltpu.VMEM((num, dim), F32)
        head = pltpu.VMEM((num, hd), F32)
        arrived = (pltpu.VMEM(hidden_in.shape, BF16), pltpu.VMEM(cache, BF16), pltpu.VMEM(cache, BF16))
        held = pl.pallas_call(
            functools.partial(layer_kernel, n, steps, rows, heads, hd),
            name="layer",
            out_shape=arrived,
            in_specs=[hbm] * 16,
            out_specs=(vmem,) * 3,
            scratch_shapes=[
                pltpu.SMEM(start_pos.shape, jnp.int32), pltpu.VMEM(freq.shape, F32), pltpu.VMEM(hidden_in.shape, BF16), pltpu.VMEM((dim,), BF16),
                pltpu.VMEM((1, hd), BF16), pltpu.VMEM((1, hd), BF16), pltpu.VMEM((dim,), BF16),
                wide, pltpu.VMEM((num, dim), BF16), wide, wide, head, head, head,
                pltpu.VMEM((n, pairs, tall + 2 * new, hd), BF16), pltpu.VMEM((n, AWAY, tall + 2 * new, hd), BF16),
                pltpu.VMEM((n, AWAY, tall, hd), BF16), pltpu.VMEM((n, pairs, tall, hd), BF16),
                blocks, blocks, chunk, chunk,
                pltpu.VMEM((2, dim, TILE), BF16), pltpu.VMEM((2, dim, TILE), BF16), pltpu.VMEM((2, TILE, dim), BF16),
                pltpu.VMEM((slots * n, hd), F32), pltpu.VMEM((num * n, hd), F32), pltpu.VMEM((num * n, hd), F32),
                dma((2,)), dma((2,)), dma((2,)), dma((2,)), dma((2,)), dma((2,)),
                dma((n,)), dma((n,)), dma((n,)), dma((n,)), dma((2,)), dma((pairs,)), dma((pairs + PAIR + 1,)), dma((7,)), pltpu.SemaphoreType.REGULAR,
            ],
            compiler_params=pltpu.CompilerParams(collective_id=0, has_side_effects=True, vmem_limit_bytes=VMEM_LIMIT),
        )(
            start_pos, freq, hidden_in, k_heads.reshape(-1, slots, hd), v_heads.reshape(-1, slots, hd), attn_norm,
            w_q, w_k, w_v, q_norm.reshape(1, -1), k_norm.reshape(1, -1), w_o, mlp_norm, w_gate, w_up, w_down,
        )
        return pl.pallas_call(
            store_kernel,
            name="store",
            out_shape=tuple(jax.ShapeDtypeStruct(a.shape, BF16) for a in (hidden_in, held[1], held[2])),
            in_specs=[vmem] * 3,
            out_specs=(hbm,) * 3,
            scratch_shapes=[dma, dma((2, rows))],
            compiler_params=pltpu.CompilerParams(vmem_limit_bytes=2**20),
        )(*held)

    return jax.shard_map(local_run, mesh=mesh, in_specs=(P("dp"), row_spec, cache_in, cache_in) + (P(),) * 11, out_specs=(row_spec, cache_out, cache_out), check_vma=False)
```

```python
import functools

import jax
import jax.numpy as jnp
import numpy as np
from jax import lax
from jax.experimental import pallas as pl
from jax.experimental.pallas import tpu as pltpu
from jax.sharding import PartitionSpec as P

EPS = 1e-6
THETA = 1000000.0
F32 = jnp.float32
BF16 = jnp.bfloat16
MESH = pl.DeviceIdType.MESH
TILE = 512
PAIR = 2
AWAY = 2
VMEM_LIMIT = 44 * 2**20
AHEAD = 4


def rms(values, gain):
    inv_rms = lax.rsqrt(jnp.mean(values * values, axis=-1, keepdims=True) + EPS)
    return values * inv_rms * gain


def layer_kernel(
    n, steps, rows, heads, hd,
    pos_hbm, freq_hbm, hid_hbm, k_hbm, v_hbm, an_hbm, wq_hbm, wk_hbm, wv_hbm, qn_hbm, kn_hbm, wo_hbm, mn_hbm,
    wg_hbm, wu_hbm, wd_hbm,
    out_ref, ka_ref, va_ref,
    pos_ref, freq_ref, hid_ref, an_ref, qn_ref, kn_ref, mn_ref, hid_s, act_s, x1_s, acc_s, tmp_s, cs_s, sn_s, msg_s, msg_r, o_s, o_r, rk, rv, kbuf, vbuf, wbuf, ubuf, dbuf, mix_s, kmix_s, vmix_s,
    wsem, usem, dsem, ksem, vsem, own_sem, msg_ss, msg_rs, o_ss, o_rs, bulk_s, krs, vrs, in_sem, ready,
):
    me = lax.axis_index("x")
    num = steps * rows
    q_per = heads // n
    pairs = rows // PAIR
    home = pairs - AWAY
    slots = k_hbm.shape[1]
    dim = hid_ref.shape[2]
    tall = PAIR * steps * q_per
    new = PAIR * steps
    barrier = pltpu.get_barrier_semaphore()

    chips = n // 2
    chip, core = me // 2, lax.rem(me, 2)

    def peer(o):
        return lax.rem(me + o, n)

    def away(hops, cross):
        return lax.rem(chip + hops, chips) * 2 + (1 - core if cross else core)

    near = [(0, True), (1, False), (1, True), (chips - 1, False), (chips - 1, True)]
    for to in near:
        pl.semaphore_signal(barrier, inc=1, device_id={"x": away(*to)}, device_id_type=MESH)

    small = [
        pltpu.make_async_copy(src, dst, in_sem.at[i])
        for i, (src, dst) in enumerate((
            (hid_hbm, hid_ref), (an_hbm, an_ref), (freq_hbm, freq_ref), (qn_hbm, qn_ref), (kn_hbm, kn_ref), (mn_hbm, mn_ref), (pos_hbm, pos_ref),
        ))
    ]
    for c in small:
        c.start()

    def cols(hbm, i):
        return hbm.at[:, pl.ds(pl.multiple_of(i * TILE, TILE), TILE)]

    def load(src, dst, sem, slot):
        return pltpu.make_async_copy(src, dst.at[slot], sem.at[slot])

    load(cols(wq_hbm, 0), wbuf, wsem, 0).start()
    pl.semaphore_wait(barrier, len(near))
    pl.semaphore_signal(ready, inc=1, device_id={"x": away(chips - 1, False)}, device_id_type=MESH)

    def send(which, sem, first, count, lo, size, targets):
        for hops, cross in targets:
            to = away(hops, cross)
            pltpu.make_async_remote_copy(
                src_ref=(k_hbm, v_hbm)[which].at[pl.ds(to * rows + first, count), pl.ds(lo, size)],
                dst_ref=(rk, rv)[which].at[me, pl.ds(first, count), pl.ds(lo, size)],
                send_sem=bulk_s.at[which], recv_sem=(krs, vrs)[which].at[sem], device_id={"x": to}, device_id_type=MESH,
            ).start()

    far = [(hops, cross) for hops in range(2, chips - 1) for cross in (False, True)]
    order = near[1::2] + far[:1] + near[2::2] + far[1:] + near[:1]
    far_first = far + near[1::2] + near[2::2] + near[:1]

    last = [(0, pairs - 1, rows - PAIR, PAIR, 0, slots)]
    last += [(1, pairs - 1 + e, rows - PAIR + e, 1, 0, slots) for e in range(PAIR - 1)]
    for i, (lo, size) in enumerate(((0, slots // 2), (slots // 2, slots // 4), (slots * 3 // 4, slots // 4))):
        last.append((1, pairs - 2 + PAIR + i, rows - 1, 1, lo, size))

    def bulk(r):
        send(0, r, r * PAIR, PAIR, 0, slots, order)
        send(1, r, r * PAIR, PAIR, 0, slots, order)

    def bulk_last():
        for which, sem, first, count, lo, size in last:
            send(which, sem, first, count, lo, size, far_first)

    def bulk_next(r):
        @pl.when(r < pairs - 1)
        def _():
            bulk(r)

        @pl.when(r == pairs - 1)
        def _():
            bulk_last()

    def bulk_wait(which, sem, count, size):
        whole = (rk, rv)[which].at[pl.ds(0, n - 1), pl.ds(0, count), pl.ds(0, size)]
        pltpu.make_async_copy(whole, whole, (krs, vrs)[which].at[sem]).wait()

    send(0, 0, 0, PAIR, 0, slots, near[1:] + near[:1])
    pl.semaphore_wait(ready, 1)
    send(0, 0, 0, PAIR, 0, slots, far)
    send(1, 0, 0, PAIR, 0, slots, order)
    bulk(1)

    own = [
        pltpu.make_async_copy(k_hbm.at[pl.ds(me * rows, rows)], rk.at[me], own_sem.at[0]),
        pltpu.make_async_copy(v_hbm.at[pl.ds(me * rows, rows)], rv.at[me], own_sem.at[1]),
    ]

    def stream(hbm, body, started=False):
        tiles = hbm.shape[1] // TILE
        if not started:
            load(cols(hbm, 0), wbuf, wsem, 0).start()

        @pl.loop(0, tiles)
        def _(i):
            slot = lax.rem(i, 2)

            @pl.when(i + 1 < tiles)
            def _():
                load(cols(hbm, i + 1), wbuf, wsem, 1 - slot).start()

            load(cols(hbm, i), wbuf, wsem, slot).wait()
            body(i, wbuf[slot])

    for c in small:
        c.wait()
    for c in range(0, dim, hd):
        for s in range(steps):
            tmp_s[pl.ds(s, rows, stride=steps), :] = hid_ref[s, :, c : c + hd].astype(F32)
        hid_s[:, c : c + hd] = tmp_s[...]
    act_s[...] = rms(hid_s[...], an_ref[...].astype(F32).reshape(1, dim)).astype(BF16)

    row = lax.broadcasted_iota(jnp.int32, (num, hd), 0)
    pos = jnp.zeros((num, hd), jnp.int32)
    for b in range(rows):
        pos = jnp.where(row // steps == b, pos_ref[me * rows + b], pos)
    angles = (pos + row % steps).astype(F32) * freq_ref[...]
    lane = lax.broadcasted_iota(jnp.int32, (num, hd), 1)
    cs_s[...] = jnp.cos(angles)
    sn_s[...] = jnp.where(lane < hd // 2, -jnp.sin(angles), jnp.sin(angles))

    def rotate(v):
        return v * cs_s[...] + pltpu.roll(v, hd // 2, 1) * sn_s[...]

    per_tile = TILE // hd

    def q_tile(i, w):
        y = jnp.dot(act_s[...], w, preferred_element_type=F32)
        gain = qn_ref[...].astype(F32)
        for g in range(per_tile // q_per):
            parts = []
            for j in range(q_per):
                c = (g * q_per + j) * hd
                head = rotate(rms(y[:, c : c + hd], gain))
                parts.append(head.reshape(pairs, new, hd))
            msg_s[i * (per_tile // q_per) + g, :, 0:tall, :] = jnp.concatenate(parts, axis=1).astype(BF16)

    def k_tile(i, w):
        y = jnp.dot(act_s[...], w, preferred_element_type=F32)
        gain = kn_ref[...].astype(F32)
        for g in range(per_tile):
            head = rotate(rms(y[:, g * hd : (g + 1) * hd], gain))
            msg_s[i * per_tile + g, :, tall : tall + new, :] = head.reshape(pairs, new, hd).astype(BF16)
            kmix_s[pl.ds(i * per_tile + g, num, stride=n), :] = head

    def v_tile(i, w):
        y = jnp.dot(act_s[...], w, preferred_element_type=F32)
        for g in range(per_tile):
            head = y[:, g * hd : (g + 1) * hd]
            msg_s[i * per_tile + g, :, tall + new : tall + 2 * new, :] = head.reshape(pairs, new, hd).astype(BF16)
            vmix_s[pl.ds(i * per_tile + g, num, stride=n), :] = head

    stream(wq_hbm, q_tile, started=True)
    stream(wk_hbm, k_tile)
    stream(wv_hbm, v_tile)

    def msg_copy(to):
        return pltpu.make_async_remote_copy(
            src_ref=msg_s.at[to, pl.ds(home, AWAY)], dst_ref=msg_r.at[me], send_sem=msg_ss.at[to], recv_sem=msg_rs.at[me],
            device_id={"x": to}, device_id_type=MESH,
        )

    def msg_arrival(source):
        return pltpu.make_async_remote_copy(
            src_ref=msg_s.at[source, pl.ds(home, AWAY)], dst_ref=msg_r.at[source], send_sem=msg_ss.at[source],
            recv_sem=msg_rs.at[source], device_id={"x": source}, device_id_type=MESH,
        )

    def o_copy(to):
        return pltpu.make_async_remote_copy(
            src_ref=o_s.at[to], dst_ref=o_r.at[me, pl.ds(home, AWAY)], send_sem=o_ss.at[to], recv_sem=o_rs.at[me],
            device_id={"x": to}, device_id_type=MESH,
        )

    def o_arrival(source):
        return pltpu.make_async_remote_copy(
            src_ref=o_s.at[source], dst_ref=o_r.at[source, pl.ds(home, AWAY)], send_sem=o_ss.at[source], recv_sem=o_rs.at[source],
            device_id={"x": source}, device_id_type=MESH,
        )

    def kv_load(o, slot):
        first = peer(o) * rows + home * PAIR
        return (
            pltpu.make_async_copy(k_hbm.at[pl.ds(first, AWAY * PAIR)], kbuf.at[slot], ksem.at[slot]),
            pltpu.make_async_copy(v_hbm.at[pl.ds(first, AWAY * PAIR)], vbuf.at[slot], vsem.at[slot]),
        )

    for c in kv_load(0, 0):
        c.start()
    for c in own:
        c.start()
    msg_r[me] = msg_s[me, home:pairs]
    for o in range(1, n):
        msg_copy(peer(o)).start()
    for r in range(2, AHEAD):
        bulk(r)

    scale = hd ** -0.5
    nt = (((1,), (1,)), ((), ()))
    r_new = lax.broadcasted_iota(jnp.int32, (tall, new), 0) % new
    c_new = lax.broadcasted_iota(jnp.int32, (tall, new), 1)
    new_ok = (c_new // steps == r_new // steps) & (c_new % steps <= r_new % steps)
    in_pair = (lax.broadcasted_iota(jnp.int32, (tall, slots), 0) % new) // steps
    in_pair_o = (lax.broadcasted_iota(jnp.int32, (tall, hd), 0) % new) // steps
    t = lax.broadcasted_iota(jnp.int32, (tall, slots), 1)

    def attend(msg, keys, values, first):
        q = msg[0:tall]
        v_new = msg[tall + new : tall + 2 * new]
        fresh = lax.dot_general(q, msg[tall : tall + new], nt, preferred_element_type=F32)
        fresh = jnp.where(new_ok, fresh * scale, -jnp.inf)
        old = lax.dot_general(q, keys(0), nt, preferred_element_type=F32)
        start = jnp.full((tall, slots), pos_ref[first], jnp.int32)
        for e in range(1, PAIR):
            other = lax.dot_general(q, keys(e), nt, preferred_element_type=F32)
            old = jnp.where(in_pair == e, other, old)
            start = jnp.where(in_pair == e, pos_ref[first + e], start)
        old = jnp.where(t < start, old * scale, -jnp.inf)
        peak = jnp.maximum(jnp.max(old, axis=-1, keepdims=True), jnp.max(fresh, axis=-1, keepdims=True))
        old = jnp.exp(old - peak)
        fresh = jnp.exp(fresh - peak)
        total = jnp.sum(old, axis=-1, keepdims=True) + jnp.sum(fresh, axis=-1, keepdims=True)
        weights = old.astype(BF16)
        mixed = jnp.dot(weights, values(0), preferred_element_type=F32)
        for e in range(1, PAIR):
            other = jnp.dot(weights, values(e), preferred_element_type=F32)
            mixed = jnp.where(in_pair_o == e, other, mixed)
        mixed = mixed + jnp.dot(fresh.astype(BF16), v_new, preferred_element_type=F32)
        return (mixed / total).astype(BF16)

    @pl.loop(0, n)
    def _(o):
        slot = lax.rem(o, 2)
        source = peer(o)

        @pl.when(o + 1 < n)
        def _():
            for c in kv_load(o + 1, 1 - slot):
                c.start()

        for c in kv_load(o, slot):
            c.wait()

        @pl.when(o > 0)
        def _():
            msg_arrival(source).wait_recv()

        for i in range(AWAY):
            o_s[source, i] = attend(
                msg_r[source, i], lambda e: kbuf[slot, i * PAIR + e], lambda e: vbuf[slot, i * PAIR + e],
                source * rows + (home + i) * PAIR,
            )

        @pl.when(o == 0)
        def _():
            o_r[me, home:pairs] = o_s[me]

        @pl.when(o > 1)
        def _():
            o_copy(peer(o - 1)).start()

    for c in own:
        c.wait()
    o_copy(peer(n - 1)).start()

    def place(which, first, count, lo=0, size=slots):
        src, dst = ((rk, ka_ref), (rv, va_ref))[which]

        @pl.loop(0, count)
        def _(e):
            for h in range(n):
                mix_s[pl.ds(h, size, stride=n), :] = src[h, first + e, lo : lo + size].astype(F32)
            mixed = mix_s[0 : size * n].reshape(size, n, hd)
            slot = lo + lax.broadcasted_iota(jnp.int32, (size, n, hd), 0)
            for s in range(steps):
                at = pl.multiple_of(((first + e) * steps + s) * n, n)
                fresh = (kmix_s, vmix_s)[which][pl.ds(at, n), :]
                mixed = jnp.where(slot == pos_ref[me * rows + first + e] + s, fresh[None], mixed)
            dst[first + e, lo : lo + size] = mixed.astype(BF16)

    @pl.loop(0, home)
    def _(r):
        bulk_wait(0, r, PAIR, slots)
        bulk_wait(1, r, PAIR, slots)
        bulk_next(r + AHEAD)
        place(0, r * PAIR, PAIR)
        place(1, r * PAIR, PAIR)

        @pl.loop(0, n)
        def _(h):
            o_r[h, r] = attend(
                msg_s[h, r], lambda e: rk[h, r * PAIR + e], lambda e: rv[h, r * PAIR + e], me * rows + r * PAIR
            )

    for o in range(1, n):
        o_arrival(peer(o)).wait_recv()
    for h in range(n):
        both = o_r[h].astype(F32)
        for j in range(q_per):
            head = both[:, j * new : (j + 1) * new, :].reshape(num, hd)
            act_s[:, (h * q_per + j) * hd : (h * q_per + j + 1) * hd] = head.astype(BF16)

    def wo_tile(i, w):
        at = pl.ds(pl.multiple_of(i * TILE, TILE), TILE)
        y = jnp.dot(act_s[...], w, preferred_element_type=F32)
        x1_s[:, at] = (hid_s[:, at] + y).astype(BF16).astype(F32)

    stream(wo_hbm, wo_tile)
    act_s[...] = rms(x1_s[...], mn_ref[...].astype(F32).reshape(1, dim)).astype(BF16)
    acc_s[...] = jnp.zeros_like(acc_s)
    tiles = wg_hbm.shape[1] // TILE

    def mlp_loads(i, slot):
        at = pl.ds(pl.multiple_of(i * TILE, TILE), TILE)
        return (
            load(cols(wg_hbm, i), wbuf, wsem, slot),
            load(cols(wu_hbm, i), ubuf, usem, slot),
            load(wd_hbm.at[at, :], dbuf, dsem, slot),
        )

    for c in mlp_loads(0, 0):
        c.start()

    @pl.loop(0, tiles)
    def _(i):
        slot = lax.rem(i, 2)

        @pl.when(i + 1 < tiles)
        def _():
            for c in mlp_loads(i + 1, 1 - slot):
                c.start()

        for c in mlp_loads(i, slot):
            c.wait()
        z = act_s[...]
        gate = jnp.dot(z, wbuf[slot], preferred_element_type=F32)
        up = jnp.dot(z, ubuf[slot], preferred_element_type=F32)
        g = (jax.nn.silu(gate) * up).astype(BF16)
        acc_s[...] += jnp.dot(g, dbuf[slot], preferred_element_type=F32)

    for c in range(0, dim, hd):
        tmp_s[...] = x1_s[:, c : c + hd] + acc_s[:, c : c + hd]
        for s in range(steps):
            out_ref[s, :, c : c + hd] = tmp_s[pl.ds(s, rows, stride=steps), :].astype(BF16)

    for o in range(1, n):
        msg_copy(peer(o)).wait_send()
        o_copy(peer(o)).wait_send()

    @pl.loop(home, pairs - 1)
    def _(r):
        for which in range(2):
            bulk_wait(which, r, PAIR, slots)
            place(which, r * PAIR, PAIR)

    for which, sem, first, count, lo, size in last:
        bulk_wait(which, sem, count, size)
        place(which, first, count, lo, size)

    for which, dst in enumerate((rk, rv)):
        whole = dst.at[pl.ds(0, n - 1)]
        pltpu.make_async_copy(whole, whole, bulk_s.at[which]).wait()


def store_kernel(hid_ref, ka_ref, va_ref, out_hbm, ko_hbm, vo_hbm, hid_sem, sems):
    copies = []
    for b in range(ka_ref.shape[0]):
        copies.append(pltpu.make_async_copy(ka_ref.at[b], ko_hbm.at[b], sems.at[0, b]))
        copies.append(pltpu.make_async_copy(va_ref.at[b], vo_hbm.at[b], sems.at[1, b]))
    copies.append(pltpu.make_async_copy(hid_ref, out_hbm, hid_sem))
    for c in copies:
        c.start()
    for c in copies:
        c.wait()


def solution(mesh):
    row_spec = P(None, ("dp", "x"), None)
    cache_in = P("dp", None, "x", None)
    cache_out = P(("dp", "x"), None, None, None)
    n = mesh.shape["x"]

    def local_run(start_pos, hidden_in, k_heads, v_heads, attn_norm, w_q, w_k, w_v, q_norm, k_norm, w_o, mlp_norm, w_gate, w_up, w_down):
        steps, rows, dim = hidden_in.shape
        slots, hd = k_heads.shape[1], k_heads.shape[3]
        heads = w_q.shape[1] // hd
        num = steps * rows
        pairs = rows // PAIR
        half = hd // 2
        inv_freq = np.power(np.float32(THETA), -np.arange(half, dtype=np.float32) * np.float32(2.0) / np.float32(hd))
        freq = jnp.asarray(np.concatenate([inv_freq, inv_freq])[None, :], F32)
        vmem = pl.BlockSpec(memory_space=pltpu.VMEM)
        hbm = pl.BlockSpec(memory_space=pltpu.HBM)
        tall, new = PAIR * steps * (heads // n), PAIR * steps
        dma = pltpu.SemaphoreType.DMA
        cache = (rows, slots, n, hd)
        blocks = pltpu.VMEM((n, rows, slots, hd), BF16)
        chunk = pltpu.VMEM((2, AWAY * PAIR, slots, hd), BF16)
        wide = pltpu.VMEM((num, dim), F32)
        head = pltpu.VMEM((num, hd), F32)
        arrived = (pltpu.VMEM(hidden_in.shape, BF16), pltpu.VMEM(cache, BF16), pltpu.VMEM(cache, BF16))
        held = pl.pallas_call(
            functools.partial(layer_kernel, n, steps, rows, heads, hd),
            name="layer",
            out_shape=arrived,
            in_specs=[hbm] * 16,
            out_specs=(vmem,) * 3,
            scratch_shapes=[
                pltpu.SMEM(start_pos.shape, jnp.int32), pltpu.VMEM(freq.shape, F32), pltpu.VMEM(hidden_in.shape, BF16), pltpu.VMEM((dim,), BF16),
                pltpu.VMEM((1, hd), BF16), pltpu.VMEM((1, hd), BF16), pltpu.VMEM((dim,), BF16),
                wide, pltpu.VMEM((num, dim), BF16), wide, wide, head, head, head,
                pltpu.VMEM((n, pairs, tall + 2 * new, hd), BF16), pltpu.VMEM((n, AWAY, tall + 2 * new, hd), BF16),
                pltpu.VMEM((n, AWAY, tall, hd), BF16), pltpu.VMEM((n, pairs, tall, hd), BF16),
                blocks, blocks, chunk, chunk,
                pltpu.VMEM((2, dim, TILE), BF16), pltpu.VMEM((2, dim, TILE), BF16), pltpu.VMEM((2, TILE, dim), BF16),
                pltpu.VMEM((slots * n, hd), F32), pltpu.VMEM((num * n, hd), F32), pltpu.VMEM((num * n, hd), F32),
                dma((2,)), dma((2,)), dma((2,)), dma((2,)), dma((2,)), dma((2,)),
                dma((n,)), dma((n,)), dma((n,)), dma((n,)), dma((2,)), dma((pairs,)), dma((pairs + PAIR + 1,)), dma((7,)), pltpu.SemaphoreType.REGULAR,
            ],
            compiler_params=pltpu.CompilerParams(collective_id=0, has_side_effects=True, vmem_limit_bytes=VMEM_LIMIT),
        )(
            start_pos, freq, hidden_in, k_heads.reshape(-1, slots, hd), v_heads.reshape(-1, slots, hd), attn_norm,
            w_q, w_k, w_v, q_norm.reshape(1, -1), k_norm.reshape(1, -1), w_o, mlp_norm, w_gate, w_up, w_down,
        )
        return pl.pallas_call(
            store_kernel,
            name="store",
            out_shape=tuple(jax.ShapeDtypeStruct(a.shape, BF16) for a in (hidden_in, held[1], held[2])),
            in_specs=[vmem] * 3,
            out_specs=(hbm,) * 3,
            scratch_shapes=[dma, dma((2, rows))],
            compiler_params=pltpu.CompilerParams(vmem_limit_bytes=2**20),
        )(*held)

    return jax.shard_map(local_run, mesh=mesh, in_specs=(P("dp"), row_spec, cache_in, cache_in) + (P(),) * 11, out_specs=(row_spec, cache_out, cache_out), check_vma=False)
```

```python
import functools

import jax
import jax.numpy as jnp
import numpy as np
from jax import lax
from jax.experimental import pallas as pl
from jax.experimental.pallas import tpu as pltpu
from jax.sharding import PartitionSpec as P

EPS = 1e-6
THETA = 1000000.0
F32 = jnp.float32
BF16 = jnp.bfloat16
MESH = pl.DeviceIdType.MESH
TILE = 512
PAIR = 2
AWAY = 2
VMEM_LIMIT = 44 * 2**20
AHEAD = 4


def rms(values, gain):
    inv_rms = lax.rsqrt(jnp.mean(values * values, axis=-1, keepdims=True) + EPS)
    return values * inv_rms * gain


def layer_kernel(
    n, steps, rows, heads, hd,
    pos_hbm, freq_hbm, hid_hbm, k_hbm, v_hbm, an_hbm, wq_hbm, wk_hbm, wv_hbm, qn_hbm, kn_hbm, wo_hbm, mn_hbm,
    wg_hbm, wu_hbm, wd_hbm,
    out_ref, ka_ref, va_ref,
    pos_ref, freq_ref, hid_ref, an_ref, qn_ref, kn_ref, mn_ref, hid_s, act_s, x1_s, acc_s, tmp_s, cs_s, sn_s, msg_s, msg_r, o_s, o_r, rk, rv, kbuf, vbuf, wbuf, ubuf, dbuf, mix_s, kmix_s, vmix_s,
    wsem, usem, dsem, ksem, vsem, own_sem, msg_ss, msg_rs, o_ss, o_rs, bulk_s, krs, vrs, in_sem, ready,
):
    me = lax.axis_index("x")
    num = steps * rows
    q_per = heads // n
    pairs = rows // PAIR
    home = pairs - AWAY
    slots = k_hbm.shape[1]
    dim = hid_ref.shape[2]
    tall = PAIR * steps * q_per
    new = PAIR * steps
    barrier = pltpu.get_barrier_semaphore()

    chips = n // 2
    chip, core = me // 2, lax.rem(me, 2)

    def peer(o):
        return lax.rem(me + o, n)

    def away(hops, cross):
        return lax.rem(chip + hops, chips) * 2 + (1 - core if cross else core)

    near = [(0, True), (1, False), (1, True), (chips - 1, False), (chips - 1, True)]
    for to in near:
        pl.semaphore_signal(barrier, inc=1, device_id={"x": away(*to)}, device_id_type=MESH)

    small = [
        pltpu.make_async_copy(src, dst, in_sem.at[i])
        for i, (src, dst) in enumerate((
            (hid_hbm, hid_ref), (an_hbm, an_ref), (freq_hbm, freq_ref), (qn_hbm, qn_ref), (kn_hbm, kn_ref), (mn_hbm, mn_ref), (pos_hbm, pos_ref),
        ))
    ]
    for c in small:
        c.start()

    def cols(hbm, i):
        return hbm.at[:, pl.ds(pl.multiple_of(i * TILE, TILE), TILE)]

    def load(src, dst, sem, slot):
        return pltpu.make_async_copy(src, dst.at[slot], sem.at[slot])

    load(cols(wq_hbm, 0), wbuf, wsem, 0).start()
    pl.semaphore_wait(barrier, len(near))
    pl.semaphore_signal(ready, inc=1, device_id={"x": away(chips - 1, False)}, device_id_type=MESH)

    def send(which, sem, first, count, lo, size, targets):
        for hops, cross in targets:
            to = away(hops, cross)
            pltpu.make_async_remote_copy(
                src_ref=(k_hbm, v_hbm)[which].at[pl.ds(to * rows + first, count), pl.ds(lo, size)],
                dst_ref=(rk, rv)[which].at[me, pl.ds(first, count), pl.ds(lo, size)],
                send_sem=bulk_s.at[which], recv_sem=(krs, vrs)[which].at[sem], device_id={"x": to}, device_id_type=MESH,
            ).start()

    far = [(hops, cross) for hops in range(2, chips - 1) for cross in (False, True)]
    order = near[1::2] + far[:1] + near[2::2] + far[1:] + near[:1]
    far_first = far + near[1::2] + near[2::2] + near[:1]

    last = [(0, pairs - 1, rows - PAIR, PAIR, 0, slots)]
    last += [(1, pairs - 1 + e, rows - PAIR + e, 1, 0, slots) for e in range(PAIR - 1)]
    for i, (lo, size) in enumerate(((0, slots // 2), (slots // 2, slots // 4), (slots * 3 // 4, slots // 4))):
        last.append((1, pairs - 2 + PAIR + i, rows - 1, 1, lo, size))

    def bulk(r):
        for e in range(PAIR):
            for which in range(2):
                send(which, r, r * PAIR + e, 1, 0, slots, order)

    def bulk_last():
        for which, sem, first, count, lo, size in last:
            send(which, sem, first, count, lo, size, far_first)

    def bulk_next(r):
        @pl.when(r < pairs - 1)
        def _():
            bulk(r)

        @pl.when(r == pairs - 1)
        def _():
            bulk_last()

    def bulk_wait(which, sem, count, size):
        whole = (rk, rv)[which].at[pl.ds(0, n - 1), pl.ds(0, count), pl.ds(0, size)]
        pltpu.make_async_copy(whole, whole, (krs, vrs)[which].at[sem]).wait()

    send(0, 0, 0, 1, 0, slots, near[1:] + near[:1])
    pl.semaphore_wait(ready, 1)
    send(0, 0, 0, 1, 0, slots, far)
    send(1, 0, 0, 1, 0, slots, order)
    for which in range(2):
        send(which, 0, 1, PAIR - 1, 0, slots, order)
    bulk(1)

    own = [
        pltpu.make_async_copy(k_hbm.at[pl.ds(me * rows, rows)], rk.at[me], own_sem.at[0]),
        pltpu.make_async_copy(v_hbm.at[pl.ds(me * rows, rows)], rv.at[me], own_sem.at[1]),
    ]

    def stream(hbm, body, started=False):
        tiles = hbm.shape[1] // TILE
        if not started:
            load(cols(hbm, 0), wbuf, wsem, 0).start()

        @pl.loop(0, tiles)
        def _(i):
            slot = lax.rem(i, 2)

            @pl.when(i + 1 < tiles)
            def _():
                load(cols(hbm, i + 1), wbuf, wsem, 1 - slot).start()

            load(cols(hbm, i), wbuf, wsem, slot).wait()
            body(i, wbuf[slot])

    for c in small:
        c.wait()
    for c in range(0, dim, hd):
        for s in range(steps):
            tmp_s[pl.ds(s, rows, stride=steps), :] = hid_ref[s, :, c : c + hd].astype(F32)
        hid_s[:, c : c + hd] = tmp_s[...]
    act_s[...] = rms(hid_s[...], an_ref[...].astype(F32).reshape(1, dim)).astype(BF16)

    row = lax.broadcasted_iota(jnp.int32, (num, hd), 0)
    pos = jnp.zeros((num, hd), jnp.int32)
    for b in range(rows):
        pos = jnp.where(row // steps == b, pos_ref[me * rows + b], pos)
    angles = (pos + row % steps).astype(F32) * freq_ref[...]
    lane = lax.broadcasted_iota(jnp.int32, (num, hd), 1)
    cs_s[...] = jnp.cos(angles)
    sn_s[...] = jnp.where(lane < hd // 2, -jnp.sin(angles), jnp.sin(angles))

    def rotate(v):
        return v * cs_s[...] + pltpu.roll(v, hd // 2, 1) * sn_s[...]

    per_tile = TILE // hd

    def q_tile(i, w):
        y = jnp.dot(act_s[...], w, preferred_element_type=F32)
        gain = qn_ref[...].astype(F32)
        for g in range(per_tile // q_per):
            parts = []
            for j in range(q_per):
                c = (g * q_per + j) * hd
                head = rotate(rms(y[:, c : c + hd], gain))
                parts.append(head.reshape(pairs, new, hd))
            msg_s[i * (per_tile // q_per) + g, :, 0:tall, :] = jnp.concatenate(parts, axis=1).astype(BF16)

    def k_tile(i, w):
        y = jnp.dot(act_s[...], w, preferred_element_type=F32)
        gain = kn_ref[...].astype(F32)
        for g in range(per_tile):
            head = rotate(rms(y[:, g * hd : (g + 1) * hd], gain))
            msg_s[i * per_tile + g, :, tall : tall + new, :] = head.reshape(pairs, new, hd).astype(BF16)
            kmix_s[pl.ds(i * per_tile + g, num, stride=n), :] = head

    def v_tile(i, w):
        y = jnp.dot(act_s[...], w, preferred_element_type=F32)
        for g in range(per_tile):
            head = y[:, g * hd : (g + 1) * hd]
            msg_s[i * per_tile + g, :, tall + new : tall + 2 * new, :] = head.reshape(pairs, new, hd).astype(BF16)
            vmix_s[pl.ds(i * per_tile + g, num, stride=n), :] = head

    stream(wq_hbm, q_tile, started=True)
    stream(wk_hbm, k_tile)
    stream(wv_hbm, v_tile)

    def msg_copy(to):
        return pltpu.make_async_remote_copy(
            src_ref=msg_s.at[to, pl.ds(home, AWAY)], dst_ref=msg_r.at[me], send_sem=msg_ss.at[to], recv_sem=msg_rs.at[me],
            device_id={"x": to}, device_id_type=MESH,
        )

    def msg_arrival(source):
        return pltpu.make_async_remote_copy(
            src_ref=msg_s.at[source, pl.ds(home, AWAY)], dst_ref=msg_r.at[source], send_sem=msg_ss.at[source],
            recv_sem=msg_rs.at[source], device_id={"x": source}, device_id_type=MESH,
        )

    def o_copy(to):
        return pltpu.make_async_remote_copy(
            src_ref=o_s.at[to], dst_ref=o_r.at[me, pl.ds(home, AWAY)], send_sem=o_ss.at[to], recv_sem=o_rs.at[me],
            device_id={"x": to}, device_id_type=MESH,
        )

    def o_arrival(source):
        return pltpu.make_async_remote_copy(
            src_ref=o_s.at[source], dst_ref=o_r.at[source, pl.ds(home, AWAY)], send_sem=o_ss.at[source], recv_sem=o_rs.at[source],
            device_id={"x": source}, device_id_type=MESH,
        )

    def kv_load(o, slot):
        first = peer(o) * rows + home * PAIR
        return (
            pltpu.make_async_copy(k_hbm.at[pl.ds(first, AWAY * PAIR)], kbuf.at[slot], ksem.at[slot]),
            pltpu.make_async_copy(v_hbm.at[pl.ds(first, AWAY * PAIR)], vbuf.at[slot], vsem.at[slot]),
        )

    for c in kv_load(0, 0):
        c.start()
    for c in own:
        c.start()
    msg_r[me] = msg_s[me, home:pairs]
    for o in range(1, n):
        msg_copy(peer(o)).start()
    for r in range(2, AHEAD):
        bulk(r)

    scale = hd ** -0.5
    nt = (((1,), (1,)), ((), ()))
    r_new = lax.broadcasted_iota(jnp.int32, (tall, new), 0) % new
    c_new = lax.broadcasted_iota(jnp.int32, (tall, new), 1)
    new_ok = (c_new // steps == r_new // steps) & (c_new % steps <= r_new % steps)
    in_pair = (lax.broadcasted_iota(jnp.int32, (tall, slots), 0) % new) // steps
    in_pair_o = (lax.broadcasted_iota(jnp.int32, (tall, hd), 0) % new) // steps
    t = lax.broadcasted_iota(jnp.int32, (tall, slots), 1)

    def attend(msg, keys, values, first):
        q = msg[0:tall]
        v_new = msg[tall + new : tall + 2 * new]
        fresh = lax.dot_general(q, msg[tall : tall + new], nt, preferred_element_type=F32)
        fresh = jnp.where(new_ok, fresh * scale, -jnp.inf)
        old = lax.dot_general(q, keys(0), nt, preferred_element_type=F32)
        start = jnp.full((tall, slots), pos_ref[first], jnp.int32)
        for e in range(1, PAIR):
            other = lax.dot_general(q, keys(e), nt, preferred_element_type=F32)
            old = jnp.where(in_pair == e, other, old)
            start = jnp.where(in_pair == e, pos_ref[first + e], start)
        old = jnp.where(t < start, old * scale, -jnp.inf)
        peak = jnp.maximum(jnp.max(old, axis=-1, keepdims=True), jnp.max(fresh, axis=-1, keepdims=True))
        old = jnp.exp(old - peak)
        fresh = jnp.exp(fresh - peak)
        total = jnp.sum(old, axis=-1, keepdims=True) + jnp.sum(fresh, axis=-1, keepdims=True)
        weights = old.astype(BF16)
        mixed = jnp.dot(weights, values(0), preferred_element_type=F32)
        for e in range(1, PAIR):
            other = jnp.dot(weights, values(e), preferred_element_type=F32)
            mixed = jnp.where(in_pair_o == e, other, mixed)
        mixed = mixed + jnp.dot(fresh.astype(BF16), v_new, preferred_element_type=F32)
        return (mixed / total).astype(BF16)

    @pl.loop(0, n)
    def _(o):
        slot = lax.rem(o, 2)
        source = peer(o)

        @pl.when(o + 1 < n)
        def _():
            for c in kv_load(o + 1, 1 - slot):
                c.start()

        for c in kv_load(o, slot):
            c.wait()

        @pl.when(o > 0)
        def _():
            msg_arrival(source).wait_recv()

        for i in range(AWAY):
            o_s[source, i] = attend(
                msg_r[source, i], lambda e: kbuf[slot, i * PAIR + e], lambda e: vbuf[slot, i * PAIR + e],
                source * rows + (home + i) * PAIR,
            )

        @pl.when(o == 0)
        def _():
            o_r[me, home:pairs] = o_s[me]

        @pl.when(o > 1)
        def _():
            o_copy(peer(o - 1)).start()

    for c in own:
        c.wait()
    o_copy(peer(n - 1)).start()

    def place(which, first, count, lo=0, size=slots):
        src, dst = ((rk, ka_ref), (rv, va_ref))[which]

        @pl.loop(0, count)
        def _(e):
            for h in range(n):
                mix_s[pl.ds(h, size, stride=n), :] = src[h, first + e, lo : lo + size].astype(F32)
            mixed = mix_s[0 : size * n].reshape(size, n, hd)
            slot = lo + lax.broadcasted_iota(jnp.int32, (size, n, hd), 0)
            for s in range(steps):
                at = pl.multiple_of(((first + e) * steps + s) * n, n)
                fresh = (kmix_s, vmix_s)[which][pl.ds(at, n), :]
                mixed = jnp.where(slot == pos_ref[me * rows + first + e] + s, fresh[None], mixed)
            dst[first + e, lo : lo + size] = mixed.astype(BF16)

    @pl.loop(0, home)
    def _(r):
        bulk_wait(0, r, PAIR, slots)
        bulk_wait(1, r, PAIR, slots)
        bulk_next(r + AHEAD)
        place(0, r * PAIR, PAIR)
        place(1, r * PAIR, PAIR)

        @pl.loop(0, n)
        def _(h):
            o_r[h, r] = attend(
                msg_s[h, r], lambda e: rk[h, r * PAIR + e], lambda e: rv[h, r * PAIR + e], me * rows + r * PAIR
            )

    for o in range(1, n):
        o_arrival(peer(o)).wait_recv()
    for h in range(n):
        both = o_r[h].astype(F32)
        for j in range(q_per):
            head = both[:, j * new : (j + 1) * new, :].reshape(num, hd)
            act_s[:, (h * q_per + j) * hd : (h * q_per + j + 1) * hd] = head.astype(BF16)

    def wo_tile(i, w):
        at = pl.ds(pl.multiple_of(i * TILE, TILE), TILE)
        y = jnp.dot(act_s[...], w, preferred_element_type=F32)
        x1_s[:, at] = (hid_s[:, at] + y).astype(BF16).astype(F32)

    stream(wo_hbm, wo_tile)
    act_s[...] = rms(x1_s[...], mn_ref[...].astype(F32).reshape(1, dim)).astype(BF16)
    acc_s[...] = jnp.zeros_like(acc_s)
    tiles = wg_hbm.shape[1] // TILE

    def mlp_loads(i, slot):
        at = pl.ds(pl.multiple_of(i * TILE, TILE), TILE)
        return (
            load(cols(wg_hbm, i), wbuf, wsem, slot),
            load(cols(wu_hbm, i), ubuf, usem, slot),
            load(wd_hbm.at[at, :], dbuf, dsem, slot),
        )

    for c in mlp_loads(0, 0):
        c.start()

    @pl.loop(0, tiles)
    def _(i):
        slot = lax.rem(i, 2)

        @pl.when(i + 1 < tiles)
        def _():
            for c in mlp_loads(i + 1, 1 - slot):
                c.start()

        for c in mlp_loads(i, slot):
            c.wait()
        z = act_s[...]
        gate = jnp.dot(z, wbuf[slot], preferred_element_type=F32)
        up = jnp.dot(z, ubuf[slot], preferred_element_type=F32)
        g = (jax.nn.silu(gate) * up).astype(BF16)
        acc_s[...] += jnp.dot(g, dbuf[slot], preferred_element_type=F32)

    for c in range(0, dim, hd):
        tmp_s[...] = x1_s[:, c : c + hd] + acc_s[:, c : c + hd]
        for s in range(steps):
            out_ref[s, :, c : c + hd] = tmp_s[pl.ds(s, rows, stride=steps), :].astype(BF16)

    for o in range(1, n):
        msg_copy(peer(o)).wait_send()
        o_copy(peer(o)).wait_send()

    @pl.loop(home, pairs - 1)
    def _(r):
        for which in range(2):
            bulk_wait(which, r, PAIR, slots)
            place(which, r * PAIR, PAIR)

    for which, sem, first, count, lo, size in last:
        bulk_wait(which, sem, count, size)
        place(which, first, count, lo, size)

    for which, dst in enumerate((rk, rv)):
        whole = dst.at[pl.ds(0, n - 1)]
        pltpu.make_async_copy(whole, whole, bulk_s.at[which]).wait()


def store_kernel(hid_ref, ka_ref, va_ref, out_hbm, ko_hbm, vo_hbm, hid_sem, sems):
    copies = []
    for b in range(ka_ref.shape[0]):
        copies.append(pltpu.make_async_copy(ka_ref.at[b], ko_hbm.at[b], sems.at[0, b]))
        copies.append(pltpu.make_async_copy(va_ref.at[b], vo_hbm.at[b], sems.at[1, b]))
    copies.append(pltpu.make_async_copy(hid_ref, out_hbm, hid_sem))
    for c in copies:
        c.start()
    for c in copies:
        c.wait()


def solution(mesh):
    row_spec = P(None, ("dp", "x"), None)
    cache_in = P("dp", None, "x", None)
    cache_out = P(("dp", "x"), None, None, None)
    n = mesh.shape["x"]

    def local_run(start_pos, hidden_in, k_heads, v_heads, attn_norm, w_q, w_k, w_v, q_norm, k_norm, w_o, mlp_norm, w_gate, w_up, w_down):
        steps, rows, dim = hidden_in.shape
        slots, hd = k_heads.shape[1], k_heads.shape[3]
        heads = w_q.shape[1] // hd
        num = steps * rows
        pairs = rows // PAIR
        half = hd // 2
        inv_freq = np.power(np.float32(THETA), -np.arange(half, dtype=np.float32) * np.float32(2.0) / np.float32(hd))
        freq = jnp.asarray(np.concatenate([inv_freq, inv_freq])[None, :], F32)
        vmem = pl.BlockSpec(memory_space=pltpu.VMEM)
        hbm = pl.BlockSpec(memory_space=pltpu.HBM)
        tall, new = PAIR * steps * (heads // n), PAIR * steps
        dma = pltpu.SemaphoreType.DMA
        cache = (rows, slots, n, hd)
        blocks = pltpu.VMEM((n, rows, slots, hd), BF16)
        chunk = pltpu.VMEM((2, AWAY * PAIR, slots, hd), BF16)
        wide = pltpu.VMEM((num, dim), F32)
        head = pltpu.VMEM((num, hd), F32)
        arrived = (pltpu.VMEM(hidden_in.shape, BF16), pltpu.VMEM(cache, BF16), pltpu.VMEM(cache, BF16))
        held = pl.pallas_call(
            functools.partial(layer_kernel, n, steps, rows, heads, hd),
            name="layer",
            out_shape=arrived,
            in_specs=[hbm] * 16,
            out_specs=(vmem,) * 3,
            scratch_shapes=[
                pltpu.SMEM(start_pos.shape, jnp.int32), pltpu.VMEM(freq.shape, F32), pltpu.VMEM(hidden_in.shape, BF16), pltpu.VMEM((dim,), BF16),
                pltpu.VMEM((1, hd), BF16), pltpu.VMEM((1, hd), BF16), pltpu.VMEM((dim,), BF16),
                wide, pltpu.VMEM((num, dim), BF16), wide, wide, head, head, head,
                pltpu.VMEM((n, pairs, tall + 2 * new, hd), BF16), pltpu.VMEM((n, AWAY, tall + 2 * new, hd), BF16),
                pltpu.VMEM((n, AWAY, tall, hd), BF16), pltpu.VMEM((n, pairs, tall, hd), BF16),
                blocks, blocks, chunk, chunk,
                pltpu.VMEM((2, dim, TILE), BF16), pltpu.VMEM((2, dim, TILE), BF16), pltpu.VMEM((2, TILE, dim), BF16),
                pltpu.VMEM((slots * n, hd), F32), pltpu.VMEM((num * n, hd), F32), pltpu.VMEM((num * n, hd), F32),
                dma((2,)), dma((2,)), dma((2,)), dma((2,)), dma((2,)), dma((2,)),
                dma((n,)), dma((n,)), dma((n,)), dma((n,)), dma((2,)), dma((pairs,)), dma((pairs + PAIR + 1,)), dma((7,)), pltpu.SemaphoreType.REGULAR,
            ],
            compiler_params=pltpu.CompilerParams(collective_id=0, has_side_effects=True, vmem_limit_bytes=VMEM_LIMIT),
        )(
            start_pos, freq, hidden_in, k_heads.reshape(-1, slots, hd), v_heads.reshape(-1, slots, hd), attn_norm,
            w_q, w_k, w_v, q_norm.reshape(1, -1), k_norm.reshape(1, -1), w_o, mlp_norm, w_gate, w_up, w_down,
        )
        return pl.pallas_call(
            store_kernel,
            name="store",
            out_shape=tuple(jax.ShapeDtypeStruct(a.shape, BF16) for a in (hidden_in, held[1], held[2])),
            in_specs=[vmem] * 3,
            out_specs=(hbm,) * 3,
            scratch_shapes=[dma, dma((2, rows))],
            compiler_params=pltpu.CompilerParams(vmem_limit_bytes=2**20),
        )(*held)

    return jax.shard_map(local_run, mesh=mesh, in_specs=(P("dp"), row_spec, cache_in, cache_in) + (P(),) * 11, out_specs=(row_spec, cache_out, cache_out), check_vma=False)
```

```python
import functools

import jax
import jax.numpy as jnp
import numpy as np
from jax import lax
from jax.experimental import pallas as pl
from jax.experimental.pallas import tpu as pltpu
from jax.sharding import PartitionSpec as P

EPS = 1e-6
THETA = 1000000.0
F32 = jnp.float32
BF16 = jnp.bfloat16
MESH = pl.DeviceIdType.MESH
TILE = 512
PAIR = 2
AWAY = 2
VMEM_LIMIT = 44 * 2**20
AHEAD = 4


def rms(values, gain):
    inv_rms = lax.rsqrt(jnp.mean(values * values, axis=-1, keepdims=True) + EPS)
    return values * inv_rms * gain


def layer_kernel(
    n, steps, rows, heads, hd,
    pos_hbm, freq_hbm, hid_hbm, k_hbm, v_hbm, an_hbm, wq_hbm, wk_hbm, wv_hbm, qn_hbm, kn_hbm, wo_hbm, mn_hbm,
    wg_hbm, wu_hbm, wd_hbm,
    out_ref, ka_ref, va_ref,
    pos_ref, freq_ref, hid_ref, an_ref, qn_ref, kn_ref, mn_ref, hid_s, act_s, x1_s, acc_s, tmp_s, cs_s, sn_s, msg_s, msg_r, o_s, o_r, rk, rv, kbuf, vbuf, wbuf, ubuf, dbuf, mix_s, kmix_s, vmix_s,
    wsem, usem, dsem, ksem, vsem, own_sem, msg_ss, msg_rs, o_ss, o_rs, bulk_s, krs, vrs, in_sem, ready,
):
    me = lax.axis_index("x")
    num = steps * rows
    q_per = heads // n
    pairs = rows // PAIR
    home = pairs - AWAY
    slots = k_hbm.shape[1]
    dim = hid_ref.shape[2]
    tall = PAIR * steps * q_per
    new = PAIR * steps
    barrier = pltpu.get_barrier_semaphore()

    chips = n // 2
    chip, core = me // 2, lax.rem(me, 2)

    def peer(o):
        return lax.rem(me + o, n)

    def away(hops, cross):
        return lax.rem(chip + hops, chips) * 2 + (1 - core if cross else core)

    near = [(0, True), (1, False), (1, True), (chips - 1, False), (chips - 1, True)]
    for to in near:
        pl.semaphore_signal(barrier, inc=1, device_id={"x": away(*to)}, device_id_type=MESH)

    small = [
        pltpu.make_async_copy(src, dst, in_sem.at[i])
        for i, (src, dst) in enumerate((
            (hid_hbm, hid_ref), (an_hbm, an_ref), (freq_hbm, freq_ref), (qn_hbm, qn_ref), (kn_hbm, kn_ref), (mn_hbm, mn_ref), (pos_hbm, pos_ref),
        ))
    ]
    for c in small:
        c.start()

    def cols(hbm, i):
        return hbm.at[:, pl.ds(pl.multiple_of(i * TILE, TILE), TILE)]

    def load(src, dst, sem, slot):
        return pltpu.make_async_copy(src, dst.at[slot], sem.at[slot])

    load(cols(wq_hbm, 0), wbuf, wsem, 0).start()
    pl.semaphore_wait(barrier, len(near))
    pl.semaphore_signal(ready, inc=1, device_id={"x": away(chips - 1, False)}, device_id_type=MESH)

    def send(which, sem, first, count, lo, size, targets):
        for hops, cross in targets:
            to = away(hops, cross)
            pltpu.make_async_remote_copy(
                src_ref=(k_hbm, v_hbm)[which].at[pl.ds(to * rows + first, count), pl.ds(lo, size)],
                dst_ref=(rk, rv)[which].at[me, pl.ds(first, count), pl.ds(lo, size)],
                send_sem=bulk_s.at[which], recv_sem=(krs, vrs)[which].at[sem], device_id={"x": to}, device_id_type=MESH,
            ).start()

    far = [(hops, cross) for hops in range(2, chips - 1) for cross in (False, True)]
    order = near[1::2] + far[:1] + near[2::2] + far[1:] + near[:1]
    far_first = far + near[1::2] + near[2::2] + near[:1]

    last = [(0, pairs - 1, rows - PAIR, PAIR, 0, slots)]
    last += [(1, pairs - 1 + e, rows - PAIR + e, 1, 0, slots) for e in range(PAIR - 1)]
    for i, (lo, size) in enumerate(((0, slots // 2), (slots // 2, slots // 2))):
        last.append((1, pairs - 2 + PAIR + i, rows - 1, 1, lo, size))

    def bulk(r):
        for e in range(PAIR):
            for which in range(2):
                send(which, r, r * PAIR + e, 1, 0, slots, order)

    def bulk_last():
        for which, sem, first, count, lo, size in last:
            send(which, sem, first, count, lo, size, far_first)

    def bulk_next(r):
        @pl.when(r < pairs - 1)
        def _():
            bulk(r)

        @pl.when(r == pairs - 1)
        def _():
            bulk_last()

    def bulk_wait(which, sem, count, size):
        whole = (rk, rv)[which].at[pl.ds(0, n - 1), pl.ds(0, count), pl.ds(0, size)]
        pltpu.make_async_copy(whole, whole, (krs, vrs)[which].at[sem]).wait()

    send(0, 0, 0, 1, 0, slots, near[1:] + near[:1])
    pl.semaphore_wait(ready, 1)
    send(0, 0, 0, 1, 0, slots, far)
    send(1, 0, 0, 1, 0, slots, order)
    for which in range(2):
        send(which, 0, 1, PAIR - 1, 0, slots, order)
    bulk(1)

    own = [
        pltpu.make_async_copy(k_hbm.at[pl.ds(me * rows, rows)], rk.at[me], own_sem.at[0]),
        pltpu.make_async_copy(v_hbm.at[pl.ds(me * rows, rows)], rv.at[me], own_sem.at[1]),
    ]

    def stream(hbm, body, started=False):
        tiles = hbm.shape[1] // TILE
        if not started:
            load(cols(hbm, 0), wbuf, wsem, 0).start()

        @pl.loop(0, tiles)
        def _(i):
            slot = lax.rem(i, 2)

            @pl.when(i + 1 < tiles)
            def _():
                load(cols(hbm, i + 1), wbuf, wsem, 1 - slot).start()

            load(cols(hbm, i), wbuf, wsem, slot).wait()
            body(i, wbuf[slot])

    for c in small:
        c.wait()
    for c in range(0, dim, hd):
        for s in range(steps):
            tmp_s[pl.ds(s, rows, stride=steps), :] = hid_ref[s, :, c : c + hd].astype(F32)
        hid_s[:, c : c + hd] = tmp_s[...]
    act_s[...] = rms(hid_s[...], an_ref[...].astype(F32).reshape(1, dim)).astype(BF16)

    row = lax.broadcasted_iota(jnp.int32, (num, hd), 0)
    pos = jnp.zeros((num, hd), jnp.int32)
    for b in range(rows):
        pos = jnp.where(row // steps == b, pos_ref[me * rows + b], pos)
    angles = (pos + row % steps).astype(F32) * freq_ref[...]
    lane = lax.broadcasted_iota(jnp.int32, (num, hd), 1)
    cs_s[...] = jnp.cos(angles)
    sn_s[...] = jnp.where(lane < hd // 2, -jnp.sin(angles), jnp.sin(angles))

    def rotate(v):
        return v * cs_s[...] + pltpu.roll(v, hd // 2, 1) * sn_s[...]

    per_tile = TILE // hd

    def q_tile(i, w):
        y = jnp.dot(act_s[...], w, preferred_element_type=F32)
        gain = qn_ref[...].astype(F32)
        for g in range(per_tile // q_per):
            parts = []
            for j in range(q_per):
                c = (g * q_per + j) * hd
                head = rotate(rms(y[:, c : c + hd], gain))
                parts.append(head.reshape(pairs, new, hd))
            msg_s[i * (per_tile // q_per) + g, :, 0:tall, :] = jnp.concatenate(parts, axis=1).astype(BF16)

    def k_tile(i, w):
        y = jnp.dot(act_s[...], w, preferred_element_type=F32)
        gain = kn_ref[...].astype(F32)
        for g in range(per_tile):
            head = rotate(rms(y[:, g * hd : (g + 1) * hd], gain))
            msg_s[i * per_tile + g, :, tall : tall + new, :] = head.reshape(pairs, new, hd).astype(BF16)
            kmix_s[pl.ds(i * per_tile + g, num, stride=n), :] = head

    def v_tile(i, w):
        y = jnp.dot(act_s[...], w, preferred_element_type=F32)
        for g in range(per_tile):
            head = y[:, g * hd : (g + 1) * hd]
            msg_s[i * per_tile + g, :, tall + new : tall + 2 * new, :] = head.reshape(pairs, new, hd).astype(BF16)
            vmix_s[pl.ds(i * per_tile + g, num, stride=n), :] = head

    stream(wq_hbm, q_tile, started=True)
    stream(wk_hbm, k_tile)
    stream(wv_hbm, v_tile)

    def msg_copy(to):
        return pltpu.make_async_remote_copy(
            src_ref=msg_s.at[to, pl.ds(home, AWAY)], dst_ref=msg_r.at[me], send_sem=msg_ss.at[to], recv_sem=msg_rs.at[me],
            device_id={"x": to}, device_id_type=MESH,
        )

    def msg_arrival(source):
        return pltpu.make_async_remote_copy(
            src_ref=msg_s.at[source, pl.ds(home, AWAY)], dst_ref=msg_r.at[source], send_sem=msg_ss.at[source],
            recv_sem=msg_rs.at[source], device_id={"x": source}, device_id_type=MESH,
        )

    def o_copy(to):
        return pltpu.make_async_remote_copy(
            src_ref=o_s.at[to], dst_ref=o_r.at[me, pl.ds(home, AWAY)], send_sem=o_ss.at[to], recv_sem=o_rs.at[me],
            device_id={"x": to}, device_id_type=MESH,
        )

    def o_arrival(source):
        return pltpu.make_async_remote_copy(
            src_ref=o_s.at[source], dst_ref=o_r.at[source, pl.ds(home, AWAY)], send_sem=o_ss.at[source], recv_sem=o_rs.at[source],
            device_id={"x": source}, device_id_type=MESH,
        )

    def kv_load(o, slot):
        first = peer(o) * rows + home * PAIR
        return (
            pltpu.make_async_copy(k_hbm.at[pl.ds(first, AWAY * PAIR)], kbuf.at[slot], ksem.at[slot]),
            pltpu.make_async_copy(v_hbm.at[pl.ds(first, AWAY * PAIR)], vbuf.at[slot], vsem.at[slot]),
        )

    for c in kv_load(0, 0):
        c.start()
    for c in own:
        c.start()
    msg_r[me] = msg_s[me, home:pairs]
    for o in range(1, n):
        msg_copy(peer(o)).start()
    for r in range(2, AHEAD):
        bulk(r)

    scale = hd ** -0.5
    nt = (((1,), (1,)), ((), ()))
    r_new = lax.broadcasted_iota(jnp.int32, (tall, new), 0) % new
    c_new = lax.broadcasted_iota(jnp.int32, (tall, new), 1)
    new_ok = (c_new // steps == r_new // steps) & (c_new % steps <= r_new % steps)
    in_pair = (lax.broadcasted_iota(jnp.int32, (tall, slots), 0) % new) // steps
    in_pair_o = (lax.broadcasted_iota(jnp.int32, (tall, hd), 0) % new) // steps
    t = lax.broadcasted_iota(jnp.int32, (tall, slots), 1)

    def attend(msg, keys, values, first):
        q = msg[0:tall]
        v_new = msg[tall + new : tall + 2 * new]
        fresh = lax.dot_general(q, msg[tall : tall + new], nt, preferred_element_type=F32)
        fresh = jnp.where(new_ok, fresh * scale, -jnp.inf)
        old = lax.dot_general(q, keys(0), nt, preferred_element_type=F32)
        start = jnp.full((tall, slots), pos_ref[first], jnp.int32)
        for e in range(1, PAIR):
            other = lax.dot_general(q, keys(e), nt, preferred_element_type=F32)
            old = jnp.where(in_pair == e, other, old)
            start = jnp.where(in_pair == e, pos_ref[first + e], start)
        old = jnp.where(t < start, old * scale, -jnp.inf)
        peak = jnp.maximum(jnp.max(old, axis=-1, keepdims=True), jnp.max(fresh, axis=-1, keepdims=True))
        old = jnp.exp(old - peak)
        fresh = jnp.exp(fresh - peak)
        total = jnp.sum(old, axis=-1, keepdims=True) + jnp.sum(fresh, axis=-1, keepdims=True)
        weights = old.astype(BF16)
        mixed = jnp.dot(weights, values(0), preferred_element_type=F32)
        for e in range(1, PAIR):
            other = jnp.dot(weights, values(e), preferred_element_type=F32)
            mixed = jnp.where(in_pair_o == e, other, mixed)
        mixed = mixed + jnp.dot(fresh.astype(BF16), v_new, preferred_element_type=F32)
        return (mixed / total).astype(BF16)

    @pl.loop(0, n)
    def _(o):
        slot = lax.rem(o, 2)
        source = peer(o)

        @pl.when(o + 1 < n)
        def _():
            for c in kv_load(o + 1, 1 - slot):
                c.start()

        for c in kv_load(o, slot):
            c.wait()

        @pl.when(o > 0)
        def _():
            msg_arrival(source).wait_recv()

        for i in range(AWAY):
            o_s[source, i] = attend(
                msg_r[source, i], lambda e: kbuf[slot, i * PAIR + e], lambda e: vbuf[slot, i * PAIR + e],
                source * rows + (home + i) * PAIR,
            )

        @pl.when(o == 0)
        def _():
            o_r[me, home:pairs] = o_s[me]

        @pl.when(o > 1)
        def _():
            o_copy(peer(o - 1)).start()

    for c in own:
        c.wait()
    o_copy(peer(n - 1)).start()

    def place(which, first, count, lo=0, size=slots):
        src, dst = ((rk, ka_ref), (rv, va_ref))[which]

        @pl.loop(0, count)
        def _(e):
            for h in range(n):
                mix_s[pl.ds(h, size, stride=n), :] = src[h, first + e, lo : lo + size].astype(F32)
            mixed = mix_s[0 : size * n].reshape(size, n, hd)
            slot = lo + lax.broadcasted_iota(jnp.int32, (size, n, hd), 0)
            for s in range(steps):
                at = pl.multiple_of(((first + e) * steps + s) * n, n)
                fresh = (kmix_s, vmix_s)[which][pl.ds(at, n), :]
                mixed = jnp.where(slot == pos_ref[me * rows + first + e] + s, fresh[None], mixed)
            dst[first + e, lo : lo + size] = mixed.astype(BF16)

    @pl.loop(0, home)
    def _(r):
        bulk_wait(0, r, PAIR, slots)
        bulk_wait(1, r, PAIR, slots)
        bulk_next(r + AHEAD)
        place(0, r * PAIR, PAIR)
        place(1, r * PAIR, PAIR)

        @pl.loop(0, n)
        def _(h):
            o_r[h, r] = attend(
                msg_s[h, r], lambda e: rk[h, r * PAIR + e], lambda e: rv[h, r * PAIR + e], me * rows + r * PAIR
            )

    for o in range(1, n):
        o_arrival(peer(o)).wait_recv()
    for h in range(n):
        both = o_r[h].astype(F32)
        for j in range(q_per):
            head = both[:, j * new : (j + 1) * new, :].reshape(num, hd)
            act_s[:, (h * q_per + j) * hd : (h * q_per + j + 1) * hd] = head.astype(BF16)

    def wo_tile(i, w):
        at = pl.ds(pl.multiple_of(i * TILE, TILE), TILE)
        y = jnp.dot(act_s[...], w, preferred_element_type=F32)
        x1_s[:, at] = (hid_s[:, at] + y).astype(BF16).astype(F32)

    stream(wo_hbm, wo_tile)
    act_s[...] = rms(x1_s[...], mn_ref[...].astype(F32).reshape(1, dim)).astype(BF16)
    acc_s[...] = jnp.zeros_like(acc_s)
    tiles = wg_hbm.shape[1] // TILE

    def mlp_loads(i, slot):
        at = pl.ds(pl.multiple_of(i * TILE, TILE), TILE)
        return (
            load(cols(wg_hbm, i), wbuf, wsem, slot),
            load(cols(wu_hbm, i), ubuf, usem, slot),
            load(wd_hbm.at[at, :], dbuf, dsem, slot),
        )

    for c in mlp_loads(0, 0):
        c.start()

    @pl.loop(0, tiles)
    def _(i):
        slot = lax.rem(i, 2)

        @pl.when(i + 1 < tiles)
        def _():
            for c in mlp_loads(i + 1, 1 - slot):
                c.start()

        for c in mlp_loads(i, slot):
            c.wait()
        z = act_s[...]
        gate = jnp.dot(z, wbuf[slot], preferred_element_type=F32)
        up = jnp.dot(z, ubuf[slot], preferred_element_type=F32)
        g = (jax.nn.silu(gate) * up).astype(BF16)
        acc_s[...] += jnp.dot(g, dbuf[slot], preferred_element_type=F32)

    for c in range(0, dim, hd):
        tmp_s[...] = x1_s[:, c : c + hd] + acc_s[:, c : c + hd]
        for s in range(steps):
            out_ref[s, :, c : c + hd] = tmp_s[pl.ds(s, rows, stride=steps), :].astype(BF16)

    for o in range(1, n):
        msg_copy(peer(o)).wait_send()
        o_copy(peer(o)).wait_send()

    @pl.loop(home, pairs - 1)
    def _(r):
        for which in range(2):
            bulk_wait(which, r, PAIR, slots)
            place(which, r * PAIR, PAIR)

    for which, sem, first, count, lo, size in last:
        bulk_wait(which, sem, count, size)
        place(which, first, count, lo, size)

    for which, dst in enumerate((rk, rv)):
        whole = dst.at[pl.ds(0, n - 1)]
        pltpu.make_async_copy(whole, whole, bulk_s.at[which]).wait()


def store_kernel(hid_ref, ka_ref, va_ref, out_hbm, ko_hbm, vo_hbm, hid_sem, sems):
    copies = []
    parts = sems.shape[1]
    size = ka_ref.shape[0] // parts
    for b in range(parts):
        at = pl.ds(b * size, size)
        copies.append(pltpu.make_async_copy(ka_ref.at[at], ko_hbm.at[at], sems.at[0, b]))
        copies.append(pltpu.make_async_copy(va_ref.at[at], vo_hbm.at[at], sems.at[1, b]))
    copies.append(pltpu.make_async_copy(hid_ref, out_hbm, hid_sem))
    for c in copies:
        c.start()
    for c in copies:
        c.wait()


def solution(mesh):
    row_spec = P(None, ("dp", "x"), None)
    cache_in = P("dp", None, "x", None)
    cache_out = P(("dp", "x"), None, None, None)
    n = mesh.shape["x"]

    def local_run(start_pos, hidden_in, k_heads, v_heads, attn_norm, w_q, w_k, w_v, q_norm, k_norm, w_o, mlp_norm, w_gate, w_up, w_down):
        steps, rows, dim = hidden_in.shape
        slots, hd = k_heads.shape[1], k_heads.shape[3]
        heads = w_q.shape[1] // hd
        num = steps * rows
        pairs = rows // PAIR
        half = hd // 2
        inv_freq = np.power(np.float32(THETA), -np.arange(half, dtype=np.float32) * np.float32(2.0) / np.float32(hd))
        freq = jnp.asarray(np.concatenate([inv_freq, inv_freq])[None, :], F32)
        vmem = pl.BlockSpec(memory_space=pltpu.VMEM)
        hbm = pl.BlockSpec(memory_space=pltpu.HBM)
        tall, new = PAIR * steps * (heads // n), PAIR * steps
        dma = pltpu.SemaphoreType.DMA
        cache = (rows, slots, n, hd)
        blocks = pltpu.VMEM((n, rows, slots, hd), BF16)
        chunk = pltpu.VMEM((2, AWAY * PAIR, slots, hd), BF16)
        wide = pltpu.VMEM((num, dim), F32)
        head = pltpu.VMEM((num, hd), F32)
        arrived = (pltpu.VMEM(hidden_in.shape, BF16), pltpu.VMEM(cache, BF16), pltpu.VMEM(cache, BF16))
        held = pl.pallas_call(
            functools.partial(layer_kernel, n, steps, rows, heads, hd),
            name="layer",
            out_shape=arrived,
            in_specs=[hbm] * 16,
            out_specs=(vmem,) * 3,
            scratch_shapes=[
                pltpu.SMEM(start_pos.shape, jnp.int32), pltpu.VMEM(freq.shape, F32), pltpu.VMEM(hidden_in.shape, BF16), pltpu.VMEM((dim,), BF16),
                pltpu.VMEM((1, hd), BF16), pltpu.VMEM((1, hd), BF16), pltpu.VMEM((dim,), BF16),
                wide, pltpu.VMEM((num, dim), BF16), wide, wide, head, head, head,
                pltpu.VMEM((n, pairs, tall + 2 * new, hd), BF16), pltpu.VMEM((n, AWAY, tall + 2 * new, hd), BF16),
                pltpu.VMEM((n, AWAY, tall, hd), BF16), pltpu.VMEM((n, pairs, tall, hd), BF16),
                blocks, blocks, chunk, chunk,
                pltpu.VMEM((2, dim, TILE), BF16), pltpu.VMEM((2, dim, TILE), BF16), pltpu.VMEM((2, TILE, dim), BF16),
                pltpu.VMEM((slots * n, hd), F32), pltpu.VMEM((num * n, hd), F32), pltpu.VMEM((num * n, hd), F32),
                dma((2,)), dma((2,)), dma((2,)), dma((2,)), dma((2,)), dma((2,)),
                dma((n,)), dma((n,)), dma((n,)), dma((n,)), dma((2,)), dma((pairs,)), dma((pairs + PAIR,)), dma((7,)), pltpu.SemaphoreType.REGULAR,
            ],
            compiler_params=pltpu.CompilerParams(collective_id=0, has_side_effects=True, vmem_limit_bytes=VMEM_LIMIT),
        )(
            start_pos, freq, hidden_in, k_heads.reshape(-1, slots, hd), v_heads.reshape(-1, slots, hd), attn_norm,
            w_q, w_k, w_v, q_norm.reshape(1, -1), k_norm.reshape(1, -1), w_o, mlp_norm, w_gate, w_up, w_down,
        )
        return pl.pallas_call(
            store_kernel,
            name="store",
            out_shape=tuple(jax.ShapeDtypeStruct(a.shape, BF16) for a in (hidden_in, held[1], held[2])),
            in_specs=[vmem] * 3,
            out_specs=(hbm,) * 3,
            scratch_shapes=[dma, dma((2, 4))],
            compiler_params=pltpu.CompilerParams(vmem_limit_bytes=2**20),
        )(*held)

    return jax.shard_map(local_run, mesh=mesh, in_specs=(P("dp"), row_spec, cache_in, cache_in) + (P(),) * 11, out_specs=(row_spec, cache_out, cache_out), check_vma=False)
```
